256 devices in a mesh: rows: 64 (over z, x, core), cols: 4 (over y).
Axes of the slice: x: 4, y: 4, z: 8, core: 2. Of those that a mesh axis runs over, the one named last changes fastest.
Arguments:
- tables: float32 [4, 32768, 512], P(None, 'rows', 'cols'), may hold values from -1.5 to 1.5
- dense_features: float32 [2048, 512], P('rows', 'cols'), may hold values from -6 to 6
- slot_rows: int32 [64, 64, 4, 64], P('rows'), may hold values from 0 to 511, as said below
- slot_examples: int32 [64, 64, 4, 64], P('rows'), may hold values from 0 to 31, as said below
- slot_counts: int32 [64, 64, 4], P('rows'), may hold values from 21 to 64, as said below
Outputs:
- pooled: float32 [2048, 4, 512], P('rows', None, 'cols')
- interactions: float32 [2048, 10], P('rows')
The draws below stay inside these ranges and needn't reach their ends.
Inputs may be any that keep to these rules, and one draw needn't show every extreme that they name: slot_rows[s, o, t, c] names row o * 512 + value of table t. `slot_examples`: an example of the source device s. `slot_counts`: slots 0 to count - 1 of a bucket are live, the others unused; some bucket of every draw is full.
All inputs are finite; a program needn't handle non-finite values.
Results may differ from the reference program's by a relative error of at most 0.0003.
Values sent between devices are 32-bit elements; how exact they have to be, the bound alone decides.
No kernel may reach another device: no remote copies, remote signals or barrier semaphores. Data moves between devices by JAX's collectives and lax.ppermute only.
A program may use at most 64 MiB of HBM per device.

```python
import jax
import jax.numpy as jnp
import numpy as np
from jax import lax

E = 512
TABLES = 4
ROWS_DEV = 512
B_DEV = 32
CAP = 64
BATCH = 2048
TABLE_ROWS = 32768
N_ROWS = 64


def draw_slot_counts(key, part):
    first_key, second_key = jax.random.split(jax.random.fold_in(key, 11))
    base = jax.random.randint(first_key, (N_ROWS, N_ROWS, TABLES), CAP // 3, 2 * CAP // 3 + 1)
    hottest = jax.random.randint(second_key, (TABLES,), 0, N_ROWS)
    is_hot = jnp.arange(N_ROWS)[None, :, None] == hottest[None, None, :]
    return jnp.where(is_hot, CAP, base).astype(jnp.int32)


def draw_slot_rows(key, part):
    first_key, second_key, third_key = jax.random.split(jax.random.fold_in(key, 23), 3)
    shape_all = (N_ROWS, N_ROWS, TABLES, CAP)
    first_draw = jax.random.randint(first_key, shape_all, 0, ROWS_DEV)
    second_draw = jax.random.randint(second_key, shape_all, 0, ROWS_DEV)
    offsets = jax.random.randint(third_key, (N_ROWS, TABLES), 0, ROWS_DEV)
    skewed = first_draw * second_draw // ROWS_DEV
    return ((skewed + offsets[None, :, :, None]) % ROWS_DEV).astype(jnp.int32)


def draw_slot_examples(key, part):
    first_key, second_key = jax.random.split(jax.random.fold_in(key, 37))
    shape_all = (N_ROWS, N_ROWS, TABLES, CAP)
    first_draw = jax.random.randint(first_key, shape_all, 0, B_DEV)
    second_draw = jax.random.randint(second_key, shape_all, 0, B_DEV)
    return jnp.minimum(first_draw, second_draw).astype(jnp.int32)


def shard_levels(key, dims, cuts, least, top_value):
    def one(axis_at, blocks):
        heights = jax.random.uniform(jax.random.fold_in(jax.random.fold_in(key, 6), axis_at), (blocks,), jnp.float32, least / len(cuts), top_value / len(cuts))
        return jnp.repeat(jnp.exp(heights), dims[axis_at] // blocks).reshape((-1,) + (1,) * (len(dims) - axis_at - 1))

    factor_of = one(*cuts[0])
    for cut in cuts[1:]:
        factor_of = factor_of * one(*cut)
    return factor_of


def bell_draw(rng, extent, width, most, cuts=(), kind=jnp.bfloat16):
    array = jax.random.normal(rng, extent, jnp.float32) * width
    if len(cuts) > 0:
        array = shard_levels(rng, extent, cuts, -0.22, 0.18) * array
    return jnp.clip(array, min=-most, max=most).astype(kind)


def setup_inputs(seed: int = 0) -> dict:
    keys = jax.random.split(jax.random.key(seed), 6)
    tables = bell_draw(keys[0], (TABLES, TABLE_ROWS, E), 0.25, 1.5, ((1, 64), (2, 4)), jnp.float32)
    dense_features = bell_draw(keys[1], (BATCH, E), 1.0, 6.0, ((0, 64), (1, 4)), jnp.float32)
    slot_rows = draw_slot_rows(jax.random.fold_in(keys[5], 71), 0)
    slot_examples = draw_slot_examples(jax.random.fold_in(keys[5], 71), 0)
    slot_counts = draw_slot_counts(jax.random.fold_in(keys[5], 71), 0)
    return {"tables": tables, "dense_features": dense_features, "slot_rows": slot_rows, "slot_examples": slot_examples, "slot_counts": slot_counts}


def reference(tables, dense_features, slot_rows, slot_examples, slot_counts):
    slot_index = jnp.arange(CAP, dtype=jnp.int32)
    live_slots = slot_index[None, None, None, :] < slot_counts[:, :, :, None]
    owner_base = (jnp.arange(N_ROWS, dtype=jnp.int32) * ROWS_DEV)[:, None, None]
    table_index = jnp.arange(TABLES, dtype=jnp.int32)[None, :, None]

    def one_source(pieces):
        rows_here, examples_here, live_here = pieces
        global_rows = (rows_here + owner_base).astype(jnp.int32)
        looked = tables[table_index, global_rows]
        looked = jnp.where(live_here[:, :, :, None], looked, jnp.zeros_like(looked))
        segment_ids = (examples_here * TABLES + table_index).astype(jnp.int32)
        summed = jax.ops.segment_sum(looked.reshape(-1, E), segment_ids.reshape(-1), num_segments=B_DEV * TABLES)
        return summed.reshape(B_DEV, TABLES, E)

    pooled = lax.map(one_source, (slot_rows, slot_examples, live_slots)).reshape(BATCH, TABLES, E)
    vectors = jnp.concatenate([dense_features[:, None, :], pooled], axis=1)
    gram_matrix = jnp.einsum("bie,bje->bij", vectors, vectors, precision=lax.Precision.HIGHEST)
    pair_first, pair_second = np.triu_indices(TABLES + 1, 1)
    interactions = gram_matrix[:, pair_first, pair_second] * (E ** -0.5)
    return pooled, interactions
```

```python
import functools

import jax
import jax.numpy as jnp
from jax import lax
from jax.experimental import pallas as pl
from jax.experimental.pallas import tpu as pltpu
from jax.sharding import Mesh
from jax.sharding import PartitionSpec as P

ROWS = ("z", "x", "c")
DEAD = 1 << 20


def shifted(value, axis, by):
    size = lax.axis_size(axis)
    return lax.ppermute(value, axis, [(i, (i + by) % size) for i in range(size)])


def split_kernel(own_ref, other_ref, out_ref):
    for place, ref in enumerate((own_ref, other_ref)):
        full = ref[...]
        high = full.astype(jnp.bfloat16)
        low = (full - high.astype(jnp.float32)).astype(jnp.bfloat16)
        out_ref[place, :, :, :128] = high
        out_ref[place, :, :, 128:] = low


def split_tables(own, other):
    tables, rows, width = own.shape
    return pl.pallas_call(
        split_kernel,
        grid=(tables,),
        in_specs=[pl.BlockSpec((1, rows, width), lambda t: (t, 0, 0))] * 2,
        out_specs=pl.BlockSpec((2, 1, rows, 2 * width), lambda t: (0, t, 0, 0)),
        out_shape=jax.ShapeDtypeStruct((2, tables, rows, 2 * width), jnp.bfloat16),
        cost_estimate=pl.CostEstimate(flops=3000000, bytes_accessed=4 << 20, transcendentals=0),
    )(own, other)


def bags_kernel(me_ref, ids_ref, tables_ref, out_ref, *, examples):
    sources = ids_ref.shape[0]
    owners, tables, rows, wide = tables_ref.shape
    slots = ids_ref.shape[3] // 2
    group = 4
    core = me_ref[1]
    row_iota = lax.broadcasted_iota(jnp.int32, (slots, rows), 1)
    key_iota = lax.broadcasted_iota(jnp.int32, (group * examples, group * slots), 0)

    def one_hot(mask):
        return jnp.where(mask, 1.0, 0.0).astype(jnp.bfloat16)

    for t in range(tables):
        total = [None] * (sources // group)
        for o in range(owners):
            ids = ids_ref[:, 0, o * tables + t, :]
            columns = jnp.swapaxes(ids, 0, 1)
            table = tables_ref[o ^ core, t]
            for g in range(sources // group):
                picks = jnp.concatenate(
                    [
                        one_hot(columns[:slots, s : s + 1] == row_iota)
                        for s in range(g * group, (g + 1) * group)
                    ],
                    axis=0,
                )
                looked = jnp.dot(picks, table, preferred_element_type=jnp.float32)
                keys = jnp.concatenate(
                    [
                        ids[g * group + s : g * group + s + 1, slots:] + s * examples
                        for s in range(group)
                    ],
                    axis=1,
                )
                into = one_hot(keys == key_iota)
                part = jnp.dot(into, looked.astype(jnp.bfloat16), preferred_element_type=jnp.float32)
                total[g] = part if total[g] is None else total[g] + part
        for g in range(sources // group):
            summed = total[g][:, : wide // 2] + total[g][:, wide // 2 :]
            out_ref[0, g * group : (g + 1) * group, t * examples : (t + 1) * examples, :] = (
                summed.reshape(group, examples, wide // 2)
            )


def bags(me, ids, tables, offsets, examples):
    sources, ring = ids.shape[0], ids.shape[1]
    owners, count, rows, wide = tables.shape
    first = offsets[0]
    step = (offsets[1] - offsets[0]) if len(offsets) > 1 else 0
    flops = 2 * len(offsets) * sources * owners * count * 64 * wide * (rows + 128)
    return pl.pallas_call(
        functools.partial(bags_kernel, examples=examples),
        grid_spec=pltpu.PrefetchScalarGridSpec(
            num_scalar_prefetch=1,
            grid=(len(offsets),),
            in_specs=[
                pl.BlockSpec(
                    (sources, 1) + ids.shape[2:],
                    lambda k, me: (0, lax.rem(me[0] + first + k * step, ring), 0, 0),
                ),
                pl.BlockSpec(tables.shape, lambda k, me: (0, 0, 0, 0)),
            ],
            out_specs=pl.BlockSpec(
                (1, sources, count * examples, wide // 2), lambda k, me: (k, 0, 0, 0)
            ),
        ),
        out_shape=jax.ShapeDtypeStruct(
            (len(offsets), sources, count * examples, wide // 2), jnp.float32
        ),
        cost_estimate=pl.CostEstimate(flops=flops, bytes_accessed=4 << 20, transcendentals=0),
    )(me, ids, tables)


def close_kernel(parts_ref, dense_ref, pooled_ref, pairs_ref, *, examples):
    pooled = parts_ref[0]
    for k in range(1, parts_ref.shape[0]):
        pooled = pooled + parts_ref[k]
    tables = pooled.shape[0] // examples
    vectors = [dense_ref[...]]
    for t in range(tables):
        one = pooled[t * examples : (t + 1) * examples]
        pooled_ref[:, t, :] = one
        vectors.append(one)
    lane = lax.broadcasted_iota(jnp.int32, pairs_ref.shape, 1)
    pairs = jnp.zeros(pairs_ref.shape, jnp.float32)
    place = 0
    for i in range(tables + 1):
        for j in range(i + 1, tables + 1):
            product = jnp.sum(vectors[i] * vectors[j], axis=1, keepdims=True)
            pairs = jnp.where(lane == place, product, pairs)
            place += 1
    pairs_ref[...] = pairs


def close(parts, dense, tables):
    examples, width = dense.shape
    return pl.pallas_call(
        functools.partial(close_kernel, examples=examples),
        out_shape=(
            jax.ShapeDtypeStruct((examples, tables, width), jnp.float32),
            jax.ShapeDtypeStruct((examples, 128), jnp.float32),
        ),
    )(parts, dense)


def body(embedding, tables, dense_features, slot_rows, slot_examples, slot_counts):
    count = tables.shape[0]
    examples = dense_features.shape[0]
    capacity = slot_rows.shape[3]
    z, x, c = (lax.axis_size(a) for a in ROWS)
    other = shifted(tables, "c", 1)
    live = jnp.arange(capacity, dtype=jnp.int32) < slot_counts[0, :, :, None]
    ids = jnp.concatenate([slot_rows[0], jnp.where(live, slot_examples[0], DEAD)], axis=2)
    ids = ids.reshape(z * x, c * count, 2 * capacity)
    ids = lax.all_to_all(ids, ("z", "x"), 0, 0, tiled=True)
    ids = ids.reshape(z, x, c * count, 2 * capacity)
    split = split_tables(tables, other)
    me = jnp.stack([lax.axis_index("x"), lax.axis_index("c")]).astype(jnp.int32)

    far = bags(me, ids, split, (2,), examples)[0]
    half = far.shape[1] // 2
    from_left = shifted(far[:, :half], "x", 1)
    from_right = shifted(far[:, half:], "x", -1)
    near = bags(me, ids, split, (1, 3), examples)
    to_right = jnp.concatenate([near[0, :, :half] + from_left, near[0, :, half:]], axis=1)
    to_left = jnp.concatenate([near[1, :, :half], near[1, :, half:] + from_right], axis=1)
    right = shifted(to_right, "x", 1)
    left = shifted(to_left, "x", -1)
    mine = bags(me, ids, split, (0,), examples)[0]
    parts = lax.all_to_all(mine + right + left, "z", 0, 0, tiled=True)
    pooled, pairs = close(parts, dense_features, count)
    opposite = shifted(pairs, "y", 2)
    beside = shifted(pairs, "y", 1) + shifted(pairs, "y", -1)
    total = ((pairs + opposite) + beside) * embedding**-0.5
    return pooled, total[:, : count * (count + 1) // 2]


def solution(mesh):
    torus = Mesh(mesh.devices.reshape(8, 4, 2, mesh.shape["cols"]), ROWS + ("y",))
    return jax.shard_map(
        functools.partial(body, 512),
        mesh=torus,
        in_specs=(
            P(None, ROWS, "y"),
            P(ROWS, "y"),
            P(ROWS, None, None, None),
            P(ROWS, None, None, None),
            P(ROWS, None, None),
        ),
        out_specs=(P(ROWS, None, "y"), P(ROWS, None)),
        check_vma=False,
    )
```

```python
import functools

import jax
import jax.numpy as jnp
from jax import lax
from jax.experimental import pallas as pl
from jax.experimental.pallas import tpu as pltpu
from jax.sharding import Mesh
from jax.sharding import PartitionSpec as P

ROWS = ("z", "x", "c")
DEAD = 1 << 20
VMEM = pl.BlockSpec(memory_space=pltpu.VMEM)


def shifted(value, axis, by):
    size = lax.axis_size(axis)
    return lax.ppermute(value, axis, [(i, (i + by) % size) for i in range(size)])


def local_kernel(kernel, out_shape, operands, flops=1 << 20, vmem=12 << 20):
    single = not isinstance(out_shape, tuple)
    return pl.pallas_call(
        kernel,
        in_specs=[VMEM] * len(operands),
        out_specs=VMEM if single else (VMEM,) * len(out_shape),
        out_shape=out_shape,
        compiler_params=pltpu.CompilerParams(vmem_limit_bytes=vmem),
        cost_estimate=pl.CostEstimate(flops=flops, bytes_accessed=1 << 20, transcendentals=0),
    )(*operands)


def prepare_kernel(rows_ref, examples_ref, counts_ref, out_ref):
    buckets, capacity = rows_ref.shape
    tables, owners = counts_ref.shape
    bucket = lax.broadcasted_iota(jnp.int32, (buckets, owners), 0)
    owner = lax.broadcasted_iota(jnp.int32, (buckets, owners), 1)
    spread = jnp.where(bucket // tables == owner, 1.0, 0.0).astype(jnp.bfloat16)
    counts = counts_ref[...].astype(jnp.float32).astype(jnp.bfloat16)
    by_table = lax.dot_general(
        spread, counts, (((1,), (1,)), ((), ())), preferred_element_type=jnp.float32
    )
    table = lax.broadcasted_iota(jnp.int32, (buckets, tables), 1)
    own = lax.broadcasted_iota(jnp.int32, (buckets, tables), 0) % tables
    count = jnp.sum(jnp.where(table == own, by_table, 0.0), axis=1, keepdims=True)
    slot = lax.broadcasted_iota(jnp.int32, (buckets, capacity), 1).astype(jnp.float32)
    out_ref[:, :capacity] = rows_ref[...]
    out_ref[:, capacity:] = jnp.where(slot < count, examples_ref[...], DEAD)


def split_kernel(own_ref, other_ref, out_ref):
    width = own_ref.shape[2]
    for place, ref in enumerate((own_ref, other_ref)):
        for t in range(ref.shape[0]):
            full = ref[t]
            high = full.astype(jnp.bfloat16)
            out_ref[place, t, :, :width] = high
            out_ref[place, t, :, width:] = (full - high.astype(jnp.float32)).astype(jnp.bfloat16)


def one_hot(mask):
    return jnp.where(mask, 1.0, 0.0).astype(jnp.bfloat16)


def bags_kernel(ids_ref, tables_ref, *out_refs, items, examples):
    sources, ring = ids_ref.shape[:2]
    owners, count, rows, wide = tables_ref.shape
    slots = ids_ref.shape[3] // 2
    group = 4
    core = lax.axis_index("c")
    me = lax.axis_index("x")
    row_iota = lax.broadcasted_iota(jnp.int32, (slots, rows), 1)
    key_iota = lax.broadcasted_iota(jnp.int32, (group * examples, group * slots), 0)
    for (away, tables), out_ref in zip(items, out_refs):
        column = lax.rem(me + away, ring)
        for place, t in enumerate(tables):
            total = [None] * (sources // group)
            for o in range(owners):
                ids = ids_ref[:, column, o * count + t, :]
                columns = jnp.swapaxes(ids, 0, 1)
                table = tables_ref[o ^ core, t]
                for g in range(sources // group):
                    first = g * group
                    picks = jnp.concatenate(
                        [
                            one_hot(columns[:slots, s : s + 1] == row_iota)
                            for s in range(first, first + group)
                        ],
                        axis=0,
                    )
                    looked = jnp.dot(picks, table, preferred_element_type=jnp.float32)
                    keys = jnp.concatenate(
                        [
                            ids[first + s : first + s + 1, slots:] + s * examples
                            for s in range(group)
                        ],
                        axis=1,
                    )
                    part = jnp.dot(
                        one_hot(keys == key_iota),
                        looked.astype(jnp.bfloat16),
                        preferred_element_type=jnp.float32,
                    )
                    total[g] = part if total[g] is None else total[g] + part
            for g in range(sources // group):
                summed = total[g][:, : wide // 2] + total[g][:, wide // 2 :]
                out_ref[
                    g * group : (g + 1) * group, place * examples : (place + 1) * examples, :
                ] = summed.reshape(group, examples, wide // 2)


def bags(ids, tables, items, examples):
    sources = ids.shape[0]
    owners, count, rows, wide = tables.shape
    tasks = sum(len(t) for _, t in items)
    out = tuple(
        jax.ShapeDtypeStruct((sources, len(t) * examples, wide // 2), jnp.float32)
        for _, t in items
    )
    return local_kernel(
        functools.partial(bags_kernel, items=items, examples=examples),
        out,
        (ids, tables),
        flops=2 * tasks * sources * owners * 64 * wide * (rows + 128),
    )


def add_kernel(left_ref, left_part_ref, right_ref, right_part_ref, a_ref, b_ref):
    a_ref[...] = left_ref[...] + left_part_ref[...]
    b_ref[...] = right_ref[...] + right_part_ref[...]


def join_kernel(*refs):
    out_ref = refs[-1]
    half = refs[0].shape[1]
    for place in range(2):
        one, two, three = refs[3 * place : 3 * place + 3]
        out_ref[:, place * half : (place + 1) * half, :] = one[...] + two[...] + three[...]


def close_kernel(parts_ref, dense_ref, pooled_ref, pairs_ref, *, examples):
    pooled = parts_ref[0]
    for k in range(1, parts_ref.shape[0]):
        pooled = pooled + parts_ref[k]
    tables = pooled.shape[0] // examples
    vectors = [dense_ref[...]]
    for t in range(tables):
        one = pooled[t * examples : (t + 1) * examples]
        pooled_ref[:, t, :] = one
        vectors.append(one)
    lane = lax.broadcasted_iota(jnp.int32, dense_ref.shape, 1)
    pairs = jnp.zeros(dense_ref.shape, jnp.float32)
    place = 0
    for i in range(tables + 1):
        for j in range(i + 1, tables + 1):
            product = jnp.sum(vectors[i] * vectors[j], axis=1, keepdims=True)
            pairs = jnp.where(lane == place, product, pairs)
            place += 1
    pairs_ref[...] = jnp.swapaxes(pairs, 0, 1)[: pairs_ref.shape[0]]


def body(embedding, tables, dense_features, slot_rows, slot_examples, slot_counts):
    count = tables.shape[0]
    examples, width = dense_features.shape
    capacity = slot_rows.shape[3]
    z, x, c = (lax.axis_size(a) for a in ROWS)
    owners = z * x * c
    other = shifted(tables, "c", 1)
    ids = local_kernel(
        prepare_kernel,
        jax.ShapeDtypeStruct((owners * count, 2 * capacity), jnp.int32),
        (
            slot_rows.reshape(owners * count, capacity),
            slot_examples.reshape(owners * count, capacity),
            slot_counts[0].T,
        ),
    )
    ids = ids.reshape(z * x, c * count, 2 * capacity)
    ids = lax.all_to_all(ids, ("z", "x"), 0, 0, tiled=True)
    ids = ids.reshape(z, x, c * count, 2 * capacity)
    split = local_kernel(
        split_kernel,
        jax.ShapeDtypeStruct((2,) + tables.shape[:2] + (2 * width,), jnp.bfloat16),
        (tables, other),
        flops=4 << 20,
    )
    low, high = tuple(range(count // 2)), tuple(range(count // 2, count))

    far_low, far_high = bags(ids, split, ((2, low), (2, high)), examples)
    from_left = shifted(far_low, "x", 1)
    from_right = shifted(far_high, "x", -1)
    right_high, left_low = bags(ids, split, ((1, high), (3, low)), examples)
    right_high = shifted(right_high, "x", 1)
    left_low = shifted(left_low, "x", -1)
    right_low, left_high = bags(ids, split, ((1, low), (3, high)), examples)
    half = jax.ShapeDtypeStruct(right_low.shape, jnp.float32)
    right_low, left_high = local_kernel(
        add_kernel, (half, half), (right_low, from_left, left_high, from_right)
    )
    right_low = shifted(right_low, "x", 1)
    left_high = shifted(left_high, "x", -1)
    mine_low, mine_high = bags(ids, split, ((0, low), (0, high)), examples)
    parts = local_kernel(
        join_kernel,
        jax.ShapeDtypeStruct((z, count * examples, width), jnp.float32),
        (mine_low, right_low, left_low, mine_high, right_high, left_high),
    )
    parts = lax.all_to_all(parts, "z", 0, 0, tiled=True)
    pairs = count * (count + 1) // 2
    pooled, products = local_kernel(
        functools.partial(close_kernel, examples=examples),
        (
            jax.ShapeDtypeStruct((examples, count, width), jnp.float32),
            jax.ShapeDtypeStruct((pairs, examples), jnp.float32),
        ),
        (parts, dense_features),
    )
    opposite = shifted(products, "y", 2)
    beside = shifted(products, "y", 1) + shifted(products, "y", -1)
    total = ((products + opposite) + beside) * embedding**-0.5
    return pooled, total.T


def solution(mesh):
    torus = Mesh(mesh.devices.reshape(8, 4, 2, mesh.shape["cols"]), ROWS + ("y",))
    return jax.shard_map(
        functools.partial(body, 512),
        mesh=torus,
        in_specs=(
            P(None, ROWS, "y"),
            P(ROWS, "y"),
            P(ROWS, None, None, None),
            P(ROWS, None, None, None),
            P(ROWS, None, None),
        ),
        out_specs=(P(ROWS, None, "y"), P(ROWS, None)),
        check_vma=False,
    )
```

```python
import functools

import jax
import jax.numpy as jnp
from jax import lax
from jax.experimental import pallas as pl
from jax.experimental.pallas import tpu as pltpu
from jax.sharding import Mesh
from jax.sharding import PartitionSpec as P


Z = ("zq", "zp")
ROWS = Z + ("x", "c")
DEAD = 1 << 20
VMEM = pl.BlockSpec(memory_space=pltpu.VMEM)


def shifted(value, axis, by):
    size = lax.axis_size(axis)
    return lax.ppermute(value, axis, [(i, (i + by) % size) for i in range(size)])


def local_kernel(kernel, out_shape, operands, flops=1 << 20, vmem=12 << 20, scratch=()):
    single = not isinstance(out_shape, tuple)
    return pl.pallas_call(
        kernel,
        in_specs=[VMEM] * len(operands),
        out_specs=VMEM if single else (VMEM,) * len(out_shape),
        out_shape=out_shape,
        scratch_shapes=scratch,
        compiler_params=pltpu.CompilerParams(vmem_limit_bytes=vmem),
        cost_estimate=pl.CostEstimate(flops=flops, bytes_accessed=1 << 20, transcendentals=0),
    )(*operands)


def prepare_kernel(rows_ref, examples_ref, counts_ref, out_ref, live_ref):
    depth, across, under, capacity = rows_ref.shape
    tables, owners = counts_ref.shape
    buckets = owners * tables
    bucket = lax.broadcasted_iota(jnp.int32, (buckets, owners), 0)
    owner = lax.broadcasted_iota(jnp.int32, (buckets, owners), 1)
    spread = jnp.where(bucket // tables == owner, 1.0, 0.0).astype(jnp.bfloat16)
    table = lax.broadcasted_iota(jnp.int32, (buckets, tables), 1)
    own = lax.broadcasted_iota(jnp.int32, (buckets, tables), 0) % tables
    slot = lax.broadcasted_iota(jnp.int32, (buckets, capacity), 1).astype(jnp.float32)
    counts = counts_ref[...].astype(jnp.float32).astype(jnp.bfloat16)
    by_table = lax.dot_general(
        spread, counts, (((1,), (1,)), ((), ())), preferred_element_type=jnp.float32
    )
    count = jnp.sum(jnp.where(table == own, by_table, 0.0), axis=1, keepdims=True)
    live = jnp.where(slot < count, examples_ref[...].reshape(buckets, capacity), DEAD)
    live_ref[...] = live.reshape(live_ref.shape)
    odd = lax.axis_index("zp")
    early = lax.broadcasted_iota(jnp.int32, (across, under, capacity), 1) % tables < tables // 2
    for q in range(depth // 2):
        here = 2 * q + odd
        first = 2 * q + 1 - odd
        second = lax.rem(2 * q + depth - 1 + 3 * odd, depth)
        for ref, lanes in ((rows_ref, slice(0, capacity)), (live_ref, slice(capacity, None))):
            out_ref[q, :, :under, lanes] = ref[here]
            out_ref[q, :, under:, lanes] = jnp.where(early, ref[first], ref[second])


def split_kernel(*refs):
    out_ref = refs[-1]
    width = out_ref.shape[3] // 2
    sides = (refs[:1], refs[1:2]) if len(refs) == 3 else (refs[:2], refs[2:4])
    for place, pieces in enumerate(sides):
        t = 0
        for ref in pieces:
            for k in range(ref.shape[0]):
                full = ref[k]
                high = full.astype(jnp.bfloat16)
                out_ref[place, t, :, :width] = high
                out_ref[place, t, :, width:] = (full - high.astype(jnp.float32)).astype(
                    jnp.bfloat16
                )
                t += 1


def split_tables(pieces, count, rows, width):
    return local_kernel(
        split_kernel,
        jax.ShapeDtypeStruct((2, count, rows, 2 * width), jnp.bfloat16),
        pieces,
        flops=4 << 20,
    )


def one_hot(mask):
    return jnp.where(mask, 1.0, 0.0).astype(jnp.bfloat16)


def bags_kernel(ids_ref, near_ref, partner_ref, out_ref, looked_ref, *, away, examples):
    group, ring, messages, lanes = ids_ref.shape
    cores, count, rows, wide = near_ref.shape
    slots = lanes // 2
    core = lax.axis_index("c")
    column = lax.rem(lax.axis_index("x") + away, ring)
    depth = lax.axis_index("zq")
    row_iota = lax.broadcasted_iota(jnp.int32, (slots, rows), 1)
    key_iota = lax.broadcasted_iota(jnp.int32, (group * examples, group * slots), 0)
    ids = [ids_ref[lax.rem(depth + j, group), column] for j in range(group)]
    columns = jnp.swapaxes(jnp.concatenate(ids, axis=0), 0, 1)
    keys = jnp.concatenate([ids[j][:, slots:] + j * examples for j in range(group)], axis=1)
    for t in range(count):
        into = []
        for block, tables_ref in enumerate((near_ref, partner_ref)):
            for o in range(cores):
                message = (block * cores + o) * count + t
                picks = jnp.concatenate(
                    [
                        one_hot(
                            columns[:slots, j * messages + message : j * messages + message + 1]
                            == row_iota
                        )
                        for j in range(group)
                    ],
                    axis=0,
                )
                looked = jnp.dot(
                    picks, tables_ref[o ^ core, t], preferred_element_type=jnp.float32
                )
                place = (block * cores + o) * group * slots
                looked_ref[t, place : place + group * slots, :] = looked.astype(jnp.bfloat16)
                into.append(one_hot(keys[message : message + 1] == key_iota))
        total = jnp.dot(
            jnp.concatenate(into, axis=1), looked_ref[t], preferred_element_type=jnp.float32
        )
        summed = total[:, : wide // 2] + total[:, wide // 2 :]
        out_ref[:, t * examples : (t + 1) * examples, :] = summed.reshape(
            group, examples, wide // 2
        )


def bags(ids, near, partner, away, examples):
    group, _, _, lanes = ids.shape
    cores, count, rows, wide = near.shape
    work = 2 * cores * count * group * lanes // 2
    return local_kernel(
        functools.partial(bags_kernel, away=away, examples=examples),
        jax.ShapeDtypeStruct((group, count * examples, wide // 2), jnp.float32),
        (ids, near, partner),
        flops=2 * work * wide * (rows + group * examples),
        vmem=16 << 20,
        scratch=[pltpu.VMEM((count, 2 * cores * group * lanes // 2, wide), jnp.bfloat16)],
    )


def join_kernel(*refs):
    ins, outs = refs[:4], refs[4:]
    for j, out_ref in enumerate(outs):
        out_ref[...] = ins[0][j] + ins[1][j] + ins[2][j] + ins[3][j]


def close_kernel(own_ref, one_ref, two_ref, three_ref, dense_ref, pooled_ref, pairs_ref):
    examples = dense_ref.shape[0]
    pooled = own_ref[...] + one_ref[...] + two_ref[...] + three_ref[...]
    tables = pooled.shape[0] // examples
    vectors = [dense_ref[...]]
    for t in range(tables):
        one = pooled[t * examples : (t + 1) * examples]
        pooled_ref[:, t, :] = one
        vectors.append(one)
    lane = lax.broadcasted_iota(jnp.int32, dense_ref.shape, 1)
    pairs = jnp.zeros(dense_ref.shape, jnp.float32)
    place = 0
    for i in range(tables + 1):
        for j in range(i + 1, tables + 1):
            product = jnp.sum(vectors[i] * vectors[j], axis=1, keepdims=True)
            pairs = jnp.where(lane == place, product, pairs)
            place += 1
    pairs_ref[...] = jnp.swapaxes(pairs, 0, 1)[: pairs_ref.shape[0]]


def body(embedding, tables, dense_features, slot_rows, slot_examples, slot_counts):
    count, rows, width = tables.shape
    examples = dense_features.shape[0]
    capacity = slot_rows.shape[3]
    group, parities, ring, cores = (lax.axis_size(a) for a in ROWS)
    depth = group * parities
    half = count // 2

    other = shifted(tables, "c", 1)
    low = lax.ppermute(tables[:half], Z, [(i, i ^ 1) for i in range(depth)])
    high = lax.ppermute(
        tables[half:], Z, [(i, (i + (1 if i % 2 else -1)) % depth) for i in range(depth)]
    )
    split_ids = (depth, ring, cores * count, capacity)
    ids = local_kernel(
        prepare_kernel,
        jax.ShapeDtypeStruct((group, ring, 2 * cores * count, 2 * capacity), jnp.int32),
        (slot_rows.reshape(split_ids), slot_examples.reshape(split_ids), slot_counts[0].T),
        scratch=[pltpu.VMEM(split_ids, jnp.int32)],
    )
    ids = ids.reshape((group * ring,) + ids.shape[2:])
    ids = lax.all_to_all(ids, ("zq", "x"), 0, 0, tiled=True)
    ids = ids.reshape((group, ring) + ids.shape[1:])
    other_low = shifted(low, "c", 1)
    other_high = shifted(high, "c", 1)
    near = split_tables((tables, other), count, rows, width)
    partner = split_tables((low, high, other_low, other_high), count, rows, width)

    far = bags(ids, near, partner, 2, examples)
    far = shifted(far, "x", 2)
    right = bags(ids, near, partner, 1, examples)
    right = shifted(right, "x", 1)
    left = bags(ids, near, partner, 3, examples)
    left = shifted(left, "x", -1)
    own = bags(ids, near, partner, 0, examples)
    block = jax.ShapeDtypeStruct(own.shape[1:], jnp.float32)
    here, up, over, down = local_kernel(join_kernel, (block,) * group, (own, far, right, left))
    over, up, down = (
        lax.ppermute(piece, Z, [(i, (i + parities * by) % depth) for i in range(depth)])
        for piece, by in ((over, 2), (up, 1), (down, 3))
    )
    pairs = count * (count + 1) // 2
    pooled, products = local_kernel(
        close_kernel,
        (
            jax.ShapeDtypeStruct((examples, count, width), jnp.float32),
            jax.ShapeDtypeStruct((pairs, examples), jnp.float32),
        ),
        (here, over, up, down, dense_features),
    )
    opposite = shifted(products, "y", 2)
    beside = shifted(products, "y", 1) + shifted(products, "y", -1)
    total = ((products + opposite) + beside) * embedding**-0.5
    return pooled, total.T


def solution(mesh):
    torus = Mesh(mesh.devices.reshape(4, 2, 4, 2, mesh.shape["cols"]), ROWS + ("y",))

    def layer(*args):
        return body(512, *args)

    return jax.shard_map(
        layer,
        mesh=torus,
        in_specs=(
            P(None, ROWS, "y"),
            P(ROWS, "y"),
            P(ROWS, None, None, None),
            P(ROWS, None, None, None),
            P(ROWS, None, None),
        ),
        out_specs=(P(ROWS, None, "y"), P(ROWS, None)),
        check_vma=False,
    )
```

```python
import functools

import jax
import jax.numpy as jnp
from jax import lax
from jax.experimental import pallas as pl
from jax.experimental.pallas import tpu as pltpu
from jax.sharding import Mesh
from jax.sharding import PartitionSpec as P


Z = ("zq", "zp")
ROWS = Z + ("x", "c")
DEAD = 1 << 20
VMEM = pl.BlockSpec(memory_space=pltpu.VMEM)
HBM = pl.BlockSpec(memory_space=pltpu.HBM)


def shifted(value, axis, by):
    size = lax.axis_size(axis)
    return lax.ppermute(value, axis, [(i, (i + by) % size) for i in range(size)])


def local_kernel(kernel, out_shape, operands, flops=1 << 20, vmem=12 << 20, scratch=(), in_hbm=()):
    single = not isinstance(out_shape, tuple)
    return pl.pallas_call(
        kernel,
        in_specs=[HBM if k in in_hbm else VMEM for k in range(len(operands))],
        out_specs=VMEM if single else (VMEM,) * len(out_shape),
        out_shape=out_shape,
        scratch_shapes=scratch,
        compiler_params=pltpu.CompilerParams(vmem_limit_bytes=vmem),
        cost_estimate=pl.CostEstimate(flops=flops, bytes_accessed=1 << 20, transcendentals=0),
    )(*operands)


def started(pairs, sems):
    copies = [pltpu.make_async_copy(a, b, sems.at[k]) for k, (a, b) in enumerate(pairs)]
    for copy in copies:
        copy.start()
    return copies


def prepare_kernel(rows_ref, examples_ref, counts_ref, out_ref, live_ref):
    depth, across, under, capacity = rows_ref.shape
    tables, owners = counts_ref.shape
    buckets = owners * tables
    bucket = lax.broadcasted_iota(jnp.int32, (buckets, owners), 0)
    owner = lax.broadcasted_iota(jnp.int32, (buckets, owners), 1)
    spread = jnp.where(bucket // tables == owner, 1.0, 0.0).astype(jnp.bfloat16)
    table = lax.broadcasted_iota(jnp.int32, (buckets, tables), 1)
    own = lax.broadcasted_iota(jnp.int32, (buckets, tables), 0) % tables
    slot = lax.broadcasted_iota(jnp.int32, (buckets, capacity), 1).astype(jnp.float32)
    counts = counts_ref[...].astype(jnp.float32).astype(jnp.bfloat16)
    by_table = lax.dot_general(
        spread, counts, (((1,), (1,)), ((), ())), preferred_element_type=jnp.float32
    )
    count = jnp.sum(jnp.where(table == own, by_table, 0.0), axis=1, keepdims=True)
    live = jnp.where(slot < count, examples_ref[...].reshape(buckets, capacity), DEAD)
    live_ref[...] = live.reshape(live_ref.shape)
    odd = lax.axis_index("zp")
    early = lax.broadcasted_iota(jnp.int32, (across, under, capacity), 1) % tables < tables // 2
    for q in range(depth // 2):
        here = 2 * q + odd
        first = 2 * q + 1 - odd
        second = lax.rem(2 * q + depth - 1 + 3 * odd, depth)
        for ref, lanes in ((rows_ref, slice(0, capacity)), (live_ref, slice(capacity, None))):
            out_ref[q, :, :under, lanes] = ref[here]
            out_ref[q, :, under:, lanes] = jnp.where(early, ref[first], ref[second])


def split_into(out_ref, place, t, full):
    width = full.shape[1]
    high = full.astype(jnp.bfloat16)
    out_ref[place, t, :, :width] = high
    out_ref[place, t, :, width:] = (full - high.astype(jnp.float32)).astype(jnp.bfloat16)


def split_kernel(own_ref, other_ref, out_ref):
    for place, ref in enumerate((own_ref, other_ref)):
        for t in range(ref.shape[0]):
            split_into(out_ref, place, t, ref[t])


def one_hot(mask):
    return jnp.where(mask, 1.0, 0.0).astype(jnp.bfloat16)


def bags_kernel(*refs, away, examples):
    if len(refs) == 11:
        ids_ref, near_ref, *raw, out_ref, partner_ref, looked_ref, full_ref, sems = refs
        half = raw[0].shape[0]
        copies = started(
            [
                (ref, full_ref.at[k // 2, half * (k % 2) : half * (k % 2) + half])
                for k, ref in enumerate(raw)
            ],
            sems,
        )
    else:
        ids_ref, near_ref, partner_ref, out_ref, looked_ref = refs
        copies = []
    group, ring, messages, lanes = ids_ref.shape
    cores, count, rows, wide = near_ref.shape
    slots = lanes // 2
    core = lax.axis_index("c")
    chosen = away[0] + core * (away[1] - away[0])
    column = lax.rem(lax.axis_index("x") + chosen, ring)
    depth = lax.axis_index("zq")
    row_iota = lax.broadcasted_iota(jnp.int32, (slots, rows), 1)
    key_iota = lax.broadcasted_iota(jnp.int32, (group * examples, group * slots), 0)
    ids = [ids_ref[lax.rem(depth + j, group), column] for j in range(group)]
    columns = jnp.swapaxes(jnp.concatenate(ids, axis=0), 0, 1)
    keys = jnp.concatenate([ids[j][:, slots:] + j * examples for j in range(group)], axis=1)

    def look(block, tables_ref, t):
        for o in range(cores):
            message = (block * cores + o) * count + t
            picks = jnp.concatenate(
                [
                    one_hot(
                        columns[:slots, j * messages + message : j * messages + message + 1]
                        == row_iota
                    )
                    for j in range(group)
                ],
                axis=0,
            )
            looked = jnp.dot(picks, tables_ref[o ^ core, t], preferred_element_type=jnp.float32)
            place = (block * cores + o) * group * slots
            looked_ref[t, place : place + group * slots, :] = looked.astype(jnp.bfloat16)

    def pool(t):
        into = [
            one_hot(keys[b * count + t : b * count + t + 1] == key_iota) for b in range(2 * cores)
        ]
        total = jnp.dot(
            jnp.concatenate(into, axis=1), looked_ref[t], preferred_element_type=jnp.float32
        )
        summed = total[:, : wide // 2] + total[:, wide // 2 :]
        out_ref[:, t * examples : (t + 1) * examples, :] = summed.reshape(
            group, examples, wide // 2
        )

    if copies:
        for t in range(count):
            look(0, near_ref, t)
        for copy in copies:
            copy.wait()
        for t in range(count):
            for place in range(cores):
                split_into(partner_ref, place, t, full_ref[place, t])
            look(1, partner_ref, t)
            pool(t)
    else:
        for t in range(count):
            look(0, near_ref, t)
            look(1, partner_ref, t)
            pool(t)


def bags(ids, near, partner, away, examples):
    group, _, _, lanes = ids.shape
    cores, count, rows, wide = near.shape
    work = 2 * cores * count * group * lanes // 2
    out = jax.ShapeDtypeStruct((group, count * examples, wide // 2), jnp.float32)
    scratch = [pltpu.VMEM((count, 2 * cores * group * lanes // 2, wide), jnp.bfloat16)]
    raw = isinstance(partner, tuple)
    if raw:
        out = (out, jax.ShapeDtypeStruct(near.shape, near.dtype))
        scratch += [
            pltpu.VMEM((cores, count, rows, wide // 2), jnp.float32),
            pltpu.SemaphoreType.DMA((len(partner),)),
        ]
    return local_kernel(
        functools.partial(bags_kernel, away=away, examples=examples),
        out,
        (ids, near) + (partner if raw else (partner,)),
        flops=2 * work * wide * (rows + group * examples),
        vmem=16 << 20,
        scratch=scratch,
        in_hbm=range(2, 6) if raw else (),
    )


def by_core(value, by, ring):
    pairs = [
        (2 * i + c, 2 * ((i + by * (1 - 2 * c)) % ring) + c) for i in range(ring) for c in range(2)
    ]
    return lax.ppermute(value, ("x", "c"), pairs)


def add_kernel(one_ref, two_ref, out_ref):
    out_ref[...] = one_ref[...] + two_ref[...]


def join_kernel(*refs):
    ins, outs = refs[:3], refs[3:]
    for j, out_ref in enumerate(outs):
        out_ref[...] = ins[0][j] + ins[1][j] + ins[2][j]


def close_kernel(own_ref, one_ref, two_ref, three_ref, dense_ref, pooled_ref, pairs_ref):
    examples = dense_ref.shape[0]
    pooled = own_ref[...] + one_ref[...] + two_ref[...] + three_ref[...]
    tables = pooled.shape[0] // examples
    vectors = [dense_ref[...]]
    for t in range(tables):
        one = pooled[t * examples : (t + 1) * examples]
        pooled_ref[:, t, :] = one
        vectors.append(one)
    lane = lax.broadcasted_iota(jnp.int32, dense_ref.shape, 1)
    pairs = jnp.zeros(dense_ref.shape, jnp.float32)
    place = 0
    for i in range(tables + 1):
        for j in range(i + 1, tables + 1):
            product = jnp.sum(vectors[i] * vectors[j], axis=1, keepdims=True)
            pairs = jnp.where(lane == place, product, pairs)
            place += 1
    pairs_ref[...] = jnp.swapaxes(pairs, 0, 1)[: pairs_ref.shape[0]]


def body(embedding, tables, dense_features, slot_rows, slot_examples, slot_counts):
    count, _, width = tables.shape
    examples = dense_features.shape[0]
    capacity = slot_rows.shape[3]
    group, parities, ring, cores = (lax.axis_size(a) for a in ROWS)
    depth = group * parities
    half = count // 2

    other = shifted(tables, "c", 1)
    low = lax.ppermute(tables[:half], Z, [(i, i ^ 1) for i in range(depth)])
    high = lax.ppermute(
        tables[half:], Z, [(i, (i + (1 if i % 2 else -1)) % depth) for i in range(depth)]
    )
    split_ids = (depth, ring, cores * count, capacity)
    ids = local_kernel(
        prepare_kernel,
        jax.ShapeDtypeStruct((group, ring, 2 * cores * count, 2 * capacity), jnp.int32),
        (slot_rows.reshape(split_ids), slot_examples.reshape(split_ids), slot_counts[0].T),
        scratch=[pltpu.VMEM(split_ids, jnp.int32)],
    )
    ids = ids.reshape((group * ring,) + ids.shape[2:])
    ids = lax.all_to_all(ids, ("zq", "x"), 0, 0, tiled=True)
    ids = ids.reshape((group, ring) + ids.shape[1:])
    other_low = shifted(low, "c", 1)
    other_high = shifted(high, "c", 1)
    near = local_kernel(
        split_kernel,
        jax.ShapeDtypeStruct((cores,) + tables.shape[:2] + (2 * width,), jnp.bfloat16),
        (tables, other),
    )

    far, partner = bags(ids, near, (low, high, other_low, other_high), (2, 2), examples)
    far = by_core(far, 1, ring)
    soon = bags(ids, near, partner, (3, 1), examples)
    soon = by_core(soon, -1, ring)
    late = bags(ids, near, partner, (1, 3), examples)
    late = local_kernel(add_kernel, jax.ShapeDtypeStruct(late.shape, late.dtype), (late, far))
    late = by_core(late, 1, ring)
    own = bags(ids, near, partner, (0, 0), examples)
    block = jax.ShapeDtypeStruct(own.shape[1:], jnp.float32)
    here, up, over, down = local_kernel(join_kernel, (block,) * group, (own, soon, late))
    over, up, down = (
        lax.ppermute(piece, Z, [(i, (i + parities * by) % depth) for i in range(depth)])
        for piece, by in ((over, 2), (up, 1), (down, 3))
    )
    pairs = count * (count + 1) // 2
    pooled, products = local_kernel(
        close_kernel,
        (
            jax.ShapeDtypeStruct((examples, count, width), jnp.float32),
            jax.ShapeDtypeStruct((pairs, examples), jnp.float32),
        ),
        (here, over, up, down, dense_features),
    )
    opposite = shifted(products, "y", 2)
    beside = shifted(products, "y", 1) + shifted(products, "y", -1)
    total = ((products + opposite) + beside) * embedding**-0.5
    return pooled, total.T


def solution(mesh):
    torus = Mesh(mesh.devices.reshape(4, 2, 4, 2, mesh.shape["cols"]), ROWS + ("y",))

    def layer(*args):
        return body(512, *args)

    return jax.shard_map(
        layer,
        mesh=torus,
        in_specs=(
            P(None, ROWS, "y"),
            P(ROWS, "y"),
            P(ROWS, None, None, None),
            P(ROWS, None, None, None),
            P(ROWS, None, None),
        ),
        out_specs=(P(ROWS, None, "y"), P(ROWS, None)),
        check_vma=False,
    )
```

```python
import functools

import jax
import jax.numpy as jnp
from jax import lax
from jax.experimental import pallas as pl
from jax.experimental.pallas import tpu as pltpu
from jax.sharding import Mesh
from jax.sharding import PartitionSpec as P


Z = ("zq", "zp")
ROWS = Z + ("x", "c")
DEAD = 1 << 20
VMEM = pl.BlockSpec(memory_space=pltpu.VMEM)
HBM = pl.BlockSpec(memory_space=pltpu.HBM)


def shifted(value, axis, by):
    size = lax.axis_size(axis)
    return lax.ppermute(value, axis, [(i, (i + by) % size) for i in range(size)])


def local_kernel(kernel, out_shape, operands, flops=1 << 20, vmem=12 << 20, scratch=(), in_hbm=()):
    single = not isinstance(out_shape, tuple)
    return pl.pallas_call(
        kernel,
        in_specs=[HBM if k in in_hbm else VMEM for k in range(len(operands))],
        out_specs=VMEM if single else (VMEM,) * len(out_shape),
        out_shape=out_shape,
        scratch_shapes=scratch,
        compiler_params=pltpu.CompilerParams(vmem_limit_bytes=vmem),
        cost_estimate=pl.CostEstimate(flops=flops, bytes_accessed=1 << 20, transcendentals=0),
    )(*operands)


def prepare_kernel(
    counts_hbm, examples_hbm, rows_hbm, out_ref, counts_ref, examples_ref, rows_ref, live_ref, sems
):
    copies = [
        pltpu.make_async_copy(source, target, sems.at[k])
        for k, (source, target) in enumerate(
            ((counts_hbm, counts_ref), (examples_hbm, examples_ref), (rows_hbm, rows_ref))
        )
    ]
    for copy in copies:
        copy.start()
    depth, across, under, capacity = rows_ref.shape
    tables, owners = counts_ref.shape
    buckets = owners * tables
    bucket = lax.broadcasted_iota(jnp.int32, (buckets, owners), 0)
    owner = lax.broadcasted_iota(jnp.int32, (buckets, owners), 1)
    spread = jnp.where(bucket // tables == owner, 1.0, 0.0).astype(jnp.bfloat16)
    table = lax.broadcasted_iota(jnp.int32, (buckets, tables), 1)
    own = lax.broadcasted_iota(jnp.int32, (buckets, tables), 0) % tables
    slot = lax.broadcasted_iota(jnp.int32, (buckets, capacity), 1).astype(jnp.float32)
    copies[0].wait()
    counts = counts_ref[...].astype(jnp.float32).astype(jnp.bfloat16)
    by_table = lax.dot_general(
        spread, counts, (((1,), (1,)), ((), ())), preferred_element_type=jnp.float32
    )
    count = jnp.sum(jnp.where(table == own, by_table, 0.0), axis=1, keepdims=True)
    copies[1].wait()
    live = jnp.where(slot < count, examples_ref[...].reshape(buckets, capacity), DEAD)
    live_ref[...] = live.reshape(live_ref.shape)
    copies[2].wait()
    odd = lax.axis_index("zp")
    core = lax.axis_index("c")
    mine = lax.broadcasted_iota(jnp.int32, (across, under, capacity), 1) < tables

    def core_first(value):
        swapped = jnp.concatenate([value[:, tables:], value[:, :tables]], axis=1)
        return jnp.where(core == 0, value, swapped)

    for q in range(depth // 2):
        here = 2 * q + odd
        even_pair = 2 * q + 1 - odd
        odd_pair = lax.rem(2 * q + depth - 1 + 3 * odd, depth)
        first = jnp.where(core == 0, even_pair, odd_pair)
        second = jnp.where(core == 0, odd_pair, even_pair)
        for ref, lanes in ((rows_ref, slice(0, capacity)), (live_ref, slice(capacity, None))):
            out_ref[q, :, :under, lanes] = core_first(ref[here])
            out_ref[q, :, under:, lanes] = core_first(jnp.where(
                mine == (core == 0), ref[first], ref[second]
            ))


def split_into(out_ref, place, full):
    width = full.shape[1]
    high = full.astype(jnp.bfloat16)
    out_ref[place, :, :width] = high
    out_ref[place, :, width:] = (full - high.astype(jnp.float32)).astype(jnp.bfloat16)


def split_kernel(*refs):
    out_ref = refs[-1]
    count = refs[0].shape[0]
    for place, ref in enumerate(refs[:-1]):
        for t in range(count):
            split_into(out_ref, place * count + t, ref[t])


def split_tables(*tables):
    count, rows, width = tables[0].shape
    return local_kernel(
        split_kernel,
        jax.ShapeDtypeStruct((len(tables) * count, rows, 2 * width), jnp.bfloat16),
        tables,
    )


def one_hot(mask):
    return jnp.where(mask, 1.0, 0.0).astype(jnp.bfloat16)


def bags_kernel(*refs, away, examples, count, raw):
    ids_ref, near_ref, part_ref, shared_ref, out_ref, *refs = refs
    if raw:
        full_hbm = shared_ref
        shared_ref, looked_ref, full_ref, sem = refs
        copy = pltpu.make_async_copy(full_hbm, full_ref, sem)
        copy.start()
    else:
        (looked_ref,) = refs
    group, ring, messages, lanes = ids_ref.shape
    rows, wide = near_ref.shape[1:]
    owners = messages // count
    slots = lanes // 2
    core = lax.axis_index("c")
    chosen = away[0] + core * (away[1] - away[0])
    column = lax.rem(lax.axis_index("x") + chosen, ring)
    depth = lax.axis_index("zq")
    row_iota = lax.broadcasted_iota(jnp.int32, (slots, rows), 1)
    key_iota = lax.broadcasted_iota(jnp.int32, (group * examples, group * slots), 0)
    ids = [ids_ref[lax.rem(depth + j, group), column] for j in range(group)]
    columns = jnp.swapaxes(jnp.concatenate(ids, axis=0), 0, 1)
    keys = jnp.concatenate([ids[j][:, slots:] + j * examples for j in range(group)], axis=1)

    def look(o, t):
        ref, place = ((near_ref, t), (near_ref, count + t), (part_ref, t), (shared_ref, t))[o]
        message = o * count + t
        picks = jnp.concatenate(
            [
                one_hot(
                    columns[:slots, j * messages + message : j * messages + message + 1] == row_iota
                )
                for j in range(group)
            ],
            axis=0,
        )
        looked = jnp.dot(picks, ref[place], preferred_element_type=jnp.float32)
        looked_ref[t, o * group * slots : (o + 1) * group * slots, :] = looked.astype(jnp.bfloat16)

    def pool(t):
        into = [one_hot(keys[o * count + t : o * count + t + 1] == key_iota) for o in range(owners)]
        total = jnp.dot(
            jnp.concatenate(into, axis=1), looked_ref[t], preferred_element_type=jnp.float32
        )
        summed = total[:, : wide // 2] + total[:, wide // 2 :]
        out_ref[:, t * examples : (t + 1) * examples, :] = summed.reshape(
            group, examples, wide // 2
        )

    early = owners - 1 if raw else 0
    for t in range(count):
        for o in range(early):
            look(o, t)
    if raw:
        copy.wait()
    for t in range(count):
        if raw:
            split_into(shared_ref, t, full_ref[t])
        for o in range(early, owners):
            look(o, t)
        pool(t)


def bags(ids, near, part, shared, away, examples, raw=False):
    group, _, messages, lanes = ids.shape
    count, rows, wide = part.shape
    work = messages * group * lanes // 2
    out = jax.ShapeDtypeStruct((group, count * examples, wide // 2), jnp.float32)
    scratch = [pltpu.VMEM((count, messages // count * group * lanes // 2, wide), jnp.bfloat16)]
    if raw:
        out = (out, jax.ShapeDtypeStruct(part.shape, part.dtype))
        scratch += [pltpu.VMEM(shared.shape, jnp.float32), pltpu.SemaphoreType.DMA]
    return local_kernel(
        functools.partial(bags_kernel, away=away, examples=examples, count=count, raw=raw),
        out,
        (ids, near, part, shared),
        flops=2 * work * wide * (rows + group * examples),
        vmem=16 << 20,
        scratch=scratch,
        in_hbm=(3,) if raw else (),
    )


def by_core(value, by, ring):
    pairs = [
        (2 * i + c, 2 * ((i + by * (1 - 2 * c)) % ring) + c) for i in range(ring) for c in range(2)
    ]
    return lax.ppermute(value, ("x", "c"), pairs)


def add_kernel(one_ref, two_ref, out_ref):
    out_ref[...] = one_ref[...] + two_ref[...]


def join_kernel(*refs):
    ins, outs = refs[:3], refs[3:]
    for j, out_ref in enumerate(outs):
        out_ref[...] = ins[0][j] + ins[1][j] + ins[2][j]


def close_kernel(own_ref, one_ref, two_ref, three_ref, dense_ref, pooled_ref, pairs_ref):
    examples = dense_ref.shape[0]
    pooled = own_ref[...] + one_ref[...] + two_ref[...] + three_ref[...]
    tables = pooled.shape[0] // examples
    vectors = [dense_ref[...]]
    for t in range(tables):
        one = pooled[t * examples : (t + 1) * examples]
        pooled_ref[:, t, :] = one
        vectors.append(one)
    lane = lax.broadcasted_iota(jnp.int32, dense_ref.shape, 1)
    pairs = jnp.zeros(dense_ref.shape, jnp.float32)
    place = 0
    for i in range(tables + 1):
        for j in range(i + 1, tables + 1):
            product = jnp.sum(vectors[i] * vectors[j], axis=1, keepdims=True)
            pairs = jnp.where(lane == place, product, pairs)
            place += 1
    pairs_ref[...] = jnp.swapaxes(pairs, 0, 1)[: pairs_ref.shape[0]]


def body(embedding, tables, dense_features, slot_rows, slot_examples, slot_counts):
    count, _, width = tables.shape
    examples = dense_features.shape[0]
    capacity = slot_rows.shape[3]
    group, parities, ring, cores = (lax.axis_size(a) for a in ROWS)
    depth = group * parities

    pairs = [
        (2 * i + k, 2 * (i ^ 1 if k == 0 else (i + (1 if i % 2 else -1)) % depth) + k)
        for i in range(depth)
        for k in range(cores)
    ]
    part = lax.ppermute(tables, Z + ("c",), pairs)
    other = shifted(tables, "c", 1)
    split_ids = (depth, ring, cores * count, capacity)
    ids = local_kernel(
        prepare_kernel,
        jax.ShapeDtypeStruct((group, ring, 2 * cores * count, 2 * capacity), jnp.int32),
        (slot_counts[0].T, slot_examples.reshape(split_ids), slot_rows.reshape(split_ids)),
        vmem=67043328,
        scratch=[
            pltpu.VMEM(slot_counts.shape[:0:-1], jnp.int32),
            pltpu.VMEM(split_ids, jnp.int32),
            pltpu.VMEM(split_ids, jnp.int32),
            pltpu.VMEM(split_ids, jnp.int32),
            pltpu.SemaphoreType.DMA((3,)),
        ],
        in_hbm=range(3),
    )
    ids = ids.reshape((group * ring,) + ids.shape[2:])
    ids = lax.all_to_all(ids, ("zq", "x"), 0, 0, tiled=True)
    ids = ids.reshape((group, ring) + ids.shape[1:])
    shared = shifted(part, "c", 1)
    near = split_tables(tables, other)
    part = split_tables(part)

    far, shared = bags(ids, near, part, shared, (2, 2), examples, raw=True)
    far = by_core(far, 1, ring)
    soon = bags(ids, near, part, shared, (3, 1), examples)
    soon = by_core(soon, -1, ring)
    late = bags(ids, near, part, shared, (1, 3), examples)
    late = local_kernel(add_kernel, jax.ShapeDtypeStruct(late.shape, late.dtype), (late, far))
    late = by_core(late, 1, ring)
    own = bags(ids, near, part, shared, (0, 0), examples)
    block = jax.ShapeDtypeStruct(own.shape[1:], jnp.float32)
    here, up, over, down = local_kernel(join_kernel, (block,) * group, (own, soon, late))
    over, up, down = (
        lax.ppermute(piece, Z, [(i, (i + parities * by) % depth) for i in range(depth)])
        for piece, by in ((over, 2), (up, 1), (down, 3))
    )
    pairs = count * (count + 1) // 2
    pooled, products = local_kernel(
        close_kernel,
        (
            jax.ShapeDtypeStruct((examples, count, width), jnp.float32),
            jax.ShapeDtypeStruct((pairs, examples), jnp.float32),
        ),
        (here, over, up, down, dense_features),
    )
    opposite = shifted(products, "y", 2)
    beside = shifted(products, "y", 1) + shifted(products, "y", -1)
    total = ((products + opposite) + beside) * embedding**-0.5
    return pooled, total.T


def solution(mesh):
    torus = Mesh(mesh.devices.reshape(4, 2, 4, 2, mesh.shape["cols"]), ROWS + ("y",))

    def layer(*args):
        return body(512, *args)

    return jax.shard_map(
        layer,
        mesh=torus,
        in_specs=(
            P(None, ROWS, "y"),
            P(ROWS, "y"),
            P(ROWS, None, None, None),
            P(ROWS, None, None, None),
            P(ROWS, None, None),
        ),
        out_specs=(P(ROWS, None, "y"), P(ROWS, None)),
        check_vma=False,
    )
```

```python
import functools

import jax
import jax.numpy as jnp
from jax import lax
from jax.experimental import pallas as pl
from jax.experimental.pallas import tpu as pltpu
from jax.sharding import Mesh
from jax.sharding import PartitionSpec as P


Z = ("zq", "zp")
ROWS = Z + ("x", "c")
DEAD = 1 << 20
VMEM = pl.BlockSpec(memory_space=pltpu.VMEM)
HBM = pl.BlockSpec(memory_space=pltpu.HBM)


def shifted(value, axis, by):
    size = lax.axis_size(axis)
    return lax.ppermute(value, axis, [(i, (i + by) % size) for i in range(size)])


def local_kernel(kernel, out_shape, operands, flops=1 << 20, vmem=12 << 20, scratch=(), in_hbm=()):
    single = not isinstance(out_shape, tuple)
    return pl.pallas_call(
        kernel,
        in_specs=[HBM if k in in_hbm else VMEM for k in range(len(operands))],
        out_specs=VMEM if single else (VMEM,) * len(out_shape),
        out_shape=out_shape,
        scratch_shapes=scratch,
        compiler_params=pltpu.CompilerParams(vmem_limit_bytes=vmem),
        cost_estimate=pl.CostEstimate(flops=flops, bytes_accessed=1 << 20, transcendentals=0),
    )(*operands)


def prepare_kernel(
    counts_hbm, examples_hbm, rows_hbm, out_ref, counts_ref, examples_ref, rows_ref, live_ref, sems
):
    copies = [
        pltpu.make_async_copy(source, target, sems.at[k])
        for k, (source, target) in enumerate(
            ((counts_hbm, counts_ref), (examples_hbm, examples_ref), (rows_hbm, rows_ref))
        )
    ]
    for copy in copies:
        copy.start()
    depth, across, under, capacity = rows_ref.shape
    tables, owners = counts_ref.shape
    buckets = owners * tables
    bucket = lax.broadcasted_iota(jnp.int32, (buckets, owners), 0)
    owner = lax.broadcasted_iota(jnp.int32, (buckets, owners), 1)
    spread = jnp.where(bucket // tables == owner, 1.0, 0.0).astype(jnp.bfloat16)
    table = lax.broadcasted_iota(jnp.int32, (buckets, tables), 1)
    own = lax.broadcasted_iota(jnp.int32, (buckets, tables), 0) % tables
    slot = lax.broadcasted_iota(jnp.int32, (buckets, capacity), 1).astype(jnp.float32)
    copies[0].wait()
    counts = counts_ref[...].astype(jnp.float32).astype(jnp.bfloat16)
    by_table = lax.dot_general(
        spread, counts, (((1,), (1,)), ((), ())), preferred_element_type=jnp.float32
    )
    count = jnp.sum(jnp.where(table == own, by_table, 0.0), axis=1, keepdims=True)
    copies[1].wait()
    live = jnp.where(slot < count, examples_ref[...].reshape(buckets, capacity), DEAD)
    live_ref[...] = live.reshape(live_ref.shape)
    copies[2].wait()
    odd = lax.axis_index("zp")
    core = lax.axis_index("c")
    mine = lax.broadcasted_iota(jnp.int32, (across, under, capacity), 1) < tables

    def core_first(value):
        swapped = jnp.concatenate([value[:, tables:], value[:, :tables]], axis=1)
        return jnp.where(core == 0, value, swapped)

    for q in range(depth // 2):
        here = 2 * q + odd
        even_pair = 2 * q + 1 - odd
        odd_pair = lax.rem(2 * q + depth - 1 + 3 * odd, depth)
        first = jnp.where(core == 0, even_pair, odd_pair)
        second = jnp.where(core == 0, odd_pair, even_pair)
        for ref, lanes in ((rows_ref, slice(0, capacity)), (live_ref, slice(capacity, None))):
            out_ref[q, :, :under, lanes] = core_first(ref[here])
            out_ref[q, :, under:, lanes] = core_first(jnp.where(
                mine == (core == 0), ref[first], ref[second]
            ))


def split_into(out_ref, place, full):
    width = full.shape[1]
    high = full.astype(jnp.bfloat16)
    out_ref[place, :, :width] = high
    out_ref[place, :, width:] = (full - high.astype(jnp.float32)).astype(jnp.bfloat16)


def split_kernel(*refs):
    out_ref = refs[-1]
    count = refs[0].shape[0]
    for place, ref in enumerate(refs[:-1]):
        for t in range(count):
            split_into(out_ref, place * count + t, ref[t])


def split_tables(*tables):
    count, rows, width = tables[0].shape
    return local_kernel(
        split_kernel,
        jax.ShapeDtypeStruct((len(tables) * count, rows, 2 * width), jnp.bfloat16),
        tables,
    )


def one_hot(mask):
    return jnp.where(mask, 1.0, 0.0).astype(jnp.bfloat16)


def bags_kernel(*refs, away, examples, count, raw):
    if raw:
        ids_ref, near_ref, part_hbm, shared_ref, out_ref, moved_ref, looked_ref, full_ref, sems = refs
        copies = [
            pltpu.make_async_copy(part_hbm.at[t], full_ref.at[t], sems.at[t]) for t in range(count)
        ]
        for copy in copies:
            copy.start()
    else:
        ids_ref, near_ref, moved_ref, out_ref, looked_ref = refs
    group, ring, messages, lanes = ids_ref.shape
    rows, wide = near_ref.shape[1:]
    owners = messages // count
    slots = lanes // 2
    core = lax.axis_index("c")
    chosen = away[0] + core * (away[1] - away[0])
    column = lax.rem(lax.axis_index("x") + chosen, ring)
    depth = lax.axis_index("zq")
    row_iota = lax.broadcasted_iota(jnp.int32, (slots, rows), 1)
    key_iota = lax.broadcasted_iota(jnp.int32, (group * examples, group * slots), 0)
    ids = [ids_ref[lax.rem(depth + j, group), column] for j in range(group)]
    columns = jnp.swapaxes(jnp.concatenate(ids, axis=0), 0, 1)
    keys = jnp.concatenate([ids[j][:, slots:] + j * examples for j in range(group)], axis=1)

    def look(o, t):
        ref, place = (near_ref, moved_ref)[o // 2], o % 2 * count + t
        if raw and o == 2:
            copies[t].wait()
            split_into(ref, place, full_ref[t])
        if raw and o == 3:
            split_into(ref, place, shared_ref[t])
        message = o * count + t
        picks = jnp.concatenate(
            [
                one_hot(
                    columns[:slots, j * messages + message : j * messages + message + 1] == row_iota
                )
                for j in range(group)
            ],
            axis=0,
        )
        looked = jnp.dot(picks, ref[place], preferred_element_type=jnp.float32)
        looked_ref[t, o * group * slots : (o + 1) * group * slots, :] = looked.astype(jnp.bfloat16)

    def pool(t):
        into = [one_hot(keys[o * count + t : o * count + t + 1] == key_iota) for o in range(owners)]
        total = jnp.dot(
            jnp.concatenate(into, axis=1), looked_ref[t], preferred_element_type=jnp.float32
        )
        summed = total[:, : wide // 2] + total[:, wide // 2 :]
        out_ref[:, t * examples : (t + 1) * examples, :] = summed.reshape(
            group, examples, wide // 2
        )

    if raw:
        for o in (0, 1, 3):
            for t in range(count):
                look(o, t)
    for t in range(count):
        for o in (2,) if raw else range(owners):
            look(o, t)
        pool(t)


def bags(ids, near, moved, away, examples, raw=False):
    group, _, messages, lanes = ids.shape
    rows, wide = near.shape[1:]
    count = near.shape[0] // 2
    work = messages * group * lanes // 2
    out = jax.ShapeDtypeStruct((group, count * examples, wide // 2), jnp.float32)
    scratch = [pltpu.VMEM((count, messages // count * group * lanes // 2, wide), jnp.bfloat16)]
    if raw:
        out = (out, jax.ShapeDtypeStruct(near.shape, near.dtype))
        scratch += [
            pltpu.VMEM((count, rows, wide // 2), jnp.float32),
            pltpu.SemaphoreType.DMA((count,)),
        ]
    return local_kernel(
        functools.partial(bags_kernel, away=away, examples=examples, count=count, raw=raw),
        out,
        (ids, near) + (moved if raw else (moved,)),
        flops=2 * work * wide * (rows + group * examples),
        vmem=16 << 20,
        scratch=scratch,
        in_hbm=(2,) if raw else (),
    )


def by_core(value, by, ring):
    pairs = [
        (2 * i + c, 2 * ((i + by * (1 - 2 * c)) % ring) + c) for i in range(ring) for c in range(2)
    ]
    return lax.ppermute(value, ("x", "c"), pairs)


def add_kernel(one_ref, two_ref, out_ref):
    out_ref[...] = one_ref[...] + two_ref[...]


def join_kernel(*refs):
    ins, outs = refs[:3], refs[3:]
    for j, out_ref in enumerate(outs):
        out_ref[...] = ins[0][j] + ins[1][j] + ins[2][j]


def close_kernel(own_ref, one_ref, two_ref, three_ref, dense_ref, pooled_ref, pairs_ref):
    examples = dense_ref.shape[0]
    pooled = own_ref[...] + one_ref[...] + two_ref[...] + three_ref[...]
    tables = pooled.shape[0] // examples
    vectors = [dense_ref[...]]
    for t in range(tables):
        one = pooled[t * examples : (t + 1) * examples]
        pooled_ref[:, t, :] = one
        vectors.append(one)
    lane = lax.broadcasted_iota(jnp.int32, dense_ref.shape, 1)
    pairs = jnp.zeros(dense_ref.shape, jnp.float32)
    place = 0
    for i in range(tables + 1):
        for j in range(i + 1, tables + 1):
            product = jnp.sum(vectors[i] * vectors[j], axis=1, keepdims=True)
            pairs = jnp.where(lane == place, product, pairs)
            place += 1
    pairs_ref[...] = jnp.swapaxes(pairs, 0, 1)[: pairs_ref.shape[0]]


def body(embedding, tables, dense_features, slot_rows, slot_examples, slot_counts):
    count, _, width = tables.shape
    examples = dense_features.shape[0]
    capacity = slot_rows.shape[3]
    group, parities, ring, cores = (lax.axis_size(a) for a in ROWS)
    depth = group * parities

    pairs = [
        (2 * i + k, 2 * (i ^ 1 if k == 0 else (i + (1 if i % 2 else -1)) % depth) + k)
        for i in range(depth)
        for k in range(cores)
    ]
    part = lax.ppermute(tables, Z + ("c",), pairs)
    other = shifted(tables, "c", 1)
    split_ids = (depth, ring, cores * count, capacity)
    ids = local_kernel(
        prepare_kernel,
        jax.ShapeDtypeStruct((group, ring, 2 * cores * count, 2 * capacity), jnp.int32),
        (slot_counts[0].T, slot_examples.reshape(split_ids), slot_rows.reshape(split_ids)),
        vmem=67043328,
        scratch=[
            pltpu.VMEM(slot_counts.shape[:0:-1], jnp.int32),
            pltpu.VMEM(split_ids, jnp.int32),
            pltpu.VMEM(split_ids, jnp.int32),
            pltpu.VMEM(split_ids, jnp.int32),
            pltpu.SemaphoreType.DMA((3,)),
        ],
        in_hbm=range(3),
    )
    ids = ids.reshape((group * ring,) + ids.shape[2:])
    ids = lax.all_to_all(ids, ("zq", "x"), 0, 0, tiled=True)
    ids = ids.reshape((group, ring) + ids.shape[1:])
    shared = shifted(part, "c", 1)
    near = split_tables(tables, other)
    far, moved = bags(ids, near, (part, shared), (2, 2), examples, raw=True)
    far = by_core(far, 1, ring)
    soon = bags(ids, near, moved, (3, 1), examples)
    soon = by_core(soon, -1, ring)
    late = bags(ids, near, moved, (1, 3), examples)
    late = local_kernel(add_kernel, jax.ShapeDtypeStruct(late.shape, late.dtype), (late, far))
    late = by_core(late, 1, ring)
    own = bags(ids, near, moved, (0, 0), examples)
    block = jax.ShapeDtypeStruct(own.shape[1:], jnp.float32)
    here, up, over, down = local_kernel(join_kernel, (block,) * group, (own, soon, late))
    over, up, down = (
        lax.ppermute(piece, Z, [(i, (i + parities * by) % depth) for i in range(depth)])
        for piece, by in ((over, 2), (up, 1), (down, 3))
    )
    pairs = count * (count + 1) // 2
    pooled, products = local_kernel(
        close_kernel,
        (
            jax.ShapeDtypeStruct((examples, count, width), jnp.float32),
            jax.ShapeDtypeStruct((pairs, examples), jnp.float32),
        ),
        (here, over, up, down, dense_features),
    )
    opposite = shifted(products, "y", 2)
    after = shifted(products, "y", 1)
    before = shifted(products, "y", -1)
    total = ((products + opposite) + (after + before)) * embedding**-0.5
    return pooled, total.T


def solution(mesh):
    torus = Mesh(mesh.devices.reshape(4, 2, 4, 2, mesh.shape["cols"]), ROWS + ("y",))

    def layer(*args):
        return body(512, *args)

    return jax.shard_map(
        layer,
        mesh=torus,
        in_specs=(
            P(None, ROWS, "y"),
            P(ROWS, "y"),
            P(ROWS, None, None, None),
            P(ROWS, None, None, None),
            P(ROWS, None, None),
        ),
        out_specs=(P(ROWS, None, "y"), P(ROWS, None)),
        check_vma=False,
    )
```

```python
import functools

import jax
import jax.numpy as jnp
from jax import lax
from jax.experimental import pallas as pl
from jax.experimental.pallas import tpu as pltpu
from jax.sharding import Mesh
from jax.sharding import PartitionSpec as P


Z = ("zq", "zp")
ROWS = Z + ("x", "c")
DEAD = 1 << 20
VMEM = pl.BlockSpec(memory_space=pltpu.VMEM)
HBM = pl.BlockSpec(memory_space=pltpu.HBM)


def shifted(value, axis, by):
    size = lax.axis_size(axis)
    return lax.ppermute(value, axis, [(i, (i + by) % size) for i in range(size)])


def local_kernel(kernel, out_shape, operands, flops=1 << 20, vmem=12 << 20, scratch=(), in_hbm=()):
    single = not isinstance(out_shape, tuple)
    return pl.pallas_call(
        kernel,
        in_specs=[HBM if k in in_hbm else VMEM for k in range(len(operands))],
        out_specs=VMEM if single else (VMEM,) * len(out_shape),
        out_shape=out_shape,
        scratch_shapes=scratch,
        compiler_params=pltpu.CompilerParams(vmem_limit_bytes=vmem),
        cost_estimate=pl.CostEstimate(flops=flops, bytes_accessed=1 << 20, transcendentals=0),
    )(*operands)


def prepare_kernel(
    counts_hbm, examples_hbm, rows_hbm, out_ref, counts_ref, examples_ref, rows_ref, live_ref, sems
):
    copies = [
        pltpu.make_async_copy(source, target, sems.at[k])
        for k, (source, target) in enumerate(
            ((counts_hbm, counts_ref), (examples_hbm, examples_ref), (rows_hbm, rows_ref))
        )
    ]
    for copy in copies:
        copy.start()
    depth, across, under, capacity = rows_ref.shape
    tables, owners = counts_ref.shape
    buckets = owners * tables
    bucket = lax.broadcasted_iota(jnp.int32, (buckets, owners), 0)
    owner = lax.broadcasted_iota(jnp.int32, (buckets, owners), 1)
    spread = jnp.where(bucket // tables == owner, 1.0, 0.0).astype(jnp.bfloat16)
    table = lax.broadcasted_iota(jnp.int32, (buckets, tables), 1)
    own = lax.broadcasted_iota(jnp.int32, (buckets, tables), 0) % tables
    slot = lax.broadcasted_iota(jnp.int32, (buckets, capacity), 1).astype(jnp.float32)
    copies[0].wait()
    counts = counts_ref[...].astype(jnp.float32).astype(jnp.bfloat16)
    by_table = lax.dot_general(
        spread, counts, (((1,), (1,)), ((), ())), preferred_element_type=jnp.float32
    )
    count = jnp.sum(jnp.where(table == own, by_table, 0.0), axis=1, keepdims=True)
    copies[1].wait()
    live = jnp.where(slot < count, examples_ref[...].reshape(buckets, capacity), DEAD)
    live_ref[...] = live.reshape(live_ref.shape)
    copies[2].wait()
    odd = lax.axis_index("zp")
    core = lax.axis_index("c")
    mine = lax.broadcasted_iota(jnp.int32, (across, under, capacity), 1) < tables

    def core_first(value):
        swapped = jnp.concatenate([value[:, tables:], value[:, :tables]], axis=1)
        return jnp.where(core == 0, value, swapped)

    for q in range(depth // 2):
        here = 2 * q + odd
        even_pair = 2 * q + 1 - odd
        odd_pair = lax.rem(2 * q + depth - 1 + 3 * odd, depth)
        first = jnp.where(core == 0, even_pair, odd_pair)
        second = jnp.where(core == 0, odd_pair, even_pair)
        for ref, lanes in ((rows_ref, slice(0, capacity)), (live_ref, slice(capacity, None))):
            out_ref[q, :, :under, lanes] = core_first(ref[here])
            out_ref[q, :, under:, lanes] = core_first(jnp.where(
                mine == (core == 0), ref[first], ref[second]
            ))


def split_into(out_ref, place, full):
    width = full.shape[1]
    high = full.astype(jnp.bfloat16)
    out_ref[place, :, :width] = high
    out_ref[place, :, width:] = (full - high.astype(jnp.float32)).astype(jnp.bfloat16)


def split_kernel(*refs):
    out_ref = refs[-1]
    count = refs[0].shape[0]
    for place, ref in enumerate(refs[:-1]):
        for t in range(count):
            split_into(out_ref, place * count + t, ref[t])


def split_tables(*tables):
    count, rows, width = tables[0].shape
    return local_kernel(
        split_kernel,
        jax.ShapeDtypeStruct((len(tables) * count, rows, 2 * width), jnp.bfloat16),
        tables,
    )


def one_hot(mask):
    return jnp.where(mask, 1.0, 0.0).astype(jnp.bfloat16)


def bags_kernel(*refs, away, examples, count, raw):
    ids_ref, near_ref, part_ref, shared_ref, out_ref, *refs = refs
    if raw:
        shared_hbm = shared_ref
        shared_ref, looked_ref, full_ref, sems = refs
        copies = [
            pltpu.make_async_copy(shared_hbm.at[t], full_ref.at[t], sems.at[t])
            for t in range(count)
        ]
        for copy in copies:
            copy.start()
    else:
        (looked_ref,) = refs
    group, ring, messages, lanes = ids_ref.shape
    rows, wide = near_ref.shape[1:]
    owners = messages // count
    slots = lanes // 2
    core = lax.axis_index("c")
    chosen = away[0] + core * (away[1] - away[0])
    column = lax.rem(lax.axis_index("x") + chosen, ring)
    depth = lax.axis_index("zq")
    row_iota = lax.broadcasted_iota(jnp.int32, (slots, rows), 1)
    key_iota = lax.broadcasted_iota(jnp.int32, (group * examples, group * slots), 0)
    ids = [ids_ref[lax.rem(depth + j, group), column] for j in range(group)]
    columns = jnp.swapaxes(jnp.concatenate(ids, axis=0), 0, 1)
    keys = jnp.concatenate([ids[j][:, slots:] + j * examples for j in range(group)], axis=1)

    def look(o, t):
        ref, place = ((near_ref, t), (near_ref, count + t), (part_ref, t), (shared_ref, t))[o]
        if raw and o == owners - 1:
            copies[t].wait()
            split_into(ref, t, full_ref[t])
        message = o * count + t
        picks = jnp.concatenate(
            [
                one_hot(
                    columns[:slots, j * messages + message : j * messages + message + 1] == row_iota
                )
                for j in range(group)
            ],
            axis=0,
        )
        looked = jnp.dot(picks, ref[place], preferred_element_type=jnp.float32)
        looked_ref[t, o * group * slots : (o + 1) * group * slots, :] = looked.astype(jnp.bfloat16)

    def pool(t):
        into = [one_hot(keys[o * count + t : o * count + t + 1] == key_iota) for o in range(owners)]
        total = jnp.dot(
            jnp.concatenate(into, axis=1), looked_ref[t], preferred_element_type=jnp.float32
        )
        summed = total[:, : wide // 2] + total[:, wide // 2 :]
        out_ref[:, t * examples : (t + 1) * examples, :] = summed.reshape(
            group, examples, wide // 2
        )

    early = owners - 1 if raw else 0
    for o in range(early):
        for t in range(count):
            look(o, t)
    for t in range(count):
        for o in range(early, owners):
            look(o, t)
        pool(t)


def bags(ids, near, part, shared, away, examples, raw=False):
    group, _, messages, lanes = ids.shape
    count, rows, wide = part.shape
    work = messages * group * lanes // 2
    out = jax.ShapeDtypeStruct((group, count * examples, wide // 2), jnp.float32)
    scratch = [pltpu.VMEM((count, messages // count * group * lanes // 2, wide), jnp.bfloat16)]
    if raw:
        out = (out, jax.ShapeDtypeStruct(part.shape, part.dtype))
        scratch += [pltpu.VMEM(shared.shape, jnp.float32), pltpu.SemaphoreType.DMA((count,))]
    return local_kernel(
        functools.partial(bags_kernel, away=away, examples=examples, count=count, raw=raw),
        out,
        (ids, near, part, shared),
        flops=2 * work * wide * (rows + group * examples),
        vmem=16 << 20,
        scratch=scratch,
        in_hbm=(3,) if raw else (),
    )


def by_core(value, by, ring):
    pairs = [
        (2 * i + c, 2 * ((i + by * (1 - 2 * c)) % ring) + c) for i in range(ring) for c in range(2)
    ]
    return lax.ppermute(value, ("x", "c"), pairs)


def add_kernel(one_ref, two_ref, out_ref):
    out_ref[...] = one_ref[...] + two_ref[...]


def join_kernel(*refs):
    ins, outs = refs[:3], refs[3:]
    for j, out_ref in enumerate(outs):
        out_ref[...] = ins[0][j] + ins[1][j] + ins[2][j]


def close_kernel(own_ref, one_ref, two_ref, three_ref, dense_ref, pooled_ref, pairs_ref):
    examples = dense_ref.shape[0]
    pooled = own_ref[...] + one_ref[...] + two_ref[...] + three_ref[...]
    tables = pooled.shape[0] // examples
    vectors = [dense_ref[...]]
    for t in range(tables):
        one = pooled[t * examples : (t + 1) * examples]
        pooled_ref[:, t, :] = one
        vectors.append(one)
    lane = lax.broadcasted_iota(jnp.int32, dense_ref.shape, 1)
    pairs = jnp.zeros(dense_ref.shape, jnp.float32)
    place = 0
    for i in range(tables + 1):
        for j in range(i + 1, tables + 1):
            product = jnp.sum(vectors[i] * vectors[j], axis=1, keepdims=True)
            pairs = jnp.where(lane == place, product, pairs)
            place += 1
    pairs_ref[...] = jnp.swapaxes(pairs, 0, 1)[: pairs_ref.shape[0]]


def body(embedding, tables, dense_features, slot_rows, slot_examples, slot_counts):
    count, _, width = tables.shape
    examples = dense_features.shape[0]
    capacity = slot_rows.shape[3]
    group, parities, ring, cores = (lax.axis_size(a) for a in ROWS)
    depth = group * parities

    pairs = [
        (2 * i + k, 2 * (i ^ 1 if k == 0 else (i + (1 if i % 2 else -1)) % depth) + k)
        for i in range(depth)
        for k in range(cores)
    ]
    part = lax.ppermute(tables, Z + ("c",), pairs)
    other = shifted(tables, "c", 1)
    split_ids = (depth, ring, cores * count, capacity)
    ids = local_kernel(
        prepare_kernel,
        jax.ShapeDtypeStruct((group, ring, 2 * cores * count, 2 * capacity), jnp.int32),
        (slot_counts[0].T, slot_examples.reshape(split_ids), slot_rows.reshape(split_ids)),
        vmem=67043328,
        scratch=[
            pltpu.VMEM(slot_counts.shape[:0:-1], jnp.int32),
            pltpu.VMEM(split_ids, jnp.int32),
            pltpu.VMEM(split_ids, jnp.int32),
            pltpu.VMEM(split_ids, jnp.int32),
            pltpu.SemaphoreType.DMA((3,)),
        ],
        in_hbm=range(3),
    )
    ids = ids.reshape((group * ring,) + ids.shape[2:])
    ids = lax.all_to_all(ids, ("zq", "x"), 0, 0, tiled=True)
    ids = ids.reshape((group, ring) + ids.shape[1:])
    shared = shifted(part, "c", 1)
    near = split_tables(tables, other)
    part = split_tables(part)

    far, shared = bags(ids, near, part, shared, (2, 2), examples, raw=True)
    far = by_core(far, 1, ring)
    soon = bags(ids, near, part, shared, (3, 1), examples)
    soon = by_core(soon, -1, ring)
    late = bags(ids, near, part, shared, (1, 3), examples)
    late = local_kernel(add_kernel, jax.ShapeDtypeStruct(late.shape, late.dtype), (late, far))
    late = by_core(late, 1, ring)
    own = bags(ids, near, part, shared, (0, 0), examples)
    block = jax.ShapeDtypeStruct(own.shape[1:], jnp.float32)
    here, up, over, down = local_kernel(join_kernel, (block,) * group, (own, soon, late))
    over, up, down = (
        lax.ppermute(piece, Z, [(i, (i + parities * by) % depth) for i in range(depth)])
        for piece, by in ((over, 2), (up, 1), (down, 3))
    )
    pairs = count * (count + 1) // 2
    pooled, products = local_kernel(
        close_kernel,
        (
            jax.ShapeDtypeStruct((examples, count, width), jnp.float32),
            jax.ShapeDtypeStruct((pairs, examples), jnp.float32),
        ),
        (here, over, up, down, dense_features),
    )
    opposite = shifted(products, "y", 2)
    after = shifted(products, "y", 1)
    before = shifted(products, "y", -1)
    total = ((products + opposite) + (after + before)) * embedding**-0.5
    return pooled, total.T


def solution(mesh):
    torus = Mesh(mesh.devices.reshape(4, 2, 4, 2, mesh.shape["cols"]), ROWS + ("y",))

    def layer(*args):
        return body(512, *args)

    return jax.shard_map(
        layer,
        mesh=torus,
        in_specs=(
            P(None, ROWS, "y"),
            P(ROWS, "y"),
            P(ROWS, None, None, None),
            P(ROWS, None, None, None),
            P(ROWS, None, None),
        ),
        out_specs=(P(ROWS, None, "y"), P(ROWS, None)),
        check_vma=False,
    )
```

```python
import functools

import jax
import jax.numpy as jnp
from jax import lax
from jax.experimental import pallas as pl
from jax.experimental.pallas import tpu as pltpu
from jax.sharding import Mesh
from jax.sharding import PartitionSpec as P


Z = ("zq", "zp")
ROWS = Z + ("x", "c")
DEAD = 1 << 20
VMEM = pl.BlockSpec(memory_space=pltpu.VMEM)
HBM = pl.BlockSpec(memory_space=pltpu.HBM)


def shifted(value, axis, by):
    size = lax.axis_size(axis)
    return lax.ppermute(value, axis, [(i, (i + by) % size) for i in range(size)])


def local_kernel(kernel, out_shape, operands, flops=1 << 20, vmem=12 << 20, scratch=(), in_hbm=()):
    single = not isinstance(out_shape, tuple)
    return pl.pallas_call(
        kernel,
        in_specs=[HBM if k in in_hbm else VMEM for k in range(len(operands))],
        out_specs=VMEM if single else (VMEM,) * len(out_shape),
        out_shape=out_shape,
        scratch_shapes=scratch,
        compiler_params=pltpu.CompilerParams(vmem_limit_bytes=vmem),
        cost_estimate=pl.CostEstimate(flops=flops, bytes_accessed=1 << 20, transcendentals=0),
    )(*operands)


def prepare_kernel(
    counts_hbm, examples_hbm, rows_hbm, out_ref, counts_ref, examples_ref, rows_ref, live_ref, sems
):
    copies = [
        pltpu.make_async_copy(source, target, sems.at[k])
        for k, (source, target) in enumerate(
            ((counts_hbm, counts_ref), (examples_hbm, examples_ref), (rows_hbm, rows_ref))
        )
    ]
    for copy in copies:
        copy.start()
    depth, across, under, capacity = rows_ref.shape
    tables, owners = counts_ref.shape
    buckets = owners * tables
    bucket = lax.broadcasted_iota(jnp.int32, (buckets, owners), 0)
    owner = lax.broadcasted_iota(jnp.int32, (buckets, owners), 1)
    spread = jnp.where(bucket // tables == owner, 1.0, 0.0).astype(jnp.bfloat16)
    table = lax.broadcasted_iota(jnp.int32, (buckets, tables), 1)
    own = lax.broadcasted_iota(jnp.int32, (buckets, tables), 0) % tables
    slot = lax.broadcasted_iota(jnp.int32, (buckets, capacity), 1).astype(jnp.float32)
    copies[0].wait()
    counts = counts_ref[...].astype(jnp.float32).astype(jnp.bfloat16)
    by_table = lax.dot_general(
        spread, counts, (((1,), (1,)), ((), ())), preferred_element_type=jnp.float32
    )
    count = jnp.sum(jnp.where(table == own, by_table, 0.0), axis=1, keepdims=True)
    copies[1].wait()
    live = jnp.where(slot < count, examples_ref[...].reshape(buckets, capacity), DEAD)
    live_ref[...] = live.reshape(live_ref.shape)
    copies[2].wait()
    odd = lax.axis_index("zp")
    core = lax.axis_index("c")
    mine = lax.broadcasted_iota(jnp.int32, (across, under, capacity), 1) < tables

    def core_first(value):
        swapped = jnp.concatenate([value[:, tables:], value[:, :tables]], axis=1)
        return jnp.where(core == 0, value, swapped)

    for q in range(depth // 2):
        here = 2 * q + odd
        even_pair = 2 * q + 1 - odd
        odd_pair = lax.rem(2 * q + depth - 1 + 3 * odd, depth)
        first = jnp.where(core == 0, even_pair, odd_pair)
        second = jnp.where(core == 0, odd_pair, even_pair)
        for ref, lanes in ((rows_ref, slice(0, capacity)), (live_ref, slice(capacity, None))):
            out_ref[q, :, :under, lanes] = core_first(ref[here])
            out_ref[q, :, under:, lanes] = core_first(jnp.where(
                mine == (core == 0), ref[first], ref[second]
            ))


def split_into(out_ref, place, full):
    width = full.shape[1]
    high = full.astype(jnp.bfloat16)
    out_ref[place, :, :width] = high
    out_ref[place, :, width:] = (full - high.astype(jnp.float32)).astype(jnp.bfloat16)


def split_kernel(*refs):
    out_ref = refs[-1]
    count = refs[0].shape[0]
    for place, ref in enumerate(refs[:-1]):
        for t in range(count):
            split_into(out_ref, place * count + t, ref[t])


def split_tables(*tables):
    count, rows, width = tables[0].shape
    return local_kernel(
        split_kernel,
        jax.ShapeDtypeStruct((len(tables) * count, rows, 2 * width), jnp.bfloat16),
        tables,
    )


def one_hot(mask):
    return jnp.where(mask, 1.0, 0.0).astype(jnp.bfloat16)


def bags_kernel(*refs, away, examples, count, raw):
    ids_ref, near_ref, part_ref, shared_ref, out_ref, *refs = refs
    if raw:
        shared_hbm = shared_ref
        shared_ref, looked_ref, full_ref, sem = refs
        copy = pltpu.make_async_copy(shared_hbm, full_ref, sem)
        copy.start()
    else:
        (looked_ref,) = refs
    group, ring, messages, lanes = ids_ref.shape
    rows, wide = near_ref.shape[1:]
    owners = messages // count
    slots = lanes // 2
    core = lax.axis_index("c")
    chosen = away[0] + core * (away[1] - away[0])
    column = lax.rem(lax.axis_index("x") + chosen, ring)
    depth = lax.axis_index("zq")
    row_iota = lax.broadcasted_iota(jnp.int32, (slots, rows), 1)
    key_iota = lax.broadcasted_iota(jnp.int32, (group * examples, group * slots), 0)
    ids = [ids_ref[lax.rem(depth + j, group), column] for j in range(group)]
    columns = jnp.swapaxes(jnp.concatenate(ids, axis=0), 0, 1)
    keys = jnp.concatenate([ids[j][:, slots:] + j * examples for j in range(group)], axis=1)

    def look(o, t):
        ref, place = ((near_ref, t), (near_ref, count + t), (part_ref, t), (shared_ref, t))[o]
        message = o * count + t
        picks = jnp.concatenate(
            [
                one_hot(
                    columns[:slots, j * messages + message : j * messages + message + 1] == row_iota
                )
                for j in range(group)
            ],
            axis=0,
        )
        looked = jnp.dot(picks, ref[place], preferred_element_type=jnp.float32)
        looked_ref[t, o * group * slots : (o + 1) * group * slots, :] = looked.astype(jnp.bfloat16)

    def pool(t):
        into = [one_hot(keys[o * count + t : o * count + t + 1] == key_iota) for o in range(owners)]
        total = jnp.dot(
            jnp.concatenate(into, axis=1), looked_ref[t], preferred_element_type=jnp.float32
        )
        summed = total[:, : wide // 2] + total[:, wide // 2 :]
        out_ref[:, t * examples : (t + 1) * examples, :] = summed.reshape(
            group, examples, wide // 2
        )

    early = owners - 1 if raw else 0
    for t in range(count):
        for o in range(early):
            look(o, t)
    if raw:
        copy.wait()
    for t in range(count):
        if raw:
            split_into(shared_ref, t, full_ref[t])
        for o in range(early, owners):
            look(o, t)
        pool(t)


def bags(ids, near, part, shared, away, examples, raw=False):
    group, _, messages, lanes = ids.shape
    count, rows, wide = part.shape
    work = messages * group * lanes // 2
    out = jax.ShapeDtypeStruct((group, count * examples, wide // 2), jnp.float32)
    scratch = [pltpu.VMEM((count, messages // count * group * lanes // 2, wide), jnp.bfloat16)]
    if raw:
        out = (out, jax.ShapeDtypeStruct(part.shape, part.dtype))
        scratch += [pltpu.VMEM(shared.shape, jnp.float32), pltpu.SemaphoreType.DMA]
    return local_kernel(
        functools.partial(bags_kernel, away=away, examples=examples, count=count, raw=raw),
        out,
        (ids, near, part, shared),
        flops=2 * work * wide * (rows + group * examples),
        vmem=16 << 20,
        scratch=scratch,
        in_hbm=(3,) if raw else (),
    )


def by_core(value, by, ring):
    pairs = [
        (2 * i + c, 2 * ((i + by * (1 - 2 * c)) % ring) + c) for i in range(ring) for c in range(2)
    ]
    return lax.ppermute(value, ("x", "c"), pairs)


def add_kernel(one_ref, two_ref, out_ref):
    out_ref[...] = one_ref[...] + two_ref[...]


def join_kernel(*refs):
    ins, outs = refs[:3], refs[3:]
    for j, out_ref in enumerate(outs):
        out_ref[...] = ins[0][j] + ins[1][j] + ins[2][j]


def pairs_kernel(own_ref, one_ref, two_ref, three_ref, dense_ref, pairs_ref, summed_ref):
    examples = dense_ref.shape[0]
    pooled = own_ref[...] + one_ref[...] + two_ref[...] + three_ref[...]
    summed_ref[...] = pooled
    tables = pooled.shape[0] // examples
    vectors = [dense_ref[...]]
    for t in range(tables):
        vectors.append(pooled[t * examples : (t + 1) * examples])
    lane = lax.broadcasted_iota(jnp.int32, dense_ref.shape, 1)
    pairs = jnp.zeros(dense_ref.shape, jnp.float32)
    place = 0
    for i in range(tables + 1):
        for j in range(i + 1, tables + 1):
            product = jnp.sum(vectors[i] * vectors[j], axis=1, keepdims=True)
            pairs = jnp.where(lane == place, product, pairs)
            place += 1
    pairs_ref[...] = jnp.swapaxes(pairs, 0, 1)[: pairs_ref.shape[0]]


def pooled_kernel(summed_ref, pooled_ref):
    examples, tables = pooled_ref.shape[:2]
    for t in range(tables):
        pooled_ref[:, t, :] = summed_ref[t * examples : (t + 1) * examples]


def body(embedding, tables, dense_features, slot_rows, slot_examples, slot_counts):
    count, _, width = tables.shape
    examples = dense_features.shape[0]
    capacity = slot_rows.shape[3]
    group, parities, ring, cores = (lax.axis_size(a) for a in ROWS)
    depth = group * parities

    pairs = [
        (2 * i + k, 2 * (i ^ 1 if k == 0 else (i + (1 if i % 2 else -1)) % depth) + k)
        for i in range(depth)
        for k in range(cores)
    ]
    part = lax.ppermute(tables, Z + ("c",), pairs)
    other = shifted(tables, "c", 1)
    split_ids = (depth, ring, cores * count, capacity)
    ids = local_kernel(
        prepare_kernel,
        jax.ShapeDtypeStruct((group, ring, 2 * cores * count, 2 * capacity), jnp.int32),
        (slot_counts[0].T, slot_examples.reshape(split_ids), slot_rows.reshape(split_ids)),
        vmem=67043328,
        scratch=[
            pltpu.VMEM(slot_counts.shape[:0:-1], jnp.int32),
            pltpu.VMEM(split_ids, jnp.int32),
            pltpu.VMEM(split_ids, jnp.int32),
            pltpu.VMEM(split_ids, jnp.int32),
            pltpu.SemaphoreType.DMA((3,)),
        ],
        in_hbm=range(3),
    )
    ids = ids.reshape((group * ring,) + ids.shape[2:])
    ids = lax.all_to_all(ids, ("zq", "x"), 0, 0, tiled=True)
    ids = ids.reshape((group, ring) + ids.shape[1:])
    shared = shifted(part, "c", 1)
    near = split_tables(tables, other)
    part = split_tables(part)

    far, shared = bags(ids, near, part, shared, (2, 2), examples, raw=True)
    far = by_core(far, 1, ring)
    soon = bags(ids, near, part, shared, (3, 1), examples)
    soon = by_core(soon, -1, ring)
    late = bags(ids, near, part, shared, (1, 3), examples)
    late = local_kernel(add_kernel, jax.ShapeDtypeStruct(late.shape, late.dtype), (late, far))
    late = by_core(late, 1, ring)
    own = bags(ids, near, part, shared, (0, 0), examples)
    block = jax.ShapeDtypeStruct(own.shape[1:], jnp.float32)
    here, up, over, down = local_kernel(join_kernel, (block,) * group, (own, soon, late))
    over, up, down = (
        lax.ppermute(piece, Z, [(i, (i + parities * by) % depth) for i in range(depth)])
        for piece, by in ((over, 2), (up, 1), (down, 3))
    )
    pairs = count * (count + 1) // 2
    products, summed = local_kernel(
        pairs_kernel,
        (
            jax.ShapeDtypeStruct((pairs, examples), jnp.float32),
            jax.ShapeDtypeStruct((count * examples, width), jnp.float32),
        ),
        (here, over, up, down, dense_features),
    )
    pooled = local_kernel(
        pooled_kernel,
        jax.ShapeDtypeStruct((examples, count, width), jnp.float32),
        (summed,),
    )
    opposite = shifted(products, "y", 2)
    after = shifted(products, "y", 1)
    before = shifted(products, "y", -1)
    total = ((products + opposite) + (after + before)) * embedding**-0.5
    return pooled, total.T


def solution(mesh):
    torus = Mesh(mesh.devices.reshape(4, 2, 4, 2, mesh.shape["cols"]), ROWS + ("y",))

    def layer(*args):
        return body(512, *args)

    return jax.shard_map(
        layer,
        mesh=torus,
        in_specs=(
            P(None, ROWS, "y"),
            P(ROWS, "y"),
            P(ROWS, None, None, None),
            P(ROWS, None, None, None),
            P(ROWS, None, None),
        ),
        out_specs=(P(ROWS, None, "y"), P(ROWS, None)),
        check_vma=False,
    )
```

```python
import functools

import jax
import jax.numpy as jnp
from jax import lax
from jax.experimental import pallas as pl
from jax.experimental.pallas import tpu as pltpu
from jax.sharding import Mesh
from jax.sharding import PartitionSpec as P


Z = ("zq", "zp")
ROWS = Z + ("x", "c")
DEAD = 1 << 20
VMEM = pl.BlockSpec(memory_space=pltpu.VMEM)
HBM = pl.BlockSpec(memory_space=pltpu.HBM)


def shifted(value, axis, by):
    size = lax.axis_size(axis)
    return lax.ppermute(value, axis, [(i, (i + by) % size) for i in range(size)])


def local_kernel(kernel, out_shape, operands, flops=1 << 20, vmem=12 << 20, scratch=(), in_hbm=()):
    single = not isinstance(out_shape, tuple)
    return pl.pallas_call(
        kernel,
        in_specs=[HBM if k in in_hbm else VMEM for k in range(len(operands))],
        out_specs=VMEM if single else (VMEM,) * len(out_shape),
        out_shape=out_shape,
        scratch_shapes=scratch,
        compiler_params=pltpu.CompilerParams(vmem_limit_bytes=vmem),
        cost_estimate=pl.CostEstimate(flops=flops, bytes_accessed=1 << 20, transcendentals=0),
    )(*operands)


def prepare_kernel(
    counts_hbm, examples_hbm, rows_hbm, out_ref, counts_ref, examples_ref, rows_ref, live_ref, sems
):
    copies = [
        pltpu.make_async_copy(source, target, sems.at[k])
        for k, (source, target) in enumerate(
            ((counts_hbm, counts_ref), (examples_hbm, examples_ref), (rows_hbm, rows_ref))
        )
    ]
    for copy in copies:
        copy.start()
    depth, across, under, capacity = rows_ref.shape
    tables, owners = counts_ref.shape
    buckets = owners * tables
    bucket = lax.broadcasted_iota(jnp.int32, (buckets, owners), 0)
    owner = lax.broadcasted_iota(jnp.int32, (buckets, owners), 1)
    spread = jnp.where(bucket // tables == owner, 1.0, 0.0).astype(jnp.bfloat16)
    table = lax.broadcasted_iota(jnp.int32, (buckets, tables), 1)
    own = lax.broadcasted_iota(jnp.int32, (buckets, tables), 0) % tables
    slot = lax.broadcasted_iota(jnp.int32, (buckets, capacity), 1).astype(jnp.float32)
    copies[0].wait()
    counts = counts_ref[...].astype(jnp.float32).astype(jnp.bfloat16)
    by_table = lax.dot_general(
        spread, counts, (((1,), (1,)), ((), ())), preferred_element_type=jnp.float32
    )
    count = jnp.sum(jnp.where(table == own, by_table, 0.0), axis=1, keepdims=True)
    copies[1].wait()
    live = jnp.where(slot < count, examples_ref[...].reshape(buckets, capacity), DEAD)
    live_ref[...] = live.reshape(live_ref.shape)
    copies[2].wait()
    odd = lax.axis_index("zp")
    core = lax.axis_index("c")
    mine = lax.broadcasted_iota(jnp.int32, (across, under, capacity), 1) < tables

    def core_first(value):
        swapped = jnp.concatenate([value[:, tables:], value[:, :tables]], axis=1)
        return jnp.where(core == 0, value, swapped)

    for q in range(depth // 2):
        here = 2 * q + odd
        even_pair = 2 * q + 1 - odd
        odd_pair = lax.rem(2 * q + depth - 1 + 3 * odd, depth)
        first = jnp.where(core == 0, even_pair, odd_pair)
        second = jnp.where(core == 0, odd_pair, even_pair)
        for ref, lanes in ((rows_ref, slice(0, capacity)), (live_ref, slice(capacity, None))):
            out_ref[q, :, :under, lanes] = core_first(ref[here])
            out_ref[q, :, under:, lanes] = core_first(jnp.where(
                mine == (core == 0), ref[first], ref[second]
            ))


def split_into(out_ref, place, full):
    width = full.shape[1]
    high = full.astype(jnp.bfloat16)
    out_ref[place, :, :width] = high
    out_ref[place, :, width:] = (full - high.astype(jnp.float32)).astype(jnp.bfloat16)


def split_kernel(*refs):
    out_ref = refs[-1]
    count = refs[0].shape[0]
    for place, ref in enumerate(refs[:-1]):
        for t in range(count):
            split_into(out_ref, place * count + t, ref[t])


def split_tables(*tables):
    count, rows, width = tables[0].shape
    return local_kernel(
        split_kernel,
        jax.ShapeDtypeStruct((len(tables) * count, rows, 2 * width), jnp.bfloat16),
        tables,
    )


def one_hot(mask):
    return jnp.where(mask, 1.0, 0.0).astype(jnp.bfloat16)


def bags_kernel(*refs, away, examples, count, parts, raw):
    ids_ref, near_ref, part_ref, shared_ref, *refs = refs
    out_refs, refs = refs[: len(parts)], refs[len(parts) :]
    if raw:
        shared_hbm = shared_ref
        shared_ref, looked_ref, full_ref, sems = refs
        half = count // 2
        copies = [
            pltpu.make_async_copy(
                shared_hbm.at[k * half : (k + 1) * half],
                full_ref.at[k * half : (k + 1) * half],
                sems.at[k],
            )
            for k in range(2)
        ]
        for copy in copies:
            copy.start()
    else:
        (looked_ref,) = refs
    group, ring, messages, lanes = ids_ref.shape
    rows, wide = near_ref.shape[1:]
    owners = messages // count
    slots = lanes // 2
    core = lax.axis_index("c")
    chosen = away[0] + core * (away[1] - away[0])
    column = lax.rem(lax.axis_index("x") + chosen, ring)
    depth = lax.axis_index("zq")
    row_iota = lax.broadcasted_iota(jnp.int32, (slots, rows), 1)
    key_iota = lax.broadcasted_iota(jnp.int32, (group * examples, group * slots), 0)
    ids = [ids_ref[lax.rem(depth + j, group), column] for j in range(group)]
    columns = jnp.swapaxes(jnp.concatenate(ids, axis=0), 0, 1)
    keys = jnp.concatenate([ids[j][:, slots:] + j * examples for j in range(group)], axis=1)

    def look(o, t):
        ref, place = ((near_ref, t), (near_ref, count + t), (part_ref, t), (shared_ref, t))[o]
        message = o * count + t
        picks = jnp.concatenate(
            [
                one_hot(
                    columns[:slots, j * messages + message : j * messages + message + 1] == row_iota
                )
                for j in range(group)
            ],
            axis=0,
        )
        looked = jnp.dot(picks, ref[place], preferred_element_type=jnp.float32)
        looked_ref[t, o * group * slots : (o + 1) * group * slots, :] = looked.astype(jnp.bfloat16)

    def pool(t, out_ref, place):
        into = [one_hot(keys[o * count + t : o * count + t + 1] == key_iota) for o in range(owners)]
        total = jnp.dot(
            jnp.concatenate(into, axis=1), looked_ref[t], preferred_element_type=jnp.float32
        )
        summed = total[:, : wide // 2] + total[:, wide // 2 :]
        out_ref[:, place * examples : (place + 1) * examples, :] = summed.reshape(
            group, examples, wide // 2
        )

    early = owners - 1 if raw else 0
    for tables in parts:
        for t in tables:
            for o in range(early):
                look(o, t)
    for k, (tables, out_ref) in enumerate(zip(parts, out_refs)):
        if raw:
            copies[k].wait()
        for place, t in enumerate(tables):
            if raw:
                split_into(shared_ref, t, full_ref[t])
            for o in range(early, owners):
                look(o, t)
            pool(t, out_ref, place)
    if raw:
        copies[1].wait()
        for t in range(half, count):
            split_into(shared_ref, t, full_ref[t])


def bags(ids, near, part, shared, away, examples, parts, raw=False):
    group, _, messages, lanes = ids.shape
    count, rows, wide = part.shape
    tasks = sum(len(tables) for tables in parts)
    work = messages // count * tasks * group * lanes // 2
    out = tuple(
        jax.ShapeDtypeStruct((group, len(tables) * examples, wide // 2), jnp.float32)
        for tables in parts
    )
    scratch = [pltpu.VMEM((count, messages // count * group * lanes // 2, wide), jnp.bfloat16)]
    if raw:
        out += (jax.ShapeDtypeStruct(part.shape, part.dtype),)
        scratch += [pltpu.VMEM(shared.shape, jnp.float32), pltpu.SemaphoreType.DMA((2,))]
    return local_kernel(
        functools.partial(
            bags_kernel, away=away, examples=examples, count=count, parts=parts, raw=raw
        ),
        out,
        (ids, near, part, shared),
        flops=2 * work * wide * (rows + group * examples),
        vmem=16 << 20,
        scratch=scratch,
        in_hbm=(3,) if raw else (),
    )


def by_core(value, by, ring):
    pairs = [
        (2 * i + c, 2 * ((i + by * (1 - 2 * c)) % ring) + c) for i in range(ring) for c in range(2)
    ]
    return lax.ppermute(value, ("x", "c"), pairs)


def add_kernel(one_ref, two_ref, out_ref):
    out_ref[...] = one_ref[...] + two_ref[...]


def join_kernel(own_ref, soon_ref, low_ref, high_ref, *out_refs):
    half = low_ref.shape[1]
    for j, out_ref in enumerate(out_refs):
        out_ref[:half] = own_ref[j, :half] + soon_ref[j, :half] + low_ref[j]
        out_ref[half:] = own_ref[j, half:] + soon_ref[j, half:] + high_ref[j]


def pairs_kernel(own_ref, one_ref, two_ref, three_ref, dense_ref, pairs_ref, summed_ref):
    examples = dense_ref.shape[0]
    pooled = own_ref[...] + one_ref[...] + two_ref[...] + three_ref[...]
    summed_ref[...] = pooled
    tables = pooled.shape[0] // examples
    vectors = [dense_ref[...]]
    for t in range(tables):
        vectors.append(pooled[t * examples : (t + 1) * examples])
    lane = lax.broadcasted_iota(jnp.int32, dense_ref.shape, 1)
    pairs = jnp.zeros(dense_ref.shape, jnp.float32)
    place = 0
    for i in range(tables + 1):
        for j in range(i + 1, tables + 1):
            product = jnp.sum(vectors[i] * vectors[j], axis=1, keepdims=True)
            pairs = jnp.where(lane == place, product, pairs)
            place += 1
    pairs_ref[...] = jnp.swapaxes(pairs, 0, 1)[: pairs_ref.shape[0]]


def pooled_kernel(summed_ref, pooled_ref):
    examples, tables = pooled_ref.shape[:2]
    for t in range(tables):
        pooled_ref[:, t, :] = summed_ref[t * examples : (t + 1) * examples]


def body(embedding, tables, dense_features, slot_rows, slot_examples, slot_counts):
    count, _, width = tables.shape
    examples = dense_features.shape[0]
    capacity = slot_rows.shape[3]
    group, parities, ring, cores = (lax.axis_size(a) for a in ROWS)
    depth = group * parities

    pairs = [
        (2 * i + k, 2 * (i ^ 1 if k == 0 else (i + (1 if i % 2 else -1)) % depth) + k)
        for i in range(depth)
        for k in range(cores)
    ]
    part = lax.ppermute(tables, Z + ("c",), pairs)
    other = shifted(tables, "c", 1)
    split_ids = (depth, ring, cores * count, capacity)
    ids = local_kernel(
        prepare_kernel,
        jax.ShapeDtypeStruct((group, ring, 2 * cores * count, 2 * capacity), jnp.int32),
        (slot_counts[0].T, slot_examples.reshape(split_ids), slot_rows.reshape(split_ids)),
        vmem=67043328,
        scratch=[
            pltpu.VMEM(slot_counts.shape[:0:-1], jnp.int32),
            pltpu.VMEM(split_ids, jnp.int32),
            pltpu.VMEM(split_ids, jnp.int32),
            pltpu.VMEM(split_ids, jnp.int32),
            pltpu.SemaphoreType.DMA((3,)),
        ],
        in_hbm=range(3),
    )
    ids = ids.reshape((group * ring,) + ids.shape[2:])
    ids = lax.all_to_all(ids, ("zq", "x"), 0, 0, tiled=True)
    ids = ids.reshape((group, ring) + ids.shape[1:])
    shared = shifted(part, "c", 1)
    near = split_tables(tables, other)
    part = split_tables(part)

    low, high = tuple(range(count // 2)), tuple(range(count // 2, count))
    whole = (low + high,)

    far_low, shared = bags(ids, near, part, shared, (2, 2), examples, (low,), raw=True)
    far_low = by_core(far_low, 1, ring)
    (far_high,) = bags(ids, near, part, shared, (2, 2), examples, (high,))
    far_high = by_core(far_high, 1, ring)
    (soon,) = bags(ids, near, part, shared, (3, 1), examples, whole)
    soon = by_core(soon, -1, ring)
    late_low, late_high = bags(ids, near, part, shared, (1, 3), examples, (low, high))
    piece = jax.ShapeDtypeStruct(late_low.shape, late_low.dtype)
    late_low = local_kernel(add_kernel, piece, (late_low, far_low))
    late_low = by_core(late_low, 1, ring)
    late_high = local_kernel(add_kernel, piece, (late_high, far_high))
    late_high = by_core(late_high, 1, ring)
    (own,) = bags(ids, near, part, shared, (0, 0), examples, whole)
    block = jax.ShapeDtypeStruct(own.shape[1:], jnp.float32)
    here, up, over, down = local_kernel(
        join_kernel, (block,) * group, (own, soon, late_low, late_high)
    )
    over, up, down = (
        lax.ppermute(piece, Z, [(i, (i + parities * by) % depth) for i in range(depth)])
        for piece, by in ((over, 2), (up, 1), (down, 3))
    )
    pairs = count * (count + 1) // 2
    products, summed = local_kernel(
        pairs_kernel,
        (
            jax.ShapeDtypeStruct((pairs, examples), jnp.float32),
            jax.ShapeDtypeStruct((count * examples, width), jnp.float32),
        ),
        (here, over, up, down, dense_features),
    )
    pooled = local_kernel(
        pooled_kernel,
        jax.ShapeDtypeStruct((examples, count, width), jnp.float32),
        (summed,),
    )
    opposite = shifted(products, "y", 2)
    after = shifted(products, "y", 1)
    before = shifted(products, "y", -1)
    total = ((products + opposite) + (after + before)) * embedding**-0.5
    return pooled, total.T


def solution(mesh):
    torus = Mesh(mesh.devices.reshape(4, 2, 4, 2, mesh.shape["cols"]), ROWS + ("y",))

    def layer(*args):
        return body(512, *args)

    return jax.shard_map(
        layer,
        mesh=torus,
        in_specs=(
            P(None, ROWS, "y"),
            P(ROWS, "y"),
            P(ROWS, None, None, None),
            P(ROWS, None, None, None),
            P(ROWS, None, None),
        ),
        out_specs=(P(ROWS, None, "y"), P(ROWS, None)),
        check_vma=False,
    )
```

```python
import functools

import jax
import jax.numpy as jnp
from jax import lax
from jax.experimental import pallas as pl
from jax.experimental.pallas import tpu as pltpu
from jax.sharding import Mesh
from jax.sharding import PartitionSpec as P


Z = ("zq", "zp")
ROWS = Z + ("x", "c")
DEAD = 1 << 20
VMEM = pl.BlockSpec(memory_space=pltpu.VMEM)
HBM = pl.BlockSpec(memory_space=pltpu.HBM)


def shifted(value, axis, by):
    size = lax.axis_size(axis)
    return lax.ppermute(value, axis, [(i, (i + by) % size) for i in range(size)])


def local_kernel(kernel, out_shape, operands, flops=1 << 20, vmem=12 << 20, scratch=(), in_hbm=()):
    single = not isinstance(out_shape, tuple)
    return pl.pallas_call(
        kernel,
        in_specs=[HBM if k in in_hbm else VMEM for k in range(len(operands))],
        out_specs=VMEM if single else (VMEM,) * len(out_shape),
        out_shape=out_shape,
        scratch_shapes=scratch,
        compiler_params=pltpu.CompilerParams(vmem_limit_bytes=vmem),
        cost_estimate=pl.CostEstimate(flops=flops, bytes_accessed=1 << 20, transcendentals=0),
    )(*operands)


def prepare_kernel(
    counts_hbm, examples_hbm, rows_hbm, out_ref, counts_ref, examples_ref, rows_ref, live_ref, sems
):
    copies = [
        pltpu.make_async_copy(source, target, sems.at[k])
        for k, (source, target) in enumerate(
            ((counts_hbm, counts_ref), (examples_hbm, examples_ref), (rows_hbm, rows_ref))
        )
    ]
    for copy in copies:
        copy.start()
    depth, across, under, capacity = rows_ref.shape
    tables, owners = counts_ref.shape
    buckets = owners * tables
    bucket = lax.broadcasted_iota(jnp.int32, (buckets, owners), 0)
    owner = lax.broadcasted_iota(jnp.int32, (buckets, owners), 1)
    spread = jnp.where(bucket // tables == owner, 1.0, 0.0).astype(jnp.bfloat16)
    table = lax.broadcasted_iota(jnp.int32, (buckets, tables), 1)
    own = lax.broadcasted_iota(jnp.int32, (buckets, tables), 0) % tables
    slot = lax.broadcasted_iota(jnp.int32, (buckets, capacity), 1).astype(jnp.float32)
    copies[0].wait()
    counts = counts_ref[...].astype(jnp.float32).astype(jnp.bfloat16)
    by_table = lax.dot_general(
        spread, counts, (((1,), (1,)), ((), ())), preferred_element_type=jnp.float32
    )
    count = jnp.sum(jnp.where(table == own, by_table, 0.0), axis=1, keepdims=True)
    copies[1].wait()
    live = jnp.where(slot < count, examples_ref[...].reshape(buckets, capacity), DEAD)
    live_ref[...] = live.reshape(live_ref.shape)
    copies[2].wait()
    odd = lax.axis_index("zp")
    core = lax.axis_index("c")
    mine = lax.broadcasted_iota(jnp.int32, (across, under, capacity), 1) < tables

    def core_first(value):
        swapped = jnp.concatenate([value[:, tables:], value[:, :tables]], axis=1)
        return jnp.where(core == 0, value, swapped)

    for q in range(depth // 2):
        here = 2 * q + odd
        even_pair = 2 * q + 1 - odd
        odd_pair = lax.rem(2 * q + depth - 1 + 3 * odd, depth)
        first = jnp.where(core == 0, even_pair, odd_pair)
        second = jnp.where(core == 0, odd_pair, even_pair)
        for ref, lanes in ((rows_ref, slice(0, capacity)), (live_ref, slice(capacity, None))):
            out_ref[q, :, :under, lanes] = core_first(ref[here])
            out_ref[q, :, under:, lanes] = core_first(jnp.where(
                mine == (core == 0), ref[first], ref[second]
            ))


def split_into(out_ref, place, full):
    width = full.shape[1]
    high = full.astype(jnp.bfloat16)
    out_ref[place, :, :width] = high
    out_ref[place, :, width:] = (full - high.astype(jnp.float32)).astype(jnp.bfloat16)


def split_kernel(*refs):
    out_ref = refs[-1]
    count = refs[0].shape[0]
    for place, ref in enumerate(refs[:-1]):
        for t in range(count):
            split_into(out_ref, place * count + t, ref[t])


def split_tables(*tables):
    count, rows, width = tables[0].shape
    return local_kernel(
        split_kernel,
        jax.ShapeDtypeStruct((len(tables) * count, rows, 2 * width), jnp.bfloat16),
        tables,
    )


def one_hot(mask):
    return jnp.where(mask, 1.0, 0.0).astype(jnp.bfloat16)


def bags_kernel(*refs, examples, count, parts, raw):
    ids_ref, near_ref, part_ref, shared_ref, *refs = refs
    out_refs, refs = refs[: len(parts)], refs[len(parts) :]
    if raw:
        shared_hbm = shared_ref
        shared_ref, looked_ref, full_ref, sems = refs
        half = count // 2
        copies = [
            pltpu.make_async_copy(
                shared_hbm.at[k * half : (k + 1) * half],
                full_ref.at[k * half : (k + 1) * half],
                sems.at[k],
            )
            for k in range(2)
        ]
        for copy in copies:
            copy.start()
    else:
        (looked_ref,) = refs
    group, ring, messages, lanes = ids_ref.shape
    rows, wide = near_ref.shape[1:]
    owners = messages // count
    slots = lanes // 2
    core = lax.axis_index("c")
    aways = tuple(dict.fromkeys(away for away, _ in parts))
    depth = lax.axis_index("zq")
    row_iota = lax.broadcasted_iota(jnp.int32, (slots, rows), 1)
    key_iota = lax.broadcasted_iota(jnp.int32, (group * examples, group * slots), 0)
    columns, keys = [], []
    for away in aways:
        chosen = away[0] + core * (away[1] - away[0])
        column = lax.rem(lax.axis_index("x") + chosen, ring)
        ids = [ids_ref[lax.rem(depth + j, group), column] for j in range(group)]
        columns.append(jnp.swapaxes(jnp.concatenate(ids, axis=0), 0, 1))
        keys.append(
            jnp.concatenate([ids[j][:, slots:] + j * examples for j in range(group)], axis=1)
        )
    block = group * slots

    def look(o, t):
        ref, place = ((near_ref, t), (near_ref, count + t), (part_ref, t), (shared_ref, t))[o]
        message = o * count + t
        picks = jnp.concatenate(
            [
                one_hot(
                    one[:slots, j * messages + message : j * messages + message + 1] == row_iota
                )
                for one in columns
                for j in range(group)
            ],
            axis=0,
        )
        looked = jnp.dot(picks, ref[place], preferred_element_type=jnp.float32)
        for k in range(len(aways)):
            looked_ref[k, t, o * block : (o + 1) * block, :] = looked[
                k * block : (k + 1) * block
            ].astype(jnp.bfloat16)

    def pool(k, t, out_ref, place):
        into = [
            one_hot(keys[k][o * count + t : o * count + t + 1] == key_iota) for o in range(owners)
        ]
        total = jnp.dot(
            jnp.concatenate(into, axis=1), looked_ref[k, t], preferred_element_type=jnp.float32
        )
        summed = total[:, : wide // 2] + total[:, wide // 2 :]
        out_ref[:, place * examples : (place + 1) * examples, :] = summed.reshape(
            group, examples, wide // 2
        )

    early = owners - 1 if raw else 0
    tables = tuple(dict.fromkeys(t for _, chosen in parts for t in chosen))
    for t in tables:
        for o in range(early):
            look(o, t)
    if raw:
        copies[0].wait()
    for t in tables:
        if raw:
            split_into(shared_ref, t, full_ref[t])
        for o in range(early, owners):
            look(o, t)
        for (away, chosen), out_ref in zip(parts, out_refs):
            if t in chosen:
                pool(aways.index(away), t, out_ref, chosen.index(t))
    if raw:
        copies[1].wait()
        for t in range(half, count):
            split_into(shared_ref, t, full_ref[t])


def bags(ids, near, part, shared, examples, parts, raw=False):
    group, _, messages, lanes = ids.shape
    count, rows, wide = part.shape
    tasks = sum(len(tables) for _, tables in parts)
    work = messages // count * tasks * group * lanes // 2
    out = tuple(
        jax.ShapeDtypeStruct((group, len(tables) * examples, wide // 2), jnp.float32)
        for _, tables in parts
    )
    chunks = len(set(away for away, _ in parts))
    scratch = [
        pltpu.VMEM((chunks, count, messages // count * group * lanes // 2, wide), jnp.bfloat16)
    ]
    if raw:
        out += (jax.ShapeDtypeStruct(part.shape, part.dtype),)
        scratch += [pltpu.VMEM(shared.shape, jnp.float32), pltpu.SemaphoreType.DMA((2,))]
    return local_kernel(
        functools.partial(bags_kernel, examples=examples, count=count, parts=parts, raw=raw),
        out,
        (ids, near, part, shared),
        flops=2 * work * wide * (rows + group * examples),
        vmem=20 << 20,
        scratch=scratch,
        in_hbm=(3,) if raw else (),
    )


def by_core(value, by, ring):
    pairs = [
        (2 * i + c, 2 * ((i + by * (1 - 2 * c)) % ring) + c) for i in range(ring) for c in range(2)
    ]
    return lax.ppermute(value, ("x", "c"), pairs)


def add_kernel(one_ref, two_ref, out_ref):
    out_ref[...] = one_ref[...] + two_ref[...]


def join_kernel(own_ref, soon_ref, low_ref, high_ref, *out_refs):
    half = low_ref.shape[1]
    for j, out_ref in enumerate(out_refs):
        out_ref[:half] = own_ref[j, :half] + soon_ref[j, :half] + low_ref[j]
        out_ref[half:] = own_ref[j, half:] + soon_ref[j, half:] + high_ref[j]


def pairs_kernel(own_ref, one_ref, two_ref, three_ref, dense_ref, pairs_ref, summed_ref):
    examples = dense_ref.shape[0]
    pooled = own_ref[...] + one_ref[...] + two_ref[...] + three_ref[...]
    summed_ref[...] = pooled
    tables = pooled.shape[0] // examples
    vectors = [dense_ref[...]]
    for t in range(tables):
        vectors.append(pooled[t * examples : (t + 1) * examples])
    lane = lax.broadcasted_iota(jnp.int32, dense_ref.shape, 1)
    pairs = jnp.zeros(dense_ref.shape, jnp.float32)
    place = 0
    for i in range(tables + 1):
        for j in range(i + 1, tables + 1):
            product = jnp.sum(vectors[i] * vectors[j], axis=1, keepdims=True)
            pairs = jnp.where(lane == place, product, pairs)
            place += 1
    pairs_ref[...] = jnp.swapaxes(pairs, 0, 1)[: pairs_ref.shape[0]]


def pooled_kernel(summed_ref, pooled_ref):
    examples, tables = pooled_ref.shape[:2]
    for t in range(tables):
        pooled_ref[:, t, :] = summed_ref[t * examples : (t + 1) * examples]


def body(embedding, tables, dense_features, slot_rows, slot_examples, slot_counts):
    count, _, width = tables.shape
    examples = dense_features.shape[0]
    capacity = slot_rows.shape[3]
    group, parities, ring, cores = (lax.axis_size(a) for a in ROWS)
    depth = group * parities

    pairs = [
        (2 * i + k, 2 * (i ^ 1 if k == 0 else (i + (1 if i % 2 else -1)) % depth) + k)
        for i in range(depth)
        for k in range(cores)
    ]
    part = lax.ppermute(tables, Z + ("c",), pairs)
    other = shifted(tables, "c", 1)
    split_ids = (depth, ring, cores * count, capacity)
    ids = local_kernel(
        prepare_kernel,
        jax.ShapeDtypeStruct((group, ring, 2 * cores * count, 2 * capacity), jnp.int32),
        (slot_counts[0].T, slot_examples.reshape(split_ids), slot_rows.reshape(split_ids)),
        vmem=67043328,
        scratch=[
            pltpu.VMEM(slot_counts.shape[:0:-1], jnp.int32),
            pltpu.VMEM(split_ids, jnp.int32),
            pltpu.VMEM(split_ids, jnp.int32),
            pltpu.VMEM(split_ids, jnp.int32),
            pltpu.SemaphoreType.DMA((3,)),
        ],
        in_hbm=range(3),
    )
    ids = ids.reshape((group * ring,) + ids.shape[2:])
    ids = lax.all_to_all(ids, ("zq", "x"), 0, 0, tiled=True)
    ids = ids.reshape((group, ring) + ids.shape[1:])
    shared = shifted(part, "c", 1)
    near = split_tables(tables, other)
    part = split_tables(part)

    low, high = tuple(range(count // 2)), tuple(range(count // 2, count))
    whole = low + high

    far_low, shared = bags(ids, near, part, shared, examples, (((2, 2), low),), raw=True)
    far_low = by_core(far_low, 1, ring)
    (far_high,) = bags(ids, near, part, shared, examples, (((2, 2), high),))
    far_high = by_core(far_high, 1, ring)
    soon, late_low, late_high = bags(
        ids, near, part, shared, examples, (((3, 1), whole), ((1, 3), low), ((1, 3), high))
    )
    soon = by_core(soon, -1, ring)
    piece = jax.ShapeDtypeStruct(late_low.shape, late_low.dtype)
    late_low = local_kernel(add_kernel, piece, (late_low, far_low))
    late_low = by_core(late_low, 1, ring)
    late_high = local_kernel(add_kernel, piece, (late_high, far_high))
    late_high = by_core(late_high, 1, ring)
    (own,) = bags(ids, near, part, shared, examples, (((0, 0), whole),))
    block = jax.ShapeDtypeStruct(own.shape[1:], jnp.float32)
    here, up, over, down = local_kernel(
        join_kernel, (block,) * group, (own, soon, late_low, late_high)
    )
    over, up, down = (
        lax.ppermute(piece, Z, [(i, (i + parities * by) % depth) for i in range(depth)])
        for piece, by in ((over, 2), (up, 1), (down, 3))
    )
    pairs = count * (count + 1) // 2
    products, summed = local_kernel(
        pairs_kernel,
        (
            jax.ShapeDtypeStruct((pairs, examples), jnp.float32),
            jax.ShapeDtypeStruct((count * examples, width), jnp.float32),
        ),
        (here, over, up, down, dense_features),
    )
    pooled = local_kernel(
        pooled_kernel,
        jax.ShapeDtypeStruct((examples, count, width), jnp.float32),
        (summed,),
    )
    opposite = shifted(products, "y", 2)
    after = shifted(products, "y", 1)
    before = shifted(products, "y", -1)
    total = ((products + opposite) + (after + before)) * embedding**-0.5
    return pooled, total.T


def solution(mesh):
    torus = Mesh(mesh.devices.reshape(4, 2, 4, 2, mesh.shape["cols"]), ROWS + ("y",))

    def layer(*args):
        return body(512, *args)

    return jax.shard_map(
        layer,
        mesh=torus,
        in_specs=(
            P(None, ROWS, "y"),
            P(ROWS, "y"),
            P(ROWS, None, None, None),
            P(ROWS, None, None, None),
            P(ROWS, None, None),
        ),
        out_specs=(P(ROWS, None, "y"), P(ROWS, None)),
        check_vma=False,
    )
```

```python
import functools

import jax
import jax.numpy as jnp
from jax import lax
from jax.experimental import pallas as pl
from jax.experimental.pallas import tpu as pltpu
from jax.sharding import Mesh
from jax.sharding import PartitionSpec as P


Z = ("zq", "zp")
ROWS = Z + ("x", "c")
DEAD = 1 << 20
VMEM = pl.BlockSpec(memory_space=pltpu.VMEM)
HBM = pl.BlockSpec(memory_space=pltpu.HBM)


def shifted(value, axis, by):
    size = lax.axis_size(axis)
    return lax.ppermute(value, axis, [(i, (i + by) % size) for i in range(size)])


def local_kernel(kernel, out_shape, operands, flops=1 << 20, vmem=12 << 20, scratch=(), in_hbm=()):
    single = not isinstance(out_shape, tuple)
    return pl.pallas_call(
        kernel,
        in_specs=[HBM if k in in_hbm else VMEM for k in range(len(operands))],
        out_specs=VMEM if single else (VMEM,) * len(out_shape),
        out_shape=out_shape,
        scratch_shapes=scratch,
        compiler_params=pltpu.CompilerParams(vmem_limit_bytes=vmem),
        cost_estimate=pl.CostEstimate(flops=flops, bytes_accessed=1 << 20, transcendentals=0),
    )(*operands)


def prepare_kernel(
    counts_hbm, examples_hbm, rows_hbm, out_ref, counts_ref, examples_ref, rows_ref, live_ref, sems
):
    copies = [
        pltpu.make_async_copy(source, target, sems.at[k])
        for k, (source, target) in enumerate(
            ((counts_hbm, counts_ref), (examples_hbm, examples_ref), (rows_hbm, rows_ref))
        )
    ]
    for copy in copies:
        copy.start()
    depth, across, under, capacity = rows_ref.shape
    tables, owners = counts_ref.shape
    buckets = owners * tables
    bucket = lax.broadcasted_iota(jnp.int32, (buckets, owners), 0)
    owner = lax.broadcasted_iota(jnp.int32, (buckets, owners), 1)
    spread = jnp.where(bucket // tables == owner, 1.0, 0.0).astype(jnp.bfloat16)
    table = lax.broadcasted_iota(jnp.int32, (buckets, tables), 1)
    own = lax.broadcasted_iota(jnp.int32, (buckets, tables), 0) % tables
    slot = lax.broadcasted_iota(jnp.int32, (buckets, capacity), 1).astype(jnp.float32)
    copies[0].wait()
    counts = counts_ref[...].astype(jnp.float32).astype(jnp.bfloat16)
    by_table = lax.dot_general(
        spread, counts, (((1,), (1,)), ((), ())), preferred_element_type=jnp.float32
    )
    count = jnp.sum(jnp.where(table == own, by_table, 0.0), axis=1, keepdims=True)
    copies[1].wait()
    live = jnp.where(slot < count, examples_ref[...].reshape(buckets, capacity), DEAD)
    live_ref[...] = live.reshape(live_ref.shape)
    copies[2].wait()
    odd = lax.axis_index("zp")
    core = lax.axis_index("c")
    mine = lax.broadcasted_iota(jnp.int32, (across, under, capacity), 1) < tables

    def core_first(value):
        swapped = jnp.concatenate([value[:, tables:], value[:, :tables]], axis=1)
        return jnp.where(core == 0, value, swapped)

    for q in range(depth // 2):
        here = 2 * q + odd
        even_pair = 2 * q + 1 - odd
        odd_pair = lax.rem(2 * q + depth - 1 + 3 * odd, depth)
        first = jnp.where(core == 0, even_pair, odd_pair)
        second = jnp.where(core == 0, odd_pair, even_pair)
        for ref, lanes in ((rows_ref, slice(0, capacity)), (live_ref, slice(capacity, None))):
            out_ref[q, :, :under, lanes] = core_first(ref[here])
            out_ref[q, :, under:, lanes] = core_first(jnp.where(
                mine == (core == 0), ref[first], ref[second]
            ))


def split_into(out_ref, place, full):
    width = full.shape[1]
    high = full.astype(jnp.bfloat16)
    out_ref[place, :, :width] = high
    out_ref[place, :, width:] = (full - high.astype(jnp.float32)).astype(jnp.bfloat16)


def split_kernel(*refs):
    out_ref = refs[-1]
    count = refs[0].shape[0]
    for place, ref in enumerate(refs[:-1]):
        for t in range(count):
            split_into(out_ref, place * count + t, ref[t])


def split_tables(*tables):
    count, rows, width = tables[0].shape
    return local_kernel(
        split_kernel,
        jax.ShapeDtypeStruct((len(tables) * count, rows, 2 * width), jnp.bfloat16),
        tables,
    )


def one_hot(mask):
    return jnp.where(mask, 1.0, 0.0).astype(jnp.bfloat16)


def bags_kernel(*refs, examples, count, parts, raw):
    ids_ref, near_ref, part_ref, shared_ref, *refs = refs
    out_refs, refs = refs[: len(parts)], refs[len(parts) :]
    if raw:
        shared_hbm = shared_ref
        shared_ref, looked_ref, full_ref, sems = refs
        half = count // 2
        copies = [
            pltpu.make_async_copy(
                shared_hbm.at[k * half : (k + 1) * half],
                full_ref.at[k * half : (k + 1) * half],
                sems.at[k],
            )
            for k in range(2)
        ]
        for copy in copies:
            copy.start()
    else:
        (looked_ref,) = refs
    group, ring, messages, lanes = ids_ref.shape
    rows, wide = near_ref.shape[1:]
    owners = messages // count
    slots = lanes // 2
    core = lax.axis_index("c")
    aways = tuple(dict.fromkeys(away for away, _ in parts))
    depth = lax.axis_index("zq")
    row_iota = lax.broadcasted_iota(jnp.int32, (slots, rows), 1)
    key_iota = lax.broadcasted_iota(jnp.int32, (group * examples, group * slots), 0)
    columns, keys = [], []
    for away in aways:
        chosen = away[0] + core * (away[1] - away[0])
        column = lax.rem(lax.axis_index("x") + chosen, ring)
        ids = [ids_ref[lax.rem(depth + j, group), column] for j in range(group)]
        columns.append(jnp.swapaxes(jnp.concatenate(ids, axis=0), 0, 1))
        keys.append(
            jnp.concatenate([ids[j][:, slots:] + j * examples for j in range(group)], axis=1)
        )
    block = group * slots

    def look(o, t):
        ref, place = ((near_ref, t), (near_ref, count + t), (part_ref, t), (shared_ref, t))[o]
        message = o * count + t
        picks = jnp.concatenate(
            [
                one_hot(
                    one[:slots, j * messages + message : j * messages + message + 1] == row_iota
                )
                for one in columns
                for j in range(group)
            ],
            axis=0,
        )
        looked = jnp.dot(picks, ref[place], preferred_element_type=jnp.float32)
        for k in range(len(aways)):
            looked_ref[k, t, o * block : (o + 1) * block, :] = looked[
                k * block : (k + 1) * block
            ].astype(jnp.bfloat16)

    def pool(k, t, out_ref, place):
        into = [
            one_hot(keys[k][o * count + t : o * count + t + 1] == key_iota) for o in range(owners)
        ]
        total = jnp.dot(
            jnp.concatenate(into, axis=1), looked_ref[k, t], preferred_element_type=jnp.float32
        )
        summed = total[:, : wide // 2] + total[:, wide // 2 :]
        out_ref[:, place * examples : (place + 1) * examples, :] = summed.reshape(
            group, examples, wide // 2
        )

    early = owners - 1 if raw else 0
    tables = tuple(dict.fromkeys(t for _, chosen in parts for t in chosen))
    for t in tables:
        for o in range(early):
            look(o, t)
    if raw:
        copies[0].wait()
    for t in tables:
        if raw:
            split_into(shared_ref, t, full_ref[t])
        for o in range(early, owners):
            look(o, t)
        for (away, chosen), out_ref in zip(parts, out_refs):
            if t in chosen:
                pool(aways.index(away), t, out_ref, chosen.index(t))
    if raw:
        copies[1].wait()
        for t in range(half, count):
            split_into(shared_ref, t, full_ref[t])


def bags(ids, near, part, shared, examples, parts, raw=False):
    group, _, messages, lanes = ids.shape
    count, rows, wide = part.shape
    tasks = sum(len(tables) for _, tables in parts)
    work = messages // count * tasks * group * lanes // 2
    out = tuple(
        jax.ShapeDtypeStruct((group, len(tables) * examples, wide // 2), jnp.float32)
        for _, tables in parts
    )
    chunks = len(set(away for away, _ in parts))
    scratch = [
        pltpu.VMEM((chunks, count, messages // count * group * lanes // 2, wide), jnp.bfloat16)
    ]
    if raw:
        out += (jax.ShapeDtypeStruct(part.shape, part.dtype),)
        scratch += [pltpu.VMEM(shared.shape, jnp.float32), pltpu.SemaphoreType.DMA((2,))]
    return local_kernel(
        functools.partial(bags_kernel, examples=examples, count=count, parts=parts, raw=raw),
        out,
        (ids, near, part, shared),
        flops=2 * work * wide * (rows + group * examples),
        vmem=20 << 20,
        scratch=scratch,
        in_hbm=(3,) if raw else (),
    )


def by_core(value, by, ring):
    pairs = [
        (2 * i + c, 2 * ((i + by * (1 - 2 * c)) % ring) + c) for i in range(ring) for c in range(2)
    ]
    return lax.ppermute(value, ("x", "c"), pairs)


def add_kernel(one_ref, two_ref, out_ref):
    out_ref[...] = one_ref[...] + two_ref[...]


def join_kernel(own_ref, soon_ref, low_ref, high_ref, *out_refs):
    half = low_ref.shape[1]
    for j, out_ref in enumerate(out_refs):
        out_ref[:half] = own_ref[j, :half] + soon_ref[j, :half] + low_ref[j]
        out_ref[half:] = own_ref[j, half:] + soon_ref[j, half:] + high_ref[j]


def pairs_kernel(own_ref, one_ref, two_ref, three_ref, dense_ref, pairs_ref, summed_ref):
    examples = dense_ref.shape[0]
    pooled = own_ref[...] + one_ref[...] + two_ref[...] + three_ref[...]
    summed_ref[...] = pooled
    tables = pooled.shape[0] // examples
    vectors = [dense_ref[...]]
    for t in range(tables):
        vectors.append(pooled[t * examples : (t + 1) * examples])
    lane = lax.broadcasted_iota(jnp.int32, dense_ref.shape, 1)
    pairs = jnp.zeros(dense_ref.shape, jnp.float32)
    place = 0
    for i in range(tables + 1):
        for j in range(i + 1, tables + 1):
            product = jnp.sum(vectors[i] * vectors[j], axis=1, keepdims=True)
            pairs = jnp.where(lane == place, product, pairs)
            place += 1
    pairs_ref[...] = jnp.swapaxes(pairs, 0, 1)[: pairs_ref.shape[0]]


def pooled_kernel(summed_ref, pooled_ref):
    examples, tables = pooled_ref.shape[:2]
    for t in range(tables):
        pooled_ref[:, t, :] = summed_ref[t * examples : (t + 1) * examples]


def body(embedding, tables, dense_features, slot_rows, slot_examples, slot_counts):
    count, _, width = tables.shape
    examples = dense_features.shape[0]
    capacity = slot_rows.shape[3]
    group, parities, ring, cores = (lax.axis_size(a) for a in ROWS)
    depth = group * parities

    pairs = [
        (2 * i + k, 2 * (i ^ 1 if k == 0 else (i + (1 if i % 2 else -1)) % depth) + k)
        for i in range(depth)
        for k in range(cores)
    ]
    part = lax.ppermute(tables, Z + ("c",), pairs)
    other = shifted(tables, "c", 1)
    split_ids = (depth, ring, cores * count, capacity)
    ids = local_kernel(
        prepare_kernel,
        jax.ShapeDtypeStruct((group, ring, 2 * cores * count, 2 * capacity), jnp.int32),
        (slot_counts[0].T, slot_examples.reshape(split_ids), slot_rows.reshape(split_ids)),
        vmem=67043328,
        scratch=[
            pltpu.VMEM(slot_counts.shape[:0:-1], jnp.int32),
            pltpu.VMEM(split_ids, jnp.int32),
            pltpu.VMEM(split_ids, jnp.int32),
            pltpu.VMEM(split_ids, jnp.int32),
            pltpu.SemaphoreType.DMA((3,)),
        ],
        in_hbm=range(3),
    )
    ids = ids.reshape((group * ring,) + ids.shape[2:])
    ids = lax.all_to_all(ids, ("zq", "x"), 0, 0, tiled=True)
    ids = ids.reshape((group, ring) + ids.shape[1:])
    shared = shifted(part, "c", 1)
    near = split_tables(tables, other)
    part = split_tables(part)

    low, high = tuple(range(count // 2)), tuple(range(count // 2, count))
    whole = low + high

    far_low, shared = bags(ids, near, part, shared, examples, (((2, 2), low),), raw=True)
    far_low = by_core(far_low, 1, ring)
    (far_high,) = bags(ids, near, part, shared, examples, (((2, 2), high),))
    far_high = by_core(far_high, 1, ring)
    soon, late_low, late_high = bags(
        ids, near, part, shared, examples, (((3, 1), whole), ((1, 3), low), ((1, 3), high))
    )
    soon = by_core(soon, -1, ring)
    piece = jax.ShapeDtypeStruct(late_low.shape, late_low.dtype)
    late_low = local_kernel(add_kernel, piece, (late_low, far_low))
    late_low = by_core(late_low, 1, ring)
    late_high = local_kernel(add_kernel, piece, (late_high, far_high))
    late_high = by_core(late_high, 1, ring)
    (own,) = bags(ids, near, part, shared, examples, (((0, 0), whole),))
    block = jax.ShapeDtypeStruct(own.shape[1:], jnp.float32)
    here, up, over, down = local_kernel(
        join_kernel, (block,) * group, (own, soon, late_low, late_high)
    )
    moves = []
    for piece, by in ((up, 1), (down, 3), (over, 2)):
        moves.append(
            lax.ppermute(piece, Z, [(i, (i + parities * by) % depth) for i in range(depth)])
        )
    up, down, over = moves
    pairs = count * (count + 1) // 2
    products, summed = local_kernel(
        pairs_kernel,
        (
            jax.ShapeDtypeStruct((pairs, examples), jnp.float32),
            jax.ShapeDtypeStruct((count * examples, width), jnp.float32),
        ),
        (here, over, up, down, dense_features),
    )
    pooled = local_kernel(
        pooled_kernel,
        jax.ShapeDtypeStruct((examples, count, width), jnp.float32),
        (summed,),
    )
    opposite = shifted(products, "y", 2)
    after = shifted(products, "y", 1)
    before = shifted(products, "y", -1)
    total = ((products + opposite) + (after + before)) * embedding**-0.5
    return pooled, total.T


def solution(mesh):
    torus = Mesh(mesh.devices.reshape(4, 2, 4, 2, mesh.shape["cols"]), ROWS + ("y",))

    def layer(*args):
        return body(512, *args)

    return jax.shard_map(
        layer,
        mesh=torus,
        in_specs=(
            P(None, ROWS, "y"),
            P(ROWS, "y"),
            P(ROWS, None, None, None),
            P(ROWS, None, None, None),
            P(ROWS, None, None),
        ),
        out_specs=(P(ROWS, None, "y"), P(ROWS, None)),
        check_vma=False,
    )
```

```python
import functools

import jax
import jax.numpy as jnp
from jax import lax
from jax.experimental import pallas as pl
from jax.experimental.pallas import tpu as pltpu
from jax.sharding import Mesh
from jax.sharding import PartitionSpec as P


Z = ("zq", "zp")
ROWS = Z + ("x", "c")
DEAD = 1 << 20
VMEM = pl.BlockSpec(memory_space=pltpu.VMEM)
HBM = pl.BlockSpec(memory_space=pltpu.HBM)


def shifted(value, axis, by):
    size = lax.axis_size(axis)
    return lax.ppermute(value, axis, [(i, (i + by) % size) for i in range(size)])


def local_kernel(kernel, out_shape, operands, flops=1 << 20, vmem=12 << 20, scratch=(), in_hbm=()):
    single = not isinstance(out_shape, tuple)
    return pl.pallas_call(
        kernel,
        in_specs=[HBM if k in in_hbm else VMEM for k in range(len(operands))],
        out_specs=VMEM if single else (VMEM,) * len(out_shape),
        out_shape=out_shape,
        scratch_shapes=scratch,
        compiler_params=pltpu.CompilerParams(vmem_limit_bytes=vmem),
        cost_estimate=pl.CostEstimate(flops=flops, bytes_accessed=1 << 20, transcendentals=0),
    )(*operands)


def prepare_kernel(
    counts_hbm, examples_hbm, rows_hbm, out_ref, counts_ref, examples_ref, rows_ref, live_ref, sems
):
    copies = [
        pltpu.make_async_copy(source, target, sems.at[k])
        for k, (source, target) in enumerate(
            ((counts_hbm, counts_ref), (examples_hbm, examples_ref), (rows_hbm, rows_ref))
        )
    ]
    for copy in copies:
        copy.start()
    depth, across, under, capacity = rows_ref.shape
    tables, owners = counts_ref.shape
    buckets = owners * tables
    bucket = lax.broadcasted_iota(jnp.int32, (buckets, owners), 0)
    owner = lax.broadcasted_iota(jnp.int32, (buckets, owners), 1)
    spread = jnp.where(bucket // tables == owner, 1.0, 0.0).astype(jnp.bfloat16)
    table = lax.broadcasted_iota(jnp.int32, (buckets, tables), 1)
    own = lax.broadcasted_iota(jnp.int32, (buckets, tables), 0) % tables
    slot = lax.broadcasted_iota(jnp.int32, (buckets, capacity), 1).astype(jnp.float32)
    copies[0].wait()
    counts = counts_ref[...].astype(jnp.float32).astype(jnp.bfloat16)
    by_table = lax.dot_general(
        spread, counts, (((1,), (1,)), ((), ())), preferred_element_type=jnp.float32
    )
    count = jnp.sum(jnp.where(table == own, by_table, 0.0), axis=1, keepdims=True)
    copies[1].wait()
    live = jnp.where(slot < count, examples_ref[...].reshape(buckets, capacity), DEAD)
    live_ref[...] = live.reshape(live_ref.shape)
    copies[2].wait()
    odd = lax.axis_index("zp")
    core = lax.axis_index("c")
    mine = lax.broadcasted_iota(jnp.int32, (across, under, capacity), 1) < tables

    def core_first(value):
        swapped = jnp.concatenate([value[:, tables:], value[:, :tables]], axis=1)
        return jnp.where(core == 0, value, swapped)

    for q in range(depth // 2):
        here = 2 * q + odd
        even_pair = 2 * q + 1 - odd
        odd_pair = lax.rem(2 * q + depth - 1 + 3 * odd, depth)
        first = jnp.where(core == 0, even_pair, odd_pair)
        second = jnp.where(core == 0, odd_pair, even_pair)
        for ref, lanes in ((rows_ref, slice(0, capacity)), (live_ref, slice(capacity, None))):
            out_ref[q, :, :under, lanes] = core_first(ref[here])
            out_ref[q, :, under:, lanes] = core_first(jnp.where(
                mine == (core == 0), ref[first], ref[second]
            ))


def split_into(out_ref, place, full):
    width = full.shape[1]
    high = full.astype(jnp.bfloat16)
    out_ref[place, :, :width] = high
    out_ref[place, :, width:] = (full - high.astype(jnp.float32)).astype(jnp.bfloat16)


def split_kernel(*refs):
    out_ref = refs[-1]
    count = refs[0].shape[0]
    for place, ref in enumerate(refs[:-1]):
        for t in range(count):
            split_into(out_ref, place * count + t, ref[t])


def split_tables(*tables):
    count, rows, width = tables[0].shape
    return local_kernel(
        split_kernel,
        jax.ShapeDtypeStruct((len(tables) * count, rows, 2 * width), jnp.bfloat16),
        tables,
    )


def one_hot(mask):
    return jnp.where(mask, 1.0, 0.0).astype(jnp.bfloat16)


def bags_kernel(*refs, examples, count, parts, raw):
    ids_ref, near_ref, part_ref, shared_ref, *refs = refs
    out_refs, refs = refs[: len(parts)], refs[len(parts) :]
    if raw:
        shared_hbm = shared_ref
        shared_ref, looked_ref, full_ref, sems = refs
        half = count // 2
        copies = [
            pltpu.make_async_copy(
                shared_hbm.at[k * half : (k + 1) * half],
                full_ref.at[k * half : (k + 1) * half],
                sems.at[k],
            )
            for k in range(2)
        ]
        for copy in copies:
            copy.start()
    else:
        (looked_ref,) = refs
    group, ring, messages, lanes = ids_ref.shape
    rows, wide = near_ref.shape[1:]
    owners = messages // count
    slots = lanes // 2
    core = lax.axis_index("c")
    aways = tuple(dict.fromkeys(away for away, _ in parts))
    depth = lax.axis_index("zq")
    row_iota = lax.broadcasted_iota(jnp.int32, (slots, rows), 1)
    key_iota = lax.broadcasted_iota(jnp.int32, (group * examples, group * slots), 0)
    columns, keys = [], []
    for away in aways:
        chosen = away[0] + core * (away[1] - away[0])
        column = lax.rem(lax.axis_index("x") + chosen, ring)
        ids = [ids_ref[lax.rem(depth + j, group), column] for j in range(group)]
        columns.append(jnp.swapaxes(jnp.concatenate(ids, axis=0), 0, 1))
        keys.append(
            jnp.concatenate([ids[j][:, slots:] + j * examples for j in range(group)], axis=1)
        )
    block = group * slots

    def look(o, t):
        ref, place = ((near_ref, t), (near_ref, count + t), (part_ref, t), (shared_ref, t))[o]
        message = o * count + t
        active = [k for k, a in enumerate(aways) if any(a == b and t in c for b, c in parts)]
        picks = jnp.concatenate(
            [
                one_hot(
                    columns[k][:slots, j * messages + message : j * messages + message + 1]
                    == row_iota
                )
                for k in active
                for j in range(group)
            ],
            axis=0,
        )
        looked = jnp.dot(picks, ref[place], preferred_element_type=jnp.float32)
        for n, k in enumerate(active):
            looked_ref[k, t, o * block : (o + 1) * block, :] = looked[
                n * block : (n + 1) * block
            ].astype(jnp.bfloat16)

    def pool(k, t, out_ref, place):
        into = [
            one_hot(keys[k][o * count + t : o * count + t + 1] == key_iota) for o in range(owners)
        ]
        total = jnp.dot(
            jnp.concatenate(into, axis=1), looked_ref[k, t], preferred_element_type=jnp.float32
        )
        summed = total[:, : wide // 2] + total[:, wide // 2 :]
        out_ref[:, place * examples : (place + 1) * examples, :] = summed.reshape(
            group, examples, wide // 2
        )

    early = owners - 1 if raw else 0
    tables = tuple(dict.fromkeys(t for _, chosen in parts for t in chosen))
    for t in tables:
        for o in range(early):
            look(o, t)
    if raw:
        copies[0].wait()
    for t in tables:
        if raw:
            split_into(shared_ref, t, full_ref[t])
        for o in range(early, owners):
            look(o, t)
        for (away, chosen), out_ref in zip(parts, out_refs):
            if t in chosen:
                pool(aways.index(away), t, out_ref, chosen.index(t))
    if raw:
        copies[1].wait()
        for t in range(half, count):
            split_into(shared_ref, t, full_ref[t])


def bags(ids, near, part, shared, examples, parts, raw=False):
    group, _, messages, lanes = ids.shape
    count, rows, wide = part.shape
    tasks = sum(len(tables) for _, tables in parts)
    work = messages // count * tasks * group * lanes // 2
    out = tuple(
        jax.ShapeDtypeStruct((group, len(tables) * examples, wide // 2), jnp.float32)
        for _, tables in parts
    )
    chunks = len(set(away for away, _ in parts))
    scratch = [
        pltpu.VMEM((chunks, count, messages // count * group * lanes // 2, wide), jnp.bfloat16)
    ]
    if raw:
        out += (jax.ShapeDtypeStruct(part.shape, part.dtype),)
        scratch += [pltpu.VMEM(shared.shape, jnp.float32), pltpu.SemaphoreType.DMA((2,))]
    return local_kernel(
        functools.partial(bags_kernel, examples=examples, count=count, parts=parts, raw=raw),
        out,
        (ids, near, part, shared),
        flops=2 * work * wide * (rows + group * examples),
        vmem=20 << 20,
        scratch=scratch,
        in_hbm=(3,) if raw else (),
    )


def by_core(value, by, ring):
    pairs = [
        (2 * i + c, 2 * ((i + by * (1 - 2 * c)) % ring) + c) for i in range(ring) for c in range(2)
    ]
    return lax.ppermute(value, ("x", "c"), pairs)


def add_kernel(one_ref, two_ref, out_ref):
    out_ref[...] = one_ref[...] + two_ref[...]


def join_kernel(own_ref, soon_ref, low_ref, high_ref, *out_refs):
    half = low_ref.shape[1]
    for j, out_ref in enumerate(out_refs):
        out_ref[:half] = own_ref[j, :half] + soon_ref[j, :half] + low_ref[j]
        out_ref[half:] = own_ref[j, half:] + soon_ref[j, half:] + high_ref[j]


def pairs_kernel(own_ref, one_ref, two_ref, three_ref, dense_ref, pairs_ref, summed_ref):
    examples = dense_ref.shape[0]
    pooled = own_ref[...] + one_ref[...] + two_ref[...] + three_ref[...]
    summed_ref[...] = pooled
    tables = pooled.shape[0] // examples
    vectors = [dense_ref[...]]
    for t in range(tables):
        vectors.append(pooled[t * examples : (t + 1) * examples])
    lane = lax.broadcasted_iota(jnp.int32, dense_ref.shape, 1)
    pairs = jnp.zeros(dense_ref.shape, jnp.float32)
    place = 0
    for i in range(tables + 1):
        for j in range(i + 1, tables + 1):
            product = jnp.sum(vectors[i] * vectors[j], axis=1, keepdims=True)
            pairs = jnp.where(lane == place, product, pairs)
            place += 1
    pairs_ref[...] = jnp.swapaxes(pairs, 0, 1)[: pairs_ref.shape[0]]


def pooled_kernel(summed_ref, pooled_ref):
    examples, tables = pooled_ref.shape[:2]
    for t in range(tables):
        pooled_ref[:, t, :] = summed_ref[t * examples : (t + 1) * examples]


def body(embedding, tables, dense_features, slot_rows, slot_examples, slot_counts):
    count, _, width = tables.shape
    examples = dense_features.shape[0]
    capacity = slot_rows.shape[3]
    group, parities, ring, cores = (lax.axis_size(a) for a in ROWS)
    depth = group * parities

    pairs = [
        (2 * i + k, 2 * (i ^ 1 if k == 0 else (i + (1 if i % 2 else -1)) % depth) + k)
        for i in range(depth)
        for k in range(cores)
    ]
    part = lax.ppermute(tables, Z + ("c",), pairs)
    other = shifted(tables, "c", 1)
    split_ids = (depth, ring, cores * count, capacity)
    ids = local_kernel(
        prepare_kernel,
        jax.ShapeDtypeStruct((group, ring, 2 * cores * count, 2 * capacity), jnp.int32),
        (slot_counts[0].T, slot_examples.reshape(split_ids), slot_rows.reshape(split_ids)),
        vmem=67043328,
        scratch=[
            pltpu.VMEM(slot_counts.shape[:0:-1], jnp.int32),
            pltpu.VMEM(split_ids, jnp.int32),
            pltpu.VMEM(split_ids, jnp.int32),
            pltpu.VMEM(split_ids, jnp.int32),
            pltpu.SemaphoreType.DMA((3,)),
        ],
        in_hbm=range(3),
    )
    ids = ids.reshape((group * ring,) + ids.shape[2:])
    ids = lax.all_to_all(ids, ("zq", "x"), 0, 0, tiled=True)
    ids = ids.reshape((group, ring) + ids.shape[1:])
    shared = shifted(part, "c", 1)
    near = split_tables(tables, other)
    part = split_tables(part)

    low, high = tuple(range(count // 2)), tuple(range(count // 2, count))
    whole = low + high

    far_low, shared = bags(ids, near, part, shared, examples, (((2, 2), low),), raw=True)
    far_low = by_core(far_low, 1, ring)
    far_high, soon = bags(ids, near, part, shared, examples, (((2, 2), high), ((3, 1), whole)))
    far_high = by_core(far_high, 1, ring)
    soon = by_core(soon, -1, ring)
    late_low, late_high = bags(ids, near, part, shared, examples, (((1, 3), low), ((1, 3), high)))
    piece = jax.ShapeDtypeStruct(late_low.shape, late_low.dtype)
    late_low = local_kernel(add_kernel, piece, (late_low, far_low))
    late_low = by_core(late_low, 1, ring)
    late_high = local_kernel(add_kernel, piece, (late_high, far_high))
    late_high = by_core(late_high, 1, ring)
    (own,) = bags(ids, near, part, shared, examples, (((0, 0), whole),))
    block = jax.ShapeDtypeStruct(own.shape[1:], jnp.float32)
    here, up, over, down = local_kernel(
        join_kernel, (block,) * group, (own, soon, late_low, late_high)
    )
    over, up, down = (
        lax.ppermute(piece, Z, [(i, (i + parities * by) % depth) for i in range(depth)])
        for piece, by in ((over, 2), (up, 1), (down, 3))
    )
    pairs = count * (count + 1) // 2
    products, summed = local_kernel(
        pairs_kernel,
        (
            jax.ShapeDtypeStruct((pairs, examples), jnp.float32),
            jax.ShapeDtypeStruct((count * examples, width), jnp.float32),
        ),
        (here, over, up, down, dense_features),
    )
    pooled = local_kernel(
        pooled_kernel,
        jax.ShapeDtypeStruct((examples, count, width), jnp.float32),
        (summed,),
    )
    opposite = shifted(products, "y", 2)
    after = shifted(products, "y", 1)
    before = shifted(products, "y", -1)
    total = ((products + opposite) + (after + before)) * embedding**-0.5
    return pooled, total.T


def solution(mesh):
    torus = Mesh(mesh.devices.reshape(4, 2, 4, 2, mesh.shape["cols"]), ROWS + ("y",))

    def layer(*args):
        return body(512, *args)

    return jax.shard_map(
        layer,
        mesh=torus,
        in_specs=(
            P(None, ROWS, "y"),
            P(ROWS, "y"),
            P(ROWS, None, None, None),
            P(ROWS, None, None, None),
            P(ROWS, None, None),
        ),
        out_specs=(P(ROWS, None, "y"), P(ROWS, None)),
        check_vma=False,
    )
```

```python
import functools

import jax
import jax.numpy as jnp
from jax import lax
from jax.experimental import pallas as pl
from jax.experimental.pallas import tpu as pltpu
from jax.sharding import Mesh
from jax.sharding import PartitionSpec as P


Z = ("zq", "zp")
ROWS = Z + ("x", "c")
DEAD = 1 << 20
VMEM = pl.BlockSpec(memory_space=pltpu.VMEM)
HBM = pl.BlockSpec(memory_space=pltpu.HBM)


def shifted(value, axis, by):
    size = lax.axis_size(axis)
    return lax.ppermute(value, axis, [(i, (i + by) % size) for i in range(size)])


def local_kernel(kernel, out_shape, operands, flops=1 << 20, vmem=12 << 20, scratch=(), in_hbm=()):
    single = not isinstance(out_shape, tuple)
    return pl.pallas_call(
        kernel,
        in_specs=[HBM if k in in_hbm else VMEM for k in range(len(operands))],
        out_specs=VMEM if single else (VMEM,) * len(out_shape),
        out_shape=out_shape,
        scratch_shapes=scratch,
        compiler_params=pltpu.CompilerParams(vmem_limit_bytes=vmem),
        cost_estimate=pl.CostEstimate(flops=flops, bytes_accessed=1 << 20, transcendentals=0),
    )(*operands)


def prepare_kernel(
    counts_hbm, examples_hbm, rows_hbm, out_ref, counts_ref, examples_ref, rows_ref, live_ref, sems
):
    copies = [
        pltpu.make_async_copy(source, target, sems.at[k])
        for k, (source, target) in enumerate(
            ((counts_hbm, counts_ref), (examples_hbm, examples_ref), (rows_hbm, rows_ref))
        )
    ]
    for copy in copies:
        copy.start()
    depth, across, under, capacity = rows_ref.shape
    tables, owners = counts_ref.shape
    buckets = owners * tables
    bucket = lax.broadcasted_iota(jnp.int32, (buckets, owners), 0)
    owner = lax.broadcasted_iota(jnp.int32, (buckets, owners), 1)
    spread = jnp.where(bucket // tables == owner, 1.0, 0.0).astype(jnp.bfloat16)
    table = lax.broadcasted_iota(jnp.int32, (buckets, tables), 1)
    own = lax.broadcasted_iota(jnp.int32, (buckets, tables), 0) % tables
    slot = lax.broadcasted_iota(jnp.int32, (buckets, capacity), 1).astype(jnp.float32)
    copies[0].wait()
    counts = counts_ref[...].astype(jnp.float32).astype(jnp.bfloat16)
    by_table = lax.dot_general(
        spread, counts, (((1,), (1,)), ((), ())), preferred_element_type=jnp.float32
    )
    count = jnp.sum(jnp.where(table == own, by_table, 0.0), axis=1, keepdims=True)
    copies[1].wait()
    live = jnp.where(slot < count, examples_ref[...].reshape(buckets, capacity), DEAD)
    live_ref[...] = live.reshape(live_ref.shape)
    copies[2].wait()
    odd = lax.axis_index("zp")
    core = lax.axis_index("c")
    mine = lax.broadcasted_iota(jnp.int32, (across, under, capacity), 1) < tables

    def core_first(value):
        swapped = jnp.concatenate([value[:, tables:], value[:, :tables]], axis=1)
        return jnp.where(core == 0, value, swapped)

    for q in range(depth // 2):
        here = 2 * q + odd
        even_pair = 2 * q + 1 - odd
        odd_pair = lax.rem(2 * q + depth - 1 + 3 * odd, depth)
        first = jnp.where(core == 0, even_pair, odd_pair)
        second = jnp.where(core == 0, odd_pair, even_pair)
        for ref, lanes in ((rows_ref, slice(0, capacity)), (live_ref, slice(capacity, None))):
            out_ref[q, :, :under, lanes] = core_first(ref[here])
            out_ref[q, :, under:, lanes] = core_first(jnp.where(
                mine == (core == 0), ref[first], ref[second]
            ))


def split_into(out_ref, place, full):
    width = full.shape[1]
    high = full.astype(jnp.bfloat16)
    out_ref[place, :, :width] = high
    out_ref[place, :, width:] = (full - high.astype(jnp.float32)).astype(jnp.bfloat16)


def split_kernel(*refs):
    out_ref = refs[-1]
    count = refs[0].shape[0]
    for place, ref in enumerate(refs[:-1]):
        for t in range(count):
            split_into(out_ref, place * count + t, ref[t])


def split_tables(*tables):
    count, rows, width = tables[0].shape
    return local_kernel(
        split_kernel,
        jax.ShapeDtypeStruct((len(tables) * count, rows, 2 * width), jnp.bfloat16),
        tables,
    )


def one_hot(mask):
    return jnp.where(mask, 1.0, 0.0).astype(jnp.bfloat16)


def bags_kernel(*refs, examples, count, parts):
    ids_ref, near_ref, part_ref, shared_ref, *refs = refs
    out_refs, refs = refs[: len(parts)], refs[len(parts) :]
    (looked_ref,) = refs
    group, ring, messages, lanes = ids_ref.shape
    rows, wide = near_ref.shape[1:]
    owners = messages // count
    slots = lanes // 2
    core = lax.axis_index("c")
    aways = tuple(dict.fromkeys(away for away, _ in parts))
    depth = lax.axis_index("zq")
    row_iota = lax.broadcasted_iota(jnp.int32, (slots, rows), 1)
    key_iota = lax.broadcasted_iota(jnp.int32, (group * examples, group * slots), 0)
    columns, keys = [], []
    for away in aways:
        chosen = away[0] + core * (away[1] - away[0])
        column = lax.rem(lax.axis_index("x") + chosen, ring)
        ids = [ids_ref[lax.rem(depth + j, group), column] for j in range(group)]
        columns.append(jnp.swapaxes(jnp.concatenate(ids, axis=0), 0, 1))
        keys.append(
            jnp.concatenate([ids[j][:, slots:] + j * examples for j in range(group)], axis=1)
        )
    block = group * slots

    def look(o, t):
        ref, place = ((near_ref, t), (near_ref, count + t), (part_ref, t), (shared_ref, t))[o]
        message = o * count + t
        picks = jnp.concatenate(
            [
                one_hot(
                    one[:slots, j * messages + message : j * messages + message + 1] == row_iota
                )
                for one in columns
                for j in range(group)
            ],
            axis=0,
        )
        looked = jnp.dot(picks, ref[place], preferred_element_type=jnp.float32)
        for k in range(len(aways)):
            looked_ref[k, t, o * block : (o + 1) * block, :] = looked[
                k * block : (k + 1) * block
            ].astype(jnp.bfloat16)

    def pool(k, t, out_ref, place):
        into = [
            one_hot(keys[k][o * count + t : o * count + t + 1] == key_iota) for o in range(owners)
        ]
        total = jnp.dot(
            jnp.concatenate(into, axis=1), looked_ref[k, t], preferred_element_type=jnp.float32
        )
        summed = total[:, : wide // 2] + total[:, wide // 2 :]
        out_ref[:, place * examples : (place + 1) * examples, :] = summed.reshape(
            group, examples, wide // 2
        )

    for t in dict.fromkeys(t for _, chosen in parts for t in chosen):
        for o in range(owners):
            look(o, t)
        for (away, chosen), out_ref in zip(parts, out_refs):
            if t in chosen:
                pool(aways.index(away), t, out_ref, chosen.index(t))


def bags(ids, near, part, shared, examples, parts):
    group, _, messages, lanes = ids.shape
    count, rows, wide = part.shape
    tasks = sum(len(tables) for _, tables in parts)
    work = messages // count * tasks * group * lanes // 2
    out = tuple(
        jax.ShapeDtypeStruct((group, len(tables) * examples, wide // 2), jnp.float32)
        for _, tables in parts
    )
    chunks = len(set(away for away, _ in parts))
    scratch = [
        pltpu.VMEM((chunks, count, messages // count * group * lanes // 2, wide), jnp.bfloat16)
    ]
    return local_kernel(
        functools.partial(bags_kernel, examples=examples, count=count, parts=parts),
        out,
        (ids, near, part, shared),
        flops=2 * work * wide * (rows + group * examples),
        vmem=20 << 20,
        scratch=scratch,
    )


def far_chunk(ids_ref, examples):
    group, ring, _, lanes = ids_ref.shape
    column = lax.rem(lax.axis_index("x") + ring // 2, ring)
    depth = lax.axis_index("zq")
    ids = [ids_ref[lax.rem(depth + j, group), column] for j in range(group)]
    columns = jnp.swapaxes(jnp.concatenate(ids, axis=0), 0, 1)[: lanes // 2]
    keys = jnp.concatenate([ids[j][:, lanes // 2 :] + j * examples for j in range(group)], axis=1)
    return columns, keys


def far_look(ids_ref, columns, message, table):
    group, _, messages, lanes = ids_ref.shape
    row_iota = lax.broadcasted_iota(jnp.int32, (lanes // 2, table.shape[0]), 1)
    picks = jnp.concatenate(
        [
            one_hot(columns[:, j * messages + message : j * messages + message + 1] == row_iota)
            for j in range(group)
        ],
        axis=0,
    )
    looked = jnp.dot(picks, table, preferred_element_type=jnp.float32)
    return looked.astype(jnp.bfloat16)


def far_look_kernel(
    ids_ref, near_ref, part_ref, shared_hbm, looked_ref, shared_ref, full_ref, sem, *, examples
):
    copy = pltpu.make_async_copy(shared_hbm, full_ref, sem)
    copy.start()
    count = part_ref.shape[0]
    block = ids_ref.shape[0] * ids_ref.shape[3] // 2
    columns, _ = far_chunk(ids_ref, examples)
    for t in range(count):
        for o, ref in enumerate((near_ref.at[t], near_ref.at[count + t], part_ref.at[t])):
            looked_ref[t, o * block : (o + 1) * block, :] = far_look(
                ids_ref, columns, o * count + t, ref[...]
            )
    copy.wait()
    for t in range(count):
        split_into(shared_ref, t, full_ref[t])


def far_pool_kernel(ids_ref, shared_ref, looked_ref, out_ref, *, examples, tables):
    group, _, messages, lanes = ids_ref.shape
    count, _, wide = shared_ref.shape
    owners = messages // count
    columns, keys = far_chunk(ids_ref, examples)
    key_iota = lax.broadcasted_iota(jnp.int32, (group * examples, group * lanes // 2), 0)
    for place, t in enumerate(tables):
        last = far_look(ids_ref, columns, (owners - 1) * count + t, shared_ref[t])
        into = [one_hot(keys[o * count + t : o * count + t + 1] == key_iota) for o in range(owners)]
        total = jnp.dot(
            jnp.concatenate(into[:-1], axis=1), looked_ref[t], preferred_element_type=jnp.float32
        ) + jnp.dot(into[-1], last, preferred_element_type=jnp.float32)
        summed = total[:, : wide // 2] + total[:, wide // 2 :]
        out_ref[:, place * examples : (place + 1) * examples, :] = summed.reshape(
            group, examples, wide // 2
        )


def by_core(value, by, ring):
    pairs = [
        (2 * i + c, 2 * ((i + by * (1 - 2 * c)) % ring) + c) for i in range(ring) for c in range(2)
    ]
    return lax.ppermute(value, ("x", "c"), pairs)


def add_kernel(one_ref, two_ref, out_ref):
    out_ref[...] = one_ref[...] + two_ref[...]


def join_kernel(own_ref, soon_ref, low_ref, high_ref, *out_refs):
    half = low_ref.shape[1]
    for j, out_ref in enumerate(out_refs):
        out_ref[:half] = own_ref[j, :half] + soon_ref[j, :half] + low_ref[j]
        out_ref[half:] = own_ref[j, half:] + soon_ref[j, half:] + high_ref[j]


def pairs_kernel(own_ref, one_ref, two_ref, three_ref, dense_ref, pairs_ref, summed_ref):
    examples = dense_ref.shape[0]
    pooled = own_ref[...] + one_ref[...] + two_ref[...] + three_ref[...]
    summed_ref[...] = pooled
    tables = pooled.shape[0] // examples
    vectors = [dense_ref[...]]
    for t in range(tables):
        vectors.append(pooled[t * examples : (t + 1) * examples])
    lane = lax.broadcasted_iota(jnp.int32, dense_ref.shape, 1)
    pairs = jnp.zeros(dense_ref.shape, jnp.float32)
    place = 0
    for i in range(tables + 1):
        for j in range(i + 1, tables + 1):
            product = jnp.sum(vectors[i] * vectors[j], axis=1, keepdims=True)
            pairs = jnp.where(lane == place, product, pairs)
            place += 1
    pairs_ref[...] = jnp.swapaxes(pairs, 0, 1)[: pairs_ref.shape[0]]


def pooled_kernel(summed_ref, pooled_ref):
    examples, tables = pooled_ref.shape[:2]
    for t in range(tables):
        pooled_ref[:, t, :] = summed_ref[t * examples : (t + 1) * examples]


def body(embedding, tables, dense_features, slot_rows, slot_examples, slot_counts):
    count, rows, width = tables.shape
    examples = dense_features.shape[0]
    capacity = slot_rows.shape[3]
    group, parities, ring, cores = (lax.axis_size(a) for a in ROWS)
    depth = group * parities

    pairs = [
        (2 * i + k, 2 * (i ^ 1 if k == 0 else (i + (1 if i % 2 else -1)) % depth) + k)
        for i in range(depth)
        for k in range(cores)
    ]
    part = lax.ppermute(tables, Z + ("c",), pairs)
    other = shifted(tables, "c", 1)
    split_ids = (depth, ring, cores * count, capacity)
    ids = local_kernel(
        prepare_kernel,
        jax.ShapeDtypeStruct((group, ring, 2 * cores * count, 2 * capacity), jnp.int32),
        (slot_counts[0].T, slot_examples.reshape(split_ids), slot_rows.reshape(split_ids)),
        vmem=67043328,
        scratch=[
            pltpu.VMEM(slot_counts.shape[:0:-1], jnp.int32),
            pltpu.VMEM(split_ids, jnp.int32),
            pltpu.VMEM(split_ids, jnp.int32),
            pltpu.VMEM(split_ids, jnp.int32),
            pltpu.SemaphoreType.DMA((3,)),
        ],
        in_hbm=range(3),
    )
    ids = ids.reshape((group * ring,) + ids.shape[2:])
    ids = lax.all_to_all(ids, ("zq", "x"), 0, 0, tiled=True)
    ids = ids.reshape((group, ring) + ids.shape[1:])
    shared = shifted(part, "c", 1)
    near = split_tables(tables, other)
    part = split_tables(part)

    low, high = tuple(range(count // 2)), tuple(range(count // 2, count))
    whole = low + high

    block = group * capacity
    looked, shared = local_kernel(
        functools.partial(far_look_kernel, examples=examples),
        (
            jax.ShapeDtypeStruct((count, (2 * cores - 1) * block, 2 * width), jnp.bfloat16),
            jax.ShapeDtypeStruct(part.shape, part.dtype),
        ),
        (ids, near, part, shared),
        flops=2 * 3 * cores * count * block * rows * width,
        vmem=16 << 20,
        scratch=[pltpu.VMEM(shared.shape, jnp.float32), pltpu.SemaphoreType.DMA],
        in_hbm=(3,),
    )

    def far_pool(tables):
        return local_kernel(
            functools.partial(far_pool_kernel, examples=examples, tables=tables),
            jax.ShapeDtypeStruct((group, len(tables) * examples, width), jnp.float32),
            (ids, shared, looked),
            flops=4 * len(tables) * block * rows * width,
        )

    far_low = far_pool(low)
    far_low = by_core(far_low, 1, ring)
    far_high = far_pool(high)
    far_high = by_core(far_high, 1, ring)
    soon, late_low, late_high = bags(
        ids, near, part, shared, examples, (((3, 1), whole), ((1, 3), low), ((1, 3), high))
    )
    soon = by_core(soon, -1, ring)
    piece = jax.ShapeDtypeStruct(late_low.shape, late_low.dtype)
    late_low = local_kernel(add_kernel, piece, (late_low, far_low))
    late_low = by_core(late_low, 1, ring)
    late_high = local_kernel(add_kernel, piece, (late_high, far_high))
    late_high = by_core(late_high, 1, ring)
    (own,) = bags(ids, near, part, shared, examples, (((0, 0), whole),))
    final = jax.ShapeDtypeStruct(own.shape[1:], jnp.float32)
    here, up, over, down = local_kernel(
        join_kernel, (final,) * group, (own, soon, late_low, late_high)
    )
    over, up, down = (
        lax.ppermute(piece, Z, [(i, (i + parities * by) % depth) for i in range(depth)])
        for piece, by in ((over, 2), (up, 1), (down, 3))
    )
    pairs = count * (count + 1) // 2
    products, summed = local_kernel(
        pairs_kernel,
        (
            jax.ShapeDtypeStruct((pairs, examples), jnp.float32),
            jax.ShapeDtypeStruct((count * examples, width), jnp.float32),
        ),
        (here, over, up, down, dense_features),
    )
    pooled = local_kernel(
        pooled_kernel,
        jax.ShapeDtypeStruct((examples, count, width), jnp.float32),
        (summed,),
    )
    opposite = shifted(products, "y", 2)
    after = shifted(products, "y", 1)
    before = shifted(products, "y", -1)
    total = ((products + opposite) + (after + before)) * embedding**-0.5
    return pooled, total.T


def solution(mesh):
    torus = Mesh(mesh.devices.reshape(4, 2, 4, 2, mesh.shape["cols"]), ROWS + ("y",))

    def layer(*args):
        return body(512, *args)

    return jax.shard_map(
        layer,
        mesh=torus,
        in_specs=(
            P(None, ROWS, "y"),
            P(ROWS, "y"),
            P(ROWS, None, None, None),
            P(ROWS, None, None, None),
            P(ROWS, None, None),
        ),
        out_specs=(P(ROWS, None, "y"), P(ROWS, None)),
        check_vma=False,
    )
```

```python
import functools

import jax
import jax.numpy as jnp
from jax import lax
from jax.experimental import pallas as pl
from jax.experimental.pallas import tpu as pltpu
from jax.sharding import Mesh
from jax.sharding import PartitionSpec as P


Z = ("zq", "zp")
ROWS = Z + ("x", "c")
DEAD = 1 << 20
VMEM = pl.BlockSpec(memory_space=pltpu.VMEM)
HBM = pl.BlockSpec(memory_space=pltpu.HBM)


def shifted(value, axis, by):
    size = lax.axis_size(axis)
    return lax.ppermute(value, axis, [(i, (i + by) % size) for i in range(size)])


def local_kernel(kernel, out_shape, operands, flops=1 << 20, vmem=12 << 20, scratch=(), in_hbm=()):
    single = not isinstance(out_shape, tuple)
    return pl.pallas_call(
        kernel,
        in_specs=[HBM if k in in_hbm else VMEM for k in range(len(operands))],
        out_specs=VMEM if single else (VMEM,) * len(out_shape),
        out_shape=out_shape,
        scratch_shapes=scratch,
        compiler_params=pltpu.CompilerParams(vmem_limit_bytes=vmem),
        cost_estimate=pl.CostEstimate(flops=flops, bytes_accessed=1 << 20, transcendentals=0),
    )(*operands)


def prepare_kernel(
    counts_hbm, examples_hbm, rows_hbm, out_ref, counts_ref, examples_ref, rows_ref, live_ref, sems
):
    copies = [
        pltpu.make_async_copy(source, target, sems.at[k])
        for k, (source, target) in enumerate(
            ((counts_hbm, counts_ref), (examples_hbm, examples_ref), (rows_hbm, rows_ref))
        )
    ]
    for copy in copies:
        copy.start()
    depth, across, under, capacity = rows_ref.shape
    tables, owners = counts_ref.shape
    buckets = owners * tables
    bucket = lax.broadcasted_iota(jnp.int32, (buckets, owners), 0)
    owner = lax.broadcasted_iota(jnp.int32, (buckets, owners), 1)
    spread = jnp.where(bucket // tables == owner, 1.0, 0.0).astype(jnp.bfloat16)
    table = lax.broadcasted_iota(jnp.int32, (buckets, tables), 1)
    own = lax.broadcasted_iota(jnp.int32, (buckets, tables), 0) % tables
    slot = lax.broadcasted_iota(jnp.int32, (buckets, capacity), 1).astype(jnp.float32)
    copies[0].wait()
    counts = counts_ref[...].astype(jnp.float32).astype(jnp.bfloat16)
    by_table = lax.dot_general(
        spread, counts, (((1,), (1,)), ((), ())), preferred_element_type=jnp.float32
    )
    count = jnp.sum(jnp.where(table == own, by_table, 0.0), axis=1, keepdims=True)
    copies[1].wait()
    live = jnp.where(slot < count, examples_ref[...].reshape(buckets, capacity), DEAD)
    live_ref[...] = live.reshape(live_ref.shape)
    copies[2].wait()
    odd = lax.axis_index("zp")
    core = lax.axis_index("c")
    mine = lax.broadcasted_iota(jnp.int32, (across, under, capacity), 1) < tables

    def core_first(value):
        swapped = jnp.concatenate([value[:, tables:], value[:, :tables]], axis=1)
        return jnp.where(core == 0, value, swapped)

    for q in range(depth // 2):
        here = 2 * q + odd
        even_pair = 2 * q + 1 - odd
        odd_pair = lax.rem(2 * q + depth - 1 + 3 * odd, depth)
        first = jnp.where(core == 0, even_pair, odd_pair)
        second = jnp.where(core == 0, odd_pair, even_pair)
        for ref, lanes in ((rows_ref, slice(0, capacity)), (live_ref, slice(capacity, None))):
            out_ref[q, :, :under, lanes] = core_first(ref[here])
            out_ref[q, :, under:, lanes] = core_first(jnp.where(
                mine == (core == 0), ref[first], ref[second]
            ))


def split_into(out_ref, place, full):
    width = full.shape[1]
    high = full.astype(jnp.bfloat16)
    out_ref[place, :, :width] = high
    out_ref[place, :, width:] = (full - high.astype(jnp.float32)).astype(jnp.bfloat16)


def split_kernel(*refs):
    out_ref = refs[-1]
    count = refs[0].shape[0]
    for place, ref in enumerate(refs[:-1]):
        for t in range(count):
            split_into(out_ref, place * count + t, ref[t])


def split_tables(*tables):
    count, rows, width = tables[0].shape
    return local_kernel(
        split_kernel,
        jax.ShapeDtypeStruct((len(tables) * count, rows, 2 * width), jnp.bfloat16),
        tables,
    )


def one_hot(mask):
    return jnp.where(mask, 1.0, 0.0).astype(jnp.bfloat16)


def bags_kernel(*refs, examples, count, parts):
    ids_ref, near_ref, part_ref, shared_ref, *refs = refs
    out_refs, refs = refs[: len(parts)], refs[len(parts) :]
    (looked_ref,) = refs
    group, ring, messages, lanes = ids_ref.shape
    rows, wide = near_ref.shape[1:]
    owners = messages // count
    slots = lanes // 2
    core = lax.axis_index("c")
    aways = tuple(dict.fromkeys(away for away, _ in parts))
    depth = lax.axis_index("zq")
    row_iota = lax.broadcasted_iota(jnp.int32, (slots, rows), 1)
    key_iota = lax.broadcasted_iota(jnp.int32, (group * examples, group * slots), 0)
    columns, keys = [], []
    for away in aways:
        chosen = away[0] + core * (away[1] - away[0])
        column = lax.rem(lax.axis_index("x") + chosen, ring)
        ids = [ids_ref[lax.rem(depth + j, group), column] for j in range(group)]
        columns.append(jnp.swapaxes(jnp.concatenate(ids, axis=0), 0, 1))
        keys.append(
            jnp.concatenate([ids[j][:, slots:] + j * examples for j in range(group)], axis=1)
        )
    block = group * slots

    def look(o, t):
        ref, place = ((near_ref, t), (near_ref, count + t), (part_ref, t), (shared_ref, t))[o]
        message = o * count + t
        picks = jnp.concatenate(
            [
                one_hot(
                    one[:slots, j * messages + message : j * messages + message + 1] == row_iota
                )
                for one in columns
                for j in range(group)
            ],
            axis=0,
        )
        looked = jnp.dot(picks, ref[place], preferred_element_type=jnp.float32)
        for k in range(len(aways)):
            looked_ref[k, t, o * block : (o + 1) * block, :] = looked[
                k * block : (k + 1) * block
            ].astype(jnp.bfloat16)

    def pool(k, t, out_ref, place):
        into = [
            one_hot(keys[k][o * count + t : o * count + t + 1] == key_iota) for o in range(owners)
        ]
        total = jnp.dot(
            jnp.concatenate(into, axis=1), looked_ref[k, t], preferred_element_type=jnp.float32
        )
        summed = total[:, : wide // 2] + total[:, wide // 2 :]
        out_ref[:, place * examples : (place + 1) * examples, :] = summed.reshape(
            group, examples, wide // 2
        )

    for t in dict.fromkeys(t for _, chosen in parts for t in chosen):
        for o in range(owners):
            look(o, t)
        for (away, chosen), out_ref in zip(parts, out_refs):
            if t in chosen:
                pool(aways.index(away), t, out_ref, chosen.index(t))


def bags(ids, near, part, shared, examples, parts):
    group, _, messages, lanes = ids.shape
    count, rows, wide = part.shape
    tasks = sum(len(tables) for _, tables in parts)
    work = messages // count * tasks * group * lanes // 2
    out = tuple(
        jax.ShapeDtypeStruct((group, len(tables) * examples, wide // 2), jnp.float32)
        for _, tables in parts
    )
    chunks = len(set(away for away, _ in parts))
    scratch = [
        pltpu.VMEM((chunks, count, messages // count * group * lanes // 2, wide), jnp.bfloat16)
    ]
    return local_kernel(
        functools.partial(bags_kernel, examples=examples, count=count, parts=parts),
        out,
        (ids, near, part, shared),
        flops=2 * work * wide * (rows + group * examples),
        vmem=20 << 20,
        scratch=scratch,
    )


def far_chunk(ids_ref, examples):
    group, ring, _, lanes = ids_ref.shape
    column = lax.rem(lax.axis_index("x") + ring // 2, ring)
    depth = lax.axis_index("zq")
    ids = [ids_ref[lax.rem(depth + j, group), column] for j in range(group)]
    columns = jnp.swapaxes(jnp.concatenate(ids, axis=0), 0, 1)[: lanes // 2]
    keys = jnp.concatenate([ids[j][:, lanes // 2 :] + j * examples for j in range(group)], axis=1)
    return columns, keys


def far_look(ids_ref, columns, message, table):
    group, _, messages, lanes = ids_ref.shape
    row_iota = lax.broadcasted_iota(jnp.int32, (lanes // 2, table.shape[0]), 1)
    picks = jnp.concatenate(
        [
            one_hot(columns[:, j * messages + message : j * messages + message + 1] == row_iota)
            for j in range(group)
        ],
        axis=0,
    )
    looked = jnp.dot(picks, table, preferred_element_type=jnp.float32)
    return looked.astype(jnp.bfloat16)


def far_look_kernel(
    ids_ref, near_ref, part_ref, shared_hbm, looked_ref, shared_ref, full_ref, sem, *, examples
):
    copy = pltpu.make_async_copy(shared_hbm, full_ref, sem)
    copy.start()
    count = part_ref.shape[0]
    block = ids_ref.shape[0] * ids_ref.shape[3] // 2
    columns, _ = far_chunk(ids_ref, examples)
    for t in range(count):
        for o, ref in enumerate((near_ref.at[t], near_ref.at[count + t], part_ref.at[t])):
            looked_ref[t, o * block : (o + 1) * block, :] = far_look(
                ids_ref, columns, o * count + t, ref[...]
            )
    copy.wait()
    for t in range(count):
        split_into(shared_ref, t, full_ref[t])


def far_pool_kernel(ids_ref, shared_ref, looked_ref, out_ref, *, examples, tables):
    group, _, messages, lanes = ids_ref.shape
    count, _, wide = shared_ref.shape
    owners = messages // count
    columns, keys = far_chunk(ids_ref, examples)
    key_iota = lax.broadcasted_iota(jnp.int32, (group * examples, group * lanes // 2), 0)
    for place, t in enumerate(tables):
        last = far_look(ids_ref, columns, (owners - 1) * count + t, shared_ref[t])
        into = [one_hot(keys[o * count + t : o * count + t + 1] == key_iota) for o in range(owners)]
        total = jnp.dot(
            jnp.concatenate(into[:-1], axis=1), looked_ref[t], preferred_element_type=jnp.float32
        ) + jnp.dot(into[-1], last, preferred_element_type=jnp.float32)
        summed = total[:, : wide // 2] + total[:, wide // 2 :]
        out_ref[:, place * examples : (place + 1) * examples, :] = summed.reshape(
            group, examples, wide // 2
        )


def by_core(value, by, ring):
    pairs = [
        (2 * i + c, 2 * ((i + by * (1 - 2 * c)) % ring) + c) for i in range(ring) for c in range(2)
    ]
    return lax.ppermute(value, ("x", "c"), pairs)


def add_kernel(one_ref, two_ref, out_ref):
    out_ref[...] = one_ref[...] + two_ref[...]


def join_kernel(own_ref, soon_ref, low_ref, high_ref, *out_refs):
    half = low_ref.shape[1]
    odd = lax.rem(lax.axis_index("zq"), 2)
    for j, out_ref in zip((0, 2, 3 - 2 * odd, 1 + 2 * odd), out_refs):
        out_ref[:half] = own_ref[j, :half] + soon_ref[j, :half] + low_ref[j]
        out_ref[half:] = own_ref[j, half:] + soon_ref[j, half:] + high_ref[j]


def swapped(value, axis, partner):
    return lax.ppermute(value, axis, [(i, partner(i)) for i in range(lax.axis_size(axis))])


def pairs_kernel(own_ref, one_ref, two_ref, three_ref, dense_ref, pairs_ref, summed_ref):
    examples = dense_ref.shape[0]
    pooled = own_ref[...] + one_ref[...] + two_ref[...] + three_ref[...]
    summed_ref[...] = pooled
    tables = pooled.shape[0] // examples
    vectors = [dense_ref[...]]
    for t in range(tables):
        vectors.append(pooled[t * examples : (t + 1) * examples])
    lane = lax.broadcasted_iota(jnp.int32, dense_ref.shape, 1)
    pairs = jnp.zeros(dense_ref.shape, jnp.float32)
    place = 0
    for i in range(tables + 1):
        for j in range(i + 1, tables + 1):
            product = jnp.sum(vectors[i] * vectors[j], axis=1, keepdims=True)
            pairs = jnp.where(lane == place, product, pairs)
            place += 1
    pairs_ref[...] = jnp.swapaxes(pairs, 0, 1)[: pairs_ref.shape[0]]


def pooled_kernel(summed_ref, pooled_ref):
    examples, tables = pooled_ref.shape[:2]
    for t in range(tables):
        pooled_ref[:, t, :] = summed_ref[t * examples : (t + 1) * examples]


def body(embedding, tables, dense_features, slot_rows, slot_examples, slot_counts):
    count, rows, width = tables.shape
    examples = dense_features.shape[0]
    capacity = slot_rows.shape[3]
    group, parities, ring, cores = (lax.axis_size(a) for a in ROWS)
    depth = group * parities

    pairs = [
        (2 * i + k, 2 * (i ^ 1 if k == 0 else (i + (1 if i % 2 else -1)) % depth) + k)
        for i in range(depth)
        for k in range(cores)
    ]
    part = lax.ppermute(tables, Z + ("c",), pairs)
    other = shifted(tables, "c", 1)
    split_ids = (depth, ring, cores * count, capacity)
    ids = local_kernel(
        prepare_kernel,
        jax.ShapeDtypeStruct((group, ring, 2 * cores * count, 2 * capacity), jnp.int32),
        (slot_counts[0].T, slot_examples.reshape(split_ids), slot_rows.reshape(split_ids)),
        vmem=67043328,
        scratch=[
            pltpu.VMEM(slot_counts.shape[:0:-1], jnp.int32),
            pltpu.VMEM(split_ids, jnp.int32),
            pltpu.VMEM(split_ids, jnp.int32),
            pltpu.VMEM(split_ids, jnp.int32),
            pltpu.SemaphoreType.DMA((3,)),
        ],
        in_hbm=range(3),
    )
    ids = ids.reshape((group * ring,) + ids.shape[2:])
    ids = lax.all_to_all(ids, ("zq", "x"), 0, 0, tiled=True)
    ids = ids.reshape((group, ring) + ids.shape[1:])
    shared = shifted(part, "c", 1)
    near = split_tables(tables, other)
    part = split_tables(part)

    low, high = tuple(range(count // 2)), tuple(range(count // 2, count))
    whole = low + high

    block = group * capacity
    looked, shared = local_kernel(
        functools.partial(far_look_kernel, examples=examples),
        (
            jax.ShapeDtypeStruct((count, (2 * cores - 1) * block, 2 * width), jnp.bfloat16),
            jax.ShapeDtypeStruct(part.shape, part.dtype),
        ),
        (ids, near, part, shared),
        flops=2 * 3 * cores * count * block * rows * width,
        vmem=16 << 20,
        scratch=[pltpu.VMEM(shared.shape, jnp.float32), pltpu.SemaphoreType.DMA],
        in_hbm=(3,),
    )

    def far_pool(tables):
        return local_kernel(
            functools.partial(far_pool_kernel, examples=examples, tables=tables),
            jax.ShapeDtypeStruct((group, len(tables) * examples, width), jnp.float32),
            (ids, shared, looked),
            flops=4 * len(tables) * block * rows * width,
        )

    far_low = far_pool(low)
    far_low = by_core(far_low, 1, ring)
    far_high = far_pool(high)
    far_high = by_core(far_high, 1, ring)
    (soon,) = bags(ids, near, part, shared, examples, (((3, 1), whole),))
    soon = by_core(soon, -1, ring)
    late_low, late_high = bags(ids, near, part, shared, examples, (((1, 3), low), ((1, 3), high)))
    piece = jax.ShapeDtypeStruct(late_low.shape, late_low.dtype)
    late_low = local_kernel(add_kernel, piece, (late_low, far_low))
    late_low = by_core(late_low, 1, ring)
    late_high = local_kernel(add_kernel, piece, (late_high, far_high))
    late_high = by_core(late_high, 1, ring)
    (own,) = bags(ids, near, part, shared, examples, (((0, 0), whole),))
    final = jax.ShapeDtypeStruct(own.shape[1:], jnp.float32)
    here, *others = local_kernel(
        join_kernel, (final,) * group, (own, soon, late_low, late_high)
    )
    partners = (lambda i: i ^ 2, lambda i: 3 - i, lambda i: i ^ 1)
    for k, partner in enumerate(partners):
        others[k] = swapped(others[k], "zq", partner)
    pairs = count * (count + 1) // 2
    products, summed = local_kernel(
        pairs_kernel,
        (
            jax.ShapeDtypeStruct((pairs, examples), jnp.float32),
            jax.ShapeDtypeStruct((count * examples, width), jnp.float32),
        ),
        (here, *others, dense_features),
    )
    pooled = local_kernel(
        pooled_kernel,
        jax.ShapeDtypeStruct((examples, count, width), jnp.float32),
        (summed,),
    )
    got = []
    for partner in partners:
        got.append(swapped(products, "y", partner))
    total = ((products + got[0]) + (got[1] + got[2])) * embedding**-0.5
    return pooled, total.T


def solution(mesh):
    torus = Mesh(mesh.devices.reshape(4, 2, 4, 2, mesh.shape["cols"]), ROWS + ("y",))

    def layer(*args):
        return body(512, *args)

    return jax.shard_map(
        layer,
        mesh=torus,
        in_specs=(
            P(None, ROWS, "y"),
            P(ROWS, "y"),
            P(ROWS, None, None, None),
            P(ROWS, None, None, None),
            P(ROWS, None, None),
        ),
        out_specs=(P(ROWS, None, "y"), P(ROWS, None)),
        check_vma=False,
    )
```

```python
import functools

import jax
import jax.numpy as jnp
from jax import lax
from jax.experimental import pallas as pl
from jax.experimental.pallas import tpu as pltpu
from jax.sharding import Mesh
from jax.sharding import PartitionSpec as P


Z = ("zq", "zp")
ROWS = Z + ("x", "c")
DEAD = 1 << 20
VMEM = pl.BlockSpec(memory_space=pltpu.VMEM)
HBM = pl.BlockSpec(memory_space=pltpu.HBM)


def shifted(value, axis, by):
    size = lax.axis_size(axis)
    return lax.ppermute(value, axis, [(i, (i + by) % size) for i in range(size)])


def local_kernel(kernel, out_shape, operands, flops=1 << 20, vmem=12 << 20, scratch=(), in_hbm=()):
    single = not isinstance(out_shape, tuple)
    return pl.pallas_call(
        kernel,
        in_specs=[HBM if k in in_hbm else VMEM for k in range(len(operands))],
        out_specs=VMEM if single else (VMEM,) * len(out_shape),
        out_shape=out_shape,
        scratch_shapes=scratch,
        compiler_params=pltpu.CompilerParams(vmem_limit_bytes=vmem),
        cost_estimate=pl.CostEstimate(flops=flops, bytes_accessed=1 << 20, transcendentals=0),
    )(*operands)


def prepare_kernel(
    counts_hbm, examples_hbm, rows_hbm, out_ref, counts_ref, examples_ref, rows_ref, live_ref, sems
):
    copies = [
        pltpu.make_async_copy(source, target, sems.at[k])
        for k, (source, target) in enumerate(
            ((counts_hbm, counts_ref), (examples_hbm, examples_ref), (rows_hbm, rows_ref))
        )
    ]
    for copy in copies:
        copy.start()
    depth, across, under, capacity = rows_ref.shape
    tables, owners = counts_ref.shape
    buckets = owners * tables
    bucket = lax.broadcasted_iota(jnp.int32, (buckets, owners), 0)
    owner = lax.broadcasted_iota(jnp.int32, (buckets, owners), 1)
    spread = jnp.where(bucket // tables == owner, 1.0, 0.0).astype(jnp.bfloat16)
    table = lax.broadcasted_iota(jnp.int32, (buckets, tables), 1)
    own = lax.broadcasted_iota(jnp.int32, (buckets, tables), 0) % tables
    slot = lax.broadcasted_iota(jnp.int32, (buckets, capacity), 1).astype(jnp.float32)
    copies[0].wait()
    counts = counts_ref[...].astype(jnp.float32).astype(jnp.bfloat16)
    by_table = lax.dot_general(
        spread, counts, (((1,), (1,)), ((), ())), preferred_element_type=jnp.float32
    )
    count = jnp.sum(jnp.where(table == own, by_table, 0.0), axis=1, keepdims=True)
    copies[1].wait()
    live = jnp.where(slot < count, examples_ref[...].reshape(buckets, capacity), DEAD)
    live_ref[...] = live.reshape(live_ref.shape)
    copies[2].wait()
    odd = lax.axis_index("zp")
    core = lax.axis_index("c")
    mine = lax.broadcasted_iota(jnp.int32, (across, under, capacity), 1) < tables

    def core_first(value):
        swapped = jnp.concatenate([value[:, tables:], value[:, :tables]], axis=1)
        return jnp.where(core == 0, value, swapped)

    for q in range(depth // 2):
        here = 2 * q + odd
        even_pair = 2 * q + 1 - odd
        odd_pair = lax.rem(2 * q + depth - 1 + 3 * odd, depth)
        first = jnp.where(core == 0, even_pair, odd_pair)
        second = jnp.where(core == 0, odd_pair, even_pair)
        for ref, lanes in ((rows_ref, slice(0, capacity)), (live_ref, slice(capacity, None))):
            out_ref[q, :, :under, lanes] = core_first(ref[here])
            out_ref[q, :, under:, lanes] = core_first(jnp.where(
                mine == (core == 0), ref[first], ref[second]
            ))


def split_into(out_ref, place, full):
    width = full.shape[1]
    high = full.astype(jnp.bfloat16)
    out_ref[place, :, :width] = high
    out_ref[place, :, width:] = (full - high.astype(jnp.float32)).astype(jnp.bfloat16)


def split_kernel(*refs):
    out_ref = refs[-1]
    count = refs[0].shape[0]
    for place, ref in enumerate(refs[:-1]):
        for t in range(count):
            split_into(out_ref, place * count + t, ref[t])


def split_tables(*tables):
    count, rows, width = tables[0].shape
    return local_kernel(
        split_kernel,
        jax.ShapeDtypeStruct((len(tables) * count, rows, 2 * width), jnp.bfloat16),
        tables,
    )


def one_hot(mask):
    return jnp.where(mask, 1.0, 0.0).astype(jnp.bfloat16)


def bags_kernel(*refs, examples, count, parts):
    ids_ref, near_ref, part_ref, shared_ref, *refs = refs
    out_refs, refs = refs[: len(parts)], refs[len(parts) :]
    (looked_ref,) = refs
    group, ring, messages, lanes = ids_ref.shape
    rows, wide = near_ref.shape[1:]
    owners = messages // count
    slots = lanes // 2
    core = lax.axis_index("c")
    aways = tuple(dict.fromkeys(away for away, _ in parts))
    depth = lax.axis_index("zq")
    row_iota = lax.broadcasted_iota(jnp.int32, (slots, rows), 1)
    key_iota = lax.broadcasted_iota(jnp.int32, (group * examples, group * slots), 0)
    columns, keys = [], []
    for away in aways:
        chosen = away[0] + core * (away[1] - away[0])
        column = lax.rem(lax.axis_index("x") + chosen, ring)
        ids = [ids_ref[lax.rem(depth + j, group), column] for j in range(group)]
        columns.append(jnp.swapaxes(jnp.concatenate(ids, axis=0), 0, 1))
        keys.append(
            jnp.concatenate([ids[j][:, slots:] + j * examples for j in range(group)], axis=1)
        )
    block = group * slots

    def look(o, t):
        ref, place = ((near_ref, t), (near_ref, count + t), (part_ref, t), (shared_ref, t))[o]
        message = o * count + t
        picks = jnp.concatenate(
            [
                one_hot(
                    one[:slots, j * messages + message : j * messages + message + 1] == row_iota
                )
                for one in columns
                for j in range(group)
            ],
            axis=0,
        )
        looked = jnp.dot(picks, ref[place], preferred_element_type=jnp.float32)
        for k in range(len(aways)):
            looked_ref[k, t, o * block : (o + 1) * block, :] = looked[
                k * block : (k + 1) * block
            ].astype(jnp.bfloat16)

    def pool(k, t, out_ref, place):
        into = [
            one_hot(keys[k][o * count + t : o * count + t + 1] == key_iota) for o in range(owners)
        ]
        total = jnp.dot(
            jnp.concatenate(into, axis=1), looked_ref[k, t], preferred_element_type=jnp.float32
        )
        summed = total[:, : wide // 2] + total[:, wide // 2 :]
        out_ref[:, place * examples : (place + 1) * examples, :] = summed.reshape(
            group, examples, wide // 2
        )

    for t in dict.fromkeys(t for _, chosen in parts for t in chosen):
        for o in range(owners):
            look(o, t)
        for (away, chosen), out_ref in zip(parts, out_refs):
            if t in chosen:
                pool(aways.index(away), t, out_ref, chosen.index(t))


def bags(ids, near, part, shared, examples, parts):
    group, _, messages, lanes = ids.shape
    count, rows, wide = part.shape
    tasks = sum(len(tables) for _, tables in parts)
    work = messages // count * tasks * group * lanes // 2
    out = tuple(
        jax.ShapeDtypeStruct((group, len(tables) * examples, wide // 2), jnp.float32)
        for _, tables in parts
    )
    chunks = len(set(away for away, _ in parts))
    scratch = [
        pltpu.VMEM((chunks, count, messages // count * group * lanes // 2, wide), jnp.bfloat16)
    ]
    return local_kernel(
        functools.partial(bags_kernel, examples=examples, count=count, parts=parts),
        out,
        (ids, near, part, shared),
        flops=2 * work * wide * (rows + group * examples),
        vmem=20 << 20,
        scratch=scratch,
    )


def far_chunk(ids_ref, examples):
    group, ring, _, lanes = ids_ref.shape
    column = lax.rem(lax.axis_index("x") + ring // 2, ring)
    depth = lax.axis_index("zq")
    ids = [ids_ref[lax.rem(depth + j, group), column] for j in range(group)]
    columns = jnp.swapaxes(jnp.concatenate(ids, axis=0), 0, 1)[: lanes // 2]
    keys = jnp.concatenate([ids[j][:, lanes // 2 :] + j * examples for j in range(group)], axis=1)
    return columns, keys


def far_look(ids_ref, columns, message, table):
    group, _, messages, lanes = ids_ref.shape
    row_iota = lax.broadcasted_iota(jnp.int32, (lanes // 2, table.shape[0]), 1)
    picks = jnp.concatenate(
        [
            one_hot(columns[:, j * messages + message : j * messages + message + 1] == row_iota)
            for j in range(group)
        ],
        axis=0,
    )
    looked = jnp.dot(picks, table, preferred_element_type=jnp.float32)
    return looked.astype(jnp.bfloat16)


def far_look_kernel(
    ids_ref, near_ref, part_ref, shared_hbm, looked_ref, shared_ref, full_ref, sem, *, examples
):
    copy = pltpu.make_async_copy(shared_hbm, full_ref, sem)
    copy.start()
    count = part_ref.shape[0]
    block = ids_ref.shape[0] * ids_ref.shape[3] // 2
    columns, _ = far_chunk(ids_ref, examples)
    for t in range(count):
        for o, ref in enumerate((near_ref.at[t], near_ref.at[count + t], part_ref.at[t])):
            looked_ref[t, o * block : (o + 1) * block, :] = far_look(
                ids_ref, columns, o * count + t, ref[...]
            )
    copy.wait()
    for t in range(count):
        split_into(shared_ref, t, full_ref[t])


def far_pool_kernel(ids_ref, shared_ref, looked_ref, out_ref, *, examples, tables):
    group, _, messages, lanes = ids_ref.shape
    count, _, wide = shared_ref.shape
    owners = messages // count
    columns, keys = far_chunk(ids_ref, examples)
    key_iota = lax.broadcasted_iota(jnp.int32, (group * examples, group * lanes // 2), 0)
    for place, t in enumerate(tables):
        last = far_look(ids_ref, columns, (owners - 1) * count + t, shared_ref[t])
        into = [one_hot(keys[o * count + t : o * count + t + 1] == key_iota) for o in range(owners)]
        total = jnp.dot(
            jnp.concatenate(into[:-1], axis=1), looked_ref[t], preferred_element_type=jnp.float32
        ) + jnp.dot(into[-1], last, preferred_element_type=jnp.float32)
        summed = total[:, : wide // 2] + total[:, wide // 2 :]
        out_ref[:, place * examples : (place + 1) * examples, :] = summed.reshape(
            group, examples, wide // 2
        )


def by_core(value, by, ring):
    pairs = [
        (2 * i + c, 2 * ((i + by * (1 - 2 * c)) % ring) + c) for i in range(ring) for c in range(2)
    ]
    return lax.ppermute(value, ("x", "c"), pairs)


def add_kernel(one_ref, two_ref, out_ref):
    out_ref[...] = one_ref[...] + two_ref[...]


def join_kernel(own_ref, soon_ref, low_ref, high_ref, *out_refs):
    half = low_ref.shape[1]
    odd = lax.rem(lax.axis_index("zq"), 2)
    for j, out_ref in zip((0, 2, 1 + 2 * odd, 3 - 2 * odd), out_refs):
        out_ref[:half] = own_ref[j, :half] + soon_ref[j, :half] + low_ref[j]
        out_ref[half:] = own_ref[j, half:] + soon_ref[j, half:] + high_ref[j]


def swapped(value, axis, partner):
    return lax.ppermute(value, axis, [(i, partner(i)) for i in range(lax.axis_size(axis))])


def pairs_kernel(own_ref, one_ref, two_ref, three_ref, dense_ref, pairs_ref, summed_ref):
    examples = dense_ref.shape[0]
    pooled = own_ref[...] + one_ref[...] + two_ref[...] + three_ref[...]
    summed_ref[...] = pooled
    tables = pooled.shape[0] // examples
    vectors = [dense_ref[...]]
    for t in range(tables):
        vectors.append(pooled[t * examples : (t + 1) * examples])
    lane = lax.broadcasted_iota(jnp.int32, dense_ref.shape, 1)
    pairs = jnp.zeros(dense_ref.shape, jnp.float32)
    place = 0
    for i in range(tables + 1):
        for j in range(i + 1, tables + 1):
            product = jnp.sum(vectors[i] * vectors[j], axis=1, keepdims=True)
            pairs = jnp.where(lane == place, product, pairs)
            place += 1
    pairs_ref[...] = jnp.swapaxes(pairs, 0, 1)[: pairs_ref.shape[0]]


def pooled_kernel(summed_ref, pooled_ref):
    examples, tables = pooled_ref.shape[:2]
    for t in range(tables):
        pooled_ref[:, t, :] = summed_ref[t * examples : (t + 1) * examples]


def body(embedding, tables, dense_features, slot_rows, slot_examples, slot_counts):
    count, rows, width = tables.shape
    examples = dense_features.shape[0]
    capacity = slot_rows.shape[3]
    group, parities, ring, cores = (lax.axis_size(a) for a in ROWS)
    depth = group * parities

    pairs = [
        (2 * i + k, 2 * (i ^ 1 if k == 0 else (i + (1 if i % 2 else -1)) % depth) + k)
        for i in range(depth)
        for k in range(cores)
    ]
    part = lax.ppermute(tables, Z + ("c",), pairs)
    other = shifted(tables, "c", 1)
    split_ids = (depth, ring, cores * count, capacity)
    ids = local_kernel(
        prepare_kernel,
        jax.ShapeDtypeStruct((group, ring, 2 * cores * count, 2 * capacity), jnp.int32),
        (slot_counts[0].T, slot_examples.reshape(split_ids), slot_rows.reshape(split_ids)),
        vmem=67043328,
        scratch=[
            pltpu.VMEM(slot_counts.shape[:0:-1], jnp.int32),
            pltpu.VMEM(split_ids, jnp.int32),
            pltpu.VMEM(split_ids, jnp.int32),
            pltpu.VMEM(split_ids, jnp.int32),
            pltpu.SemaphoreType.DMA((3,)),
        ],
        in_hbm=range(3),
    )
    ids = ids.reshape((group * ring,) + ids.shape[2:])
    ids = lax.all_to_all(ids, ("zq", "x"), 0, 0, tiled=True)
    ids = ids.reshape((group, ring) + ids.shape[1:])
    shared = shifted(part, "c", 1)
    near = split_tables(tables, other)
    part = split_tables(part)

    low, high = tuple(range(count // 2)), tuple(range(count // 2, count))
    whole = low + high

    block = group * capacity
    looked, shared = local_kernel(
        functools.partial(far_look_kernel, examples=examples),
        (
            jax.ShapeDtypeStruct((count, (2 * cores - 1) * block, 2 * width), jnp.bfloat16),
            jax.ShapeDtypeStruct(part.shape, part.dtype),
        ),
        (ids, near, part, shared),
        flops=2 * 3 * cores * count * block * rows * width,
        vmem=16 << 20,
        scratch=[pltpu.VMEM(shared.shape, jnp.float32), pltpu.SemaphoreType.DMA],
        in_hbm=(3,),
    )

    def far_pool(tables):
        return local_kernel(
            functools.partial(far_pool_kernel, examples=examples, tables=tables),
            jax.ShapeDtypeStruct((group, len(tables) * examples, width), jnp.float32),
            (ids, shared, looked),
            flops=4 * len(tables) * block * rows * width,
        )

    far_low = far_pool(low)
    far_low = by_core(far_low, 1, ring)
    far_high = far_pool(high)
    far_high = by_core(far_high, 1, ring)
    soon, late_low, late_high = bags(
        ids, near, part, shared, examples, (((3, 1), whole), ((1, 3), low), ((1, 3), high))
    )
    soon = by_core(soon, -1, ring)
    piece = jax.ShapeDtypeStruct(late_low.shape, late_low.dtype)
    late_low = local_kernel(add_kernel, piece, (late_low, far_low))
    late_low = by_core(late_low, 1, ring)
    late_high = local_kernel(add_kernel, piece, (late_high, far_high))
    late_high = by_core(late_high, 1, ring)
    (own,) = bags(ids, near, part, shared, examples, (((0, 0), whole),))
    final = jax.ShapeDtypeStruct(own.shape[1:], jnp.float32)
    here, *others = local_kernel(
        join_kernel, (final,) * group, (own, soon, late_low, late_high)
    )
    partners = (lambda i: i ^ 2, lambda i: 3 - i, lambda i: i ^ 1)
    for k, partner in enumerate((partners[0], partners[2], partners[1])):
        others[k] = swapped(others[k], "zq", partner)
    pairs = count * (count + 1) // 2
    products, summed = local_kernel(
        pairs_kernel,
        (
            jax.ShapeDtypeStruct((pairs, examples), jnp.float32),
            jax.ShapeDtypeStruct((count * examples, width), jnp.float32),
        ),
        (here, *others, dense_features),
    )
    pooled = local_kernel(
        pooled_kernel,
        jax.ShapeDtypeStruct((examples, count, width), jnp.float32),
        (summed,),
    )
    got = []
    for partner in partners:
        got.append(swapped(products, "y", partner))
    total = ((products + got[0]) + (got[1] + got[2])) * embedding**-0.5
    return pooled, total.T


def solution(mesh):
    torus = Mesh(mesh.devices.reshape(4, 2, 4, 2, mesh.shape["cols"]), ROWS + ("y",))

    def layer(*args):
        return body(512, *args)

    return jax.shard_map(
        layer,
        mesh=torus,
        in_specs=(
            P(None, ROWS, "y"),
            P(ROWS, "y"),
            P(ROWS, None, None, None),
            P(ROWS, None, None, None),
            P(ROWS, None, None),
        ),
        out_specs=(P(ROWS, None, "y"), P(ROWS, None)),
        check_vma=False,
    )
```
